128 devices in a mesh: dom: 32 (over x, y, core), grp: 4 (over z).
Axes of the slice: x: 4, y: 4, z: 4, core: 2. Of those that a mesh axis runs over, the one named last changes fastest.
Arguments:
- features: bfloat16 [262144, 256], P(('dom', 'grp')), may hold values from -6 to 6
- edge_src: int32 [2097152], P(('dom', 'grp')), may hold values from 0 to 3071, as said below
- edge_dst: int32 [2097152], P(('dom', 'grp')), may hold values from 0 to 2047, as said below
- edge_count: int32 [128], P(('dom', 'grp')), may hold values from 4096 to 16384, as said below
- halo_index: int32 [128, 128, 8], P(('dom', 'grp')), may hold values from 0 to 2047
- request_rows: int32 [128, 128, 16], P(('dom', 'grp')), may hold values from 0 to 2047, as said below
- pair_ends: int32 [262144, 2], P(('dom', 'grp')), may hold values from 0 to 2047
- labels: int32 [262144], P(('dom', 'grp')), may hold values 0 or 1
- pair_weight: float32 [262144], P(('dom', 'grp')), may hold values from 0.25 to 4
- w_self: bfloat16 [256, 256], replicated, may hold values from -0.375 to 0.375
- w_neigh: bfloat16 [256, 256], replicated, may hold values from -0.375 to 0.375
- w_hidden: bfloat16 [512, 256], replicated, may hold values from -0.25 to 0.25
- b_hidden: float32 [256], replicated, may hold values from -3 to 3
- w_out: float32 [256], replicated, may hold values from -0.375 to 0.375
Outputs:
- logits: float32 [262144], P(('dom', 'grp'))
- grad_features: float32 [262144, 256], P(('dom', 'grp'))
- grad_w_self: float32 [256, 256], replicated
- grad_w_neigh: float32 [256, 256], replicated
- grad_w_hidden: float32 [512, 256], replicated
- grad_b_hidden: float32 [256], replicated
- grad_w_out: float32 [256], replicated
The draws below stay inside these ranges and needn't reach their ends.
Inputs may be any that keep to these rules, and one draw needn't show every extreme that they name: `edge_src`: a row of the partition's own table. `edge_dst`: a local node of the partition; slots at or past edge_count are not live and hold arbitrary values. `edge_count`: some partition has exactly 16384 live slots. `halo_index`: local rows of the sending partition; 8 to every partition, itself included. `request_rows`: local rows of the owning partition, distinct and increasing within each list of 16. `pair_ends`: rows of the shard's own received rows.
All inputs are finite; a program needn't handle non-finite values. No bound on the sum of `labels` on one device may be relied on, other than what follows from the above.
Results may differ from the reference program's by a relative error of at most 0.02.
The reference program's roundings to bfloat16 on the way count: a program that leaves them out, or rounds other values in their place, can miss the bound.
Values may be sent and summed in bfloat16 or wider, within the bound.
No kernel may reach another device: no remote copies, remote signals or barrier semaphores. Data moves between devices by JAX's collectives and lax.ppermute only.
A program may use at most 192 MiB of HBM per device.

```python
import math
import jax
import jax.numpy as jnp
from jax import lax

D = 256
NODE_DEV = 2048
HALO = 8
REQ = 16
TE_DEV = 2048
PARTITIONS = 128
EDGE_DEV = 16384
NODES = 262144
EDGES = 2097152
TRAIN = 262144
RECEIVED = 2048


def draw_edge_src(key, part):
    key_one, key_two, key_three = jax.random.split(key, 3)
    coin_flip = jax.random.randint(key_one, (EDGES,), 0, 2)
    local_rows = jax.random.randint(key_two, (EDGES,), 0, NODE_DEV)
    remote_rows = NODE_DEV + jax.random.randint(key_three, (EDGES,), 0, HALO * PARTITIONS)
    return jnp.where(coin_flip == 0, local_rows, remote_rows).astype(jnp.int32)


def draw_edge_dst(key, part):
    key_one, key_two = jax.random.split(key, 2)
    first_draw = jax.random.randint(key_one, (EDGES,), 0, NODE_DEV)
    second_draw = jax.random.randint(key_two, (EDGES,), 0, NODE_DEV)
    return (first_draw * second_draw // (NODE_DEV - 1)).astype(jnp.int32)


def draw_edge_count(key, part):
    key_one, key_two = jax.random.split(key, 2)
    divisor = 1 + jax.random.randint(key_one, (PARTITIONS,), 0, 4)
    counts = EDGE_DEV // divisor
    full_one = jax.random.randint(key_two, (), 0, PARTITIONS)
    return jnp.where(jnp.arange(PARTITIONS) == full_one, EDGE_DEV, counts).astype(jnp.int32)


def draw_request_rows(key, part):
    stride = NODE_DEV // REQ
    offsets = jax.random.randint(key, (PARTITIONS, PARTITIONS, REQ), 0, stride)
    return (jnp.arange(REQ, dtype=jnp.int32)[None, None, :] * stride + offsets).astype(jnp.int32)


def set_ends(entries, stream_key, smallest, top_value):
    shape = entries.shape
    spot = [jax.random.randint(jax.random.fold_in(stream_key, axis), (), 0, shape[axis]) for axis in range(len(shape))]
    entries = entries.at[tuple(spot)].set(smallest)
    longest = shape.index(max(shape))
    spot[longest] = (spot[longest] + 1) % shape[longest]
    return entries.at[tuple(spot)].set(top_value)


def levels(key, extent, cuts, smallest, top_value):
    level = 1.0
    for dim, shards_of in cuts:
        heights = jax.random.uniform(jax.random.fold_in(jax.random.fold_in(key, 6), dim), (shards_of,), jnp.float32, smallest / len(cuts), top_value / len(cuts))
        level = level * jnp.repeat(jnp.exp(heights), extent[dim] // shards_of).reshape((-1,) + (1,) * (len(extent) - 1 - dim))
    return level


def noise(own_key, extent, width, most, cuts=(), kind=jnp.bfloat16):
    level = levels(own_key, extent, cuts, -0.22, 0.18) if cuts else 1.0
    entries = jax.random.normal(own_key, extent, jnp.float32) * width * level
    return jnp.minimum(jnp.maximum(entries, -most), most).astype(kind)


def setup_inputs(seed: int = 0) -> dict:
    streams_of = jax.random.split(jax.random.key(seed), 15)
    features = noise(streams_of[0], (NODES, D), 1.0, 6.0, ((0, 128),))
    edge_src = draw_edge_src(jax.random.fold_in(streams_of[14], 71), 0)
    edge_dst = draw_edge_dst(jax.random.fold_in(streams_of[14], 71), 0)
    edge_count = draw_edge_count(jax.random.fold_in(streams_of[14], 71), 0)
    halo_index = set_ends(jax.random.randint(streams_of[4], (PARTITIONS, PARTITIONS, HALO), 0, NODE_DEV), jax.random.fold_in(streams_of[4], 1), 0, NODE_DEV - 1).astype(jnp.int32)
    request_rows = draw_request_rows(jax.random.fold_in(streams_of[14], 71), 0)
    pair_ends = set_ends(jax.random.randint(streams_of[6], (TRAIN, 2), 0, RECEIVED), jax.random.fold_in(streams_of[6], 1), 0, RECEIVED - 1).astype(jnp.int32)
    labels = set_ends((jax.random.randint(streams_of[7], (TRAIN,), 0, 2) < 1).astype(jnp.int32), jax.random.fold_in(streams_of[7], 1), 0, 1)
    pair_weight = jnp.clip(jnp.exp(math.log(4.0) - 2.7725887 * jax.random.uniform(streams_of[8], (TRAIN,), jnp.float32) ** levels(streams_of[8], (TRAIN,), ((0, 128),), -0.2, 0.2)), 0.25, 4.0)
    w_self = noise(streams_of[9], (D, D), D ** -0.5, 0.375)
    w_neigh = noise(streams_of[10], (D, D), D ** -0.5, 0.375)
    w_hidden = noise(streams_of[11], (2 * D, D), (2 * D) ** -0.5, 0.25)
    b_hidden = noise(streams_of[12], (D,), 0.5, 3.0, (), jnp.float32)
    w_out = noise(streams_of[13], (D,), D ** -0.5, 0.375, (), jnp.float32)
    return dict(features=features, edge_src=edge_src, edge_dst=edge_dst, edge_count=edge_count, halo_index=halo_index, request_rows=request_rows, pair_ends=pair_ends, labels=labels, pair_weight=pair_weight, w_self=w_self, w_neigh=w_neigh, w_hidden=w_hidden, b_hidden=b_hidden, w_out=w_out)


def encode_one(own_rows, halo_rows, src_slots, dst_slots, live_count, w_self, w_neigh):
    row_table = jnp.concatenate([own_rows, halo_rows], axis=0)
    slot_ids = jnp.arange(src_slots.shape[0], dtype=jnp.int32)
    alive_slot = slot_ids < live_count
    dst_index = jnp.where(alive_slot, dst_slots, NODE_DEV).astype(jnp.int32)
    gathered = row_table[src_slots].astype(jnp.float32)
    agg_sums = jax.ops.segment_sum(gathered, dst_index, num_segments=NODE_DEV + 1)[:NODE_DEV]
    degree = jax.ops.segment_sum(alive_slot.astype(jnp.float32), dst_index, num_segments=NODE_DEV + 1)[:NODE_DEV]
    aggregate = (agg_sums / jnp.maximum(degree, 1.0)[:, None]).astype(jnp.bfloat16)
    embedding = (jnp.dot(own_rows, w_self, preferred_element_type=jnp.float32)
                 + jnp.dot(aggregate, w_neigh, preferred_element_type=jnp.float32)).astype(jnp.bfloat16)
    return embedding, aggregate, degree


def reference(features, edge_src, edge_dst, edge_count, halo_index, request_rows, pair_ends, labels, pair_weight, w_self, w_neigh, w_hidden, b_hidden, w_out):
    part_count = PARTITIONS
    own_rows = features.reshape(part_count, NODE_DEV, D)
    senders = jnp.arange(part_count, dtype=jnp.int32)[:, None, None]
    sent_rows = own_rows[senders, halo_index]
    arriving = jnp.transpose(sent_rows, (1, 0, 2, 3)).reshape(part_count, part_count * HALO, D)
    src_slots = edge_src.reshape(part_count, EDGE_DEV)
    dst_slots = edge_dst.reshape(part_count, EDGE_DEV)

    def encode_step(packed):
        return encode_one(packed[0], packed[1], packed[2], packed[3], packed[4], w_self, w_neigh)

    embedding, aggregate, degree = lax.map(encode_step, (own_rows, arriving, src_slots, dst_slots, edge_count))

    end_pairs = pair_ends.reshape(part_count, TE_DEV, 2)
    flag_rows = labels.reshape(part_count, TE_DEV).astype(jnp.float32)
    weight_rows = pair_weight.reshape(part_count, TE_DEV)
    owners = jnp.arange(part_count, dtype=jnp.int32)[:, None]

    def decode_step(carry, packed):
        emb_grad, grad_hidden, grad_bias, grad_out = carry
        wanted_rows, pair_end, flag_row, weight_row = packed
        received = embedding[owners, wanted_rows].reshape(part_count * REQ, D)
        pair_input = jnp.concatenate([received[pair_end[:, 0]], received[pair_end[:, 1]]], axis=1)
        pre_act = jnp.dot(pair_input, w_hidden, preferred_element_type=jnp.float32) + b_hidden
        hidden = jnp.maximum(pre_act, 0.0)
        logits = jnp.dot(hidden, w_out, precision=lax.Precision.HIGHEST)
        slope_term = weight_row * (jax.nn.sigmoid(logits) - flag_row)
        grad_out = grad_out + jnp.dot(slope_term, hidden, precision=lax.Precision.HIGHEST)
        delta_act = jnp.where(pre_act > 0, slope_term[:, None] * w_out[None, :], 0.0)
        grad_bias = grad_bias + jnp.sum(delta_act, axis=0)
        delta_b = delta_act.astype(jnp.bfloat16)
        grad_hidden = grad_hidden + jnp.dot(pair_input.T, delta_b, preferred_element_type=jnp.float32)
        pair_grad = jnp.dot(delta_b, w_hidden.T, preferred_element_type=jnp.float32)
        received_grad = (jax.ops.segment_sum(pair_grad[:, :D], pair_end[:, 0], num_segments=part_count * REQ)
                         + jax.ops.segment_sum(pair_grad[:, D:], pair_end[:, 1], num_segments=part_count * REQ))
        received_grad_b = lax.optimization_barrier(received_grad.astype(jnp.bfloat16))
        emb_grad = emb_grad.at[owners, wanted_rows].add(received_grad_b.astype(jnp.float32).reshape(part_count, REQ, D))
        return (emb_grad, grad_hidden, grad_bias, grad_out), logits

    start = (jnp.zeros((part_count, NODE_DEV, D), jnp.float32), jnp.zeros((2 * D, D), jnp.float32),
             jnp.zeros((D,), jnp.float32), jnp.zeros((D,), jnp.float32))
    final, logit_rows = lax.scan(decode_step, start, (request_rows, end_pairs, flag_rows, weight_rows))
    emb_grad, grad_hidden, grad_bias, grad_out = final
    grad_b = emb_grad.astype(jnp.bfloat16)

    def encode_back(packed):
        own_part, agg_part, deg_part, grad_part, src_part, dst_part, count_part = packed
        grad_self = jnp.dot(own_part.T, grad_part, preferred_element_type=jnp.float32)
        grad_neigh = jnp.dot(agg_part.T, grad_part, preferred_element_type=jnp.float32)
        direct = jnp.dot(grad_part, w_self.T, preferred_element_type=jnp.float32)
        agg_grad = jnp.dot(grad_part, w_neigh.T, preferred_element_type=jnp.float32) / jnp.maximum(deg_part, 1.0)[:, None]
        padded = jnp.concatenate([agg_grad, jnp.zeros((1, D), jnp.float32)], axis=0)
        slot_ids = jnp.arange(src_part.shape[0], dtype=jnp.int32)
        dst_index = jnp.where(slot_ids < count_part, dst_part, NODE_DEV).astype(jnp.int32)
        table_grad = jax.ops.segment_sum(padded[dst_index], src_part, num_segments=NODE_DEV + part_count * HALO)
        return (direct + table_grad[:NODE_DEV], table_grad[NODE_DEV:].reshape(part_count, HALO, D), grad_self, grad_neigh)

    local_grad, halo_back, self_terms, neigh_terms = lax.map(
        encode_back, (own_rows, aggregate, degree, grad_b, src_slots, dst_slots, edge_count))
    returned = jnp.transpose(halo_back, (1, 0, 2, 3))
    local_grad = local_grad.at[senders, halo_index].add(returned)
    return (logit_rows.reshape(part_count * TE_DEV), local_grad.reshape(part_count * NODE_DEV, D),
            jnp.sum(self_terms, axis=0), jnp.sum(neigh_terms, axis=0), grad_hidden, grad_bias, grad_out)
```

```python
import functools

import jax
import jax.numpy as jnp
from jax import lax
from jax.experimental import pallas as pl
from jax.experimental.pallas import tpu as pltpu
from jax.sharding import PartitionSpec as P

BF16, F32, I16, I32 = jnp.bfloat16, jnp.float32, jnp.int16, jnp.int32
NN = (((1,), (0,)), ((), ()))
NT = (((1,), (1,)), ((), ()))
TN = (((0,), (0,)), ((), ()))
AXES = ("dom", "grp")
DST_BLOCK = 256
SRC_BLOCK = 1024
LIMIT = pltpu.CompilerParams(vmem_limit_bytes=56 * 1024 * 1024)


def mm(left, right, dims=NN):
    return lax.dot_general(left, right, dims, preferred_element_type=F32)


def spread_hot(diff, step, count, axis):
    one, zero = jnp.ones((), BF16), jnp.zeros((), BF16)
    pieces = [jnp.where(diff == jnp.int16(step * k), one, zero) for k in range(count)]
    return jnp.concatenate(pieces, axis=axis)


def hot_rows(row, height):
    width = row.shape[1]
    wide = jnp.broadcast_to(row, (16, width)) - lax.broadcasted_iota(I32, (16, width), 0)
    return spread_hot(wide.astype(I16), 16, height // 16, 0)


def hot_tile(tile, width):
    diff = tile - lax.broadcasted_iota(I32, tile.shape, 1)
    return spread_hot(diff.astype(I16), 128, width // 128, 1)


def whole(memory_space=pltpu.VMEM):
    return pl.BlockSpec(memory_space=memory_space)


def shape_of(shape, dtype):
    return jax.ShapeDtypeStruct(shape, dtype)


def cost(flops, moved):
    return pl.CostEstimate(flops=flops, bytes_accessed=moved, transcendentals=0)


def send_body(slot_ref, halo_ref, want_ref, feat_ref, out_ref):
    parts = out_ref.shape[0]
    want = jnp.transpose(want_ref[...])
    tiled = jnp.concatenate([want] * 8, axis=1)
    lane = lax.broadcasted_iota(I32, tiled.shape, 1)
    mine = lax.shift_right_logical(lane, 4) == slot_ref[0]
    tiled = jnp.where(mine, tiled, 0)
    index = jnp.concatenate(
        [lax.shift_right_logical(tiled, 7).astype(F32), (tiled & 127).astype(F32)], axis=1
    )
    halo = halo_ref[...]
    for at in range(0, parts, 16):
        tile = jnp.concatenate(
            [jnp.broadcast_to(halo[:, p : p + 1], (8, 128)) for p in range(at, at + 16)], axis=0
        )
        rows = mm(hot_tile(tile, feat_ref.shape[0]), feat_ref[...])
        rows = rows.reshape(16, 8, rows.shape[1])
        notes = jnp.broadcast_to(index[at : at + 16, None, :], rows.shape)
        out_ref[at : at + 16] = jnp.concatenate([rows, notes], axis=1).astype(BF16)


def send_rows(slot, halo, want, features):
    parts = want.shape[1]
    return pl.pallas_call(
        send_body,
        out_shape=shape_of((parts, 16, features.shape[1]), BF16),
        in_specs=[whole(pltpu.SMEM), whole(), whole(), whole()],
        out_specs=whole(),
        compiler_params=LIMIT,
        cost_estimate=cost(10**9, 2 * 10**6),
        name="send_rows",
    )(slot, halo, want, features)


def edges_body(src_blocks, starts_ref, keys_ref, count_ref, degree_ref, acc_ref):
    block = pl.program_id(0)
    first, last = starts_ref[block], starts_ref[block + 1]
    top = keys_ref.shape[0] - 1
    row0 = lax.shift_right_logical(first, 7)
    trips = lax.shift_right_logical(lax.shift_right_logical(last + 127, 7) - row0 + 3, 2)

    def hots(trip):
        src, dst = [], []
        for i in range(4):
            row = row0 + 4 * trip + i
            keys = keys_ref[pl.ds(jnp.minimum(row, top), 1), :]
            live = jnp.logical_and(lax.shift_right_logical(keys, 18) == block, row <= top)
            dst.append(jnp.where(live, lax.shift_right_logical(keys, 10) & 255, -1))
            src.append(keys & 1023)
        return jnp.concatenate(src, axis=1), jnp.concatenate(dst, axis=1)

    def visit(trip, add):
        src, dst = hots(trip)
        right = hot_rows(dst, DST_BLOCK)
        for at in range(0, SRC_BLOCK, 256):
            part = mm(hot_rows(src - at, 256), right, NT)
            if add:
                part = acc_ref[at : at + 256, :] + part
            acc_ref[at : at + 256, :] = part

    visit(0, False)

    def again(trip, carry):
        visit(trip, True)
        return carry

    lax.fori_loop(1, trips, again, 0)
    total = acc_ref[...]
    count_ref[...] = total.astype(BF16)
    part = jnp.sum(total.reshape(SRC_BLOCK // 8, 8, DST_BLOCK), axis=0)
    opening = lax.rem(block, src_blocks) == 0

    @pl.when(opening)
    def _():
        degree_ref[...] = part

    @pl.when(jnp.logical_not(opening))
    def _():
        degree_ref[...] += part


def edge_counts(starts, keys, nodes, table):
    src_blocks = table // SRC_BLOCK
    return pl.pallas_call(
        functools.partial(edges_body, src_blocks),
        grid=(nodes // DST_BLOCK * src_blocks,),
        out_shape=(shape_of((table, nodes), BF16), shape_of((8, nodes), F32)),
        in_specs=[whole(pltpu.SMEM), whole()],
        out_specs=(
            pl.BlockSpec((SRC_BLOCK, DST_BLOCK), lambda b: (b % src_blocks, b // src_blocks)),
            pl.BlockSpec((8, DST_BLOCK), lambda b: (0, b // src_blocks)),
        ),
        scratch_shapes=[pltpu.VMEM((SRC_BLOCK, DST_BLOCK), F32)],
        compiler_params=LIMIT,
        cost_estimate=cost(14 * 10**9, 13 * 10**6),
        name="edge_counts",
    )(starts, keys)


def embed_body(
    count_ref, arrived_ref, feat_ref, degree_ref, self_ref, neigh_ref,
    served_ref, agg_ref, want_ref, table_ref, emb_ref,
):
    step = pl.program_id(0)
    nodes = feat_ref.shape[0]

    @pl.when(step == 0)
    def _():
        table_ref[:, :nodes] = jnp.transpose(feat_ref[...])
        arrived = arrived_ref[...].astype(F32)
        halo = arrived[:, :8, :].reshape(-1, arrived.shape[2]).astype(BF16)
        table_ref[:, nodes:] = jnp.transpose(halo)
        notes = arrived[:, 8:, :]
        grouped = notes.reshape(notes.shape[0] // 8, 8, 8, notes.shape[2])
        summed = jnp.sum(grouped, axis=1)[:, 0, :]
        index = summed[:, :128] * 128.0 + summed[:, 128:]
        want_ref[...] = index.astype(I32)

    sums = mm(table_ref[...], count_ref[...])
    degree = jnp.sum(degree_ref[...], axis=0, keepdims=True)
    mean = (sums / jnp.maximum(degree, 1.0)).astype(BF16)
    mean = jnp.transpose(mean)
    agg_ref[...] = mean
    at = pl.multiple_of(step * DST_BLOCK, DST_BLOCK)
    own = feat_ref[pl.ds(at, DST_BLOCK), :]
    emb_ref[pl.ds(at, DST_BLOCK), :] = (mm(own, self_ref[...]) + mm(mean, neigh_ref[...])).astype(BF16)

    @pl.when(step == pl.num_programs(0) - 1)
    def _():
        columns = jnp.transpose(want_ref[...])
        for k in range(columns.shape[1]):
            tile = jnp.broadcast_to(columns[:, k : k + 1], (128, 128))
            served_ref[k * 128 : (k + 1) * 128, :] = mm(hot_tile(tile, nodes), emb_ref[...]).astype(BF16)


def embed(counts, arrived, features, degree, w_self, w_neigh):
    table, nodes = counts.shape
    width = features.shape[1]
    return pl.pallas_call(
        embed_body,
        grid=(nodes // DST_BLOCK,),
        out_shape=(
            shape_of((nodes, width), BF16),
            shape_of((nodes, width), BF16),
            shape_of((16, 128), I32),
        ),
        in_specs=[
            pl.BlockSpec((table, DST_BLOCK), lambda i: (0, i)),
            whole(), whole(),
            pl.BlockSpec((8, DST_BLOCK), lambda i: (0, i)),
            whole(), whole(),
        ],
        out_specs=(
            pl.BlockSpec((nodes, width), lambda i: (0, 0)),
            pl.BlockSpec((DST_BLOCK, width), lambda i: (i, 0)),
            pl.BlockSpec((16, 128), lambda i: (0, 0)),
        ),
        scratch_shapes=[pltpu.VMEM((width, table), BF16), pltpu.VMEM((nodes, width), BF16)],
        compiler_params=LIMIT,
        cost_estimate=cost(6 * 10**9, 16 * 10**6),
        name="embed",
    )(counts, arrived, features, degree, w_self, w_neigh)


def decode_body(
    got_ref, ends_ref, label_ref, weight_ref, hid_ref, bias_ref, wout_ref,
    logit_ref, send_ref, grad_ref, hidden_ref, small_ref,
):
    rows, width = got_ref.shape
    pairs = ends_ref.shape[1]
    block = 256
    hidden_ref[...] = jnp.zeros_like(hidden_ref)
    small_ref[...] = jnp.zeros_like(small_ref)

    def pair_step(i, carry):
        at = pl.multiple_of(i * block, block)
        span = pl.ds(at, block)
        meta = jnp.concatenate(
            [
                ends_ref[:, span].astype(F32),
                label_ref[:, span].astype(F32),
                weight_ref[:, span],
                jnp.zeros((4, block), F32),
            ],
            axis=0,
        )
        cols = jnp.transpose(meta)
        ends = cols.astype(I32)
        left = mm(hot_tile(jnp.broadcast_to(ends[:, 0:1], (block, 128)), rows), got_ref[...])
        right = mm(hot_tile(jnp.broadcast_to(ends[:, 1:2], (block, 128)), rows), got_ref[...])
        both = jnp.concatenate([left, right], axis=1).astype(BF16)
        pre = mm(both, hid_ref[...]) + bias_ref[...]
        hidden = jnp.maximum(pre, 0.0)
        logits = jnp.sum(hidden * wout_ref[...], axis=1, keepdims=True)
        logit_ref[:, span] = jnp.transpose(jnp.broadcast_to(logits, (block, 128)))[0:1, :]
        slope = cols[:, 3:4] * (jax.nn.sigmoid(logits) - cols[:, 2:3])
        delta = jnp.where(pre > 0, slope * wout_ref[...], 0.0)
        small_ref[0:8, :] += jnp.sum(delta.reshape(block // 8, 8, width), axis=0)
        small_ref[8:16, :] += jnp.sum((slope * hidden).reshape(block // 8, 8, width), axis=0)
        delta = delta.astype(BF16)
        hidden_ref[...] += mm(both, delta, TN)
        grad_ref[span, :] = mm(delta, hid_ref[...], NT).astype(BF16)
        return carry

    lax.fori_loop(0, pairs // block, pair_step, 0)

    def row_step(i, carry):
        at = i * block
        grad = mm(hot_rows(ends_ref[0:1, :] - at, block), grad_ref[:, :width])
        grad += mm(hot_rows(ends_ref[1:2, :] - at, block), grad_ref[:, width:])
        send_ref[pl.ds(i * 16, 16), 0:16, :] = grad.reshape(16, 16, width).astype(BF16)
        return carry

    lax.fori_loop(0, rows // block, row_step, 0)
    bias = jnp.sum(small_ref[0:8, :], axis=0, keepdims=True)
    wout = jnp.sum(small_ref[8:16, :], axis=0, keepdims=True)
    lines = []
    for line in (bias, wout):
        high = line.astype(BF16).astype(F32)
        for half in (high, line - high):
            lines += [half[:, :128], half[:, 128:]]
    tail = jnp.concatenate(lines, axis=0)
    total = hidden_ref[...].reshape(-1, 8, width)
    tail = jnp.broadcast_to(tail[None], (total.shape[0], 8, 128))
    even = jnp.concatenate([total[:, :, :128], tail], axis=2)
    odd = jnp.concatenate([total[:, :, 128:], tail], axis=2)
    joined = jnp.stack([even, odd], axis=1).reshape(-1, 8, width)
    send_ref[:, 16:24, :] = joined.astype(BF16)


def decode(got, ends, labels, weights, w_hidden, bias, w_out, parts):
    rows, width = got.shape
    pairs = ends.shape[1]
    return pl.pallas_call(
        decode_body,
        out_shape=(shape_of((1, pairs), F32), shape_of((parts, 24, width), BF16)),
        in_specs=[whole()] * 7,
        out_specs=(whole(), whole()),
        scratch_shapes=[
            pltpu.VMEM((pairs, 2 * width), BF16),
            pltpu.VMEM((2 * width, width), F32),
            pltpu.VMEM((16, width), F32),
        ],
        compiler_params=LIMIT,
        cost_estimate=cost(10 * 10**9, 4 * 10**6),
        name="decode",
    )(got, ends, labels, weights, w_hidden, bias, w_out)


def spread_body(
    count_ref, back_ref, want_ref, feat_ref, agg_ref, degree_ref, self_ref, neigh_ref,
    send_ref, direct_ref, small_ref, grad_ref, mean_ref,
):
    step = pl.program_id(0)
    nodes, width = feat_ref.shape
    halo_steps = 2
    rows = count_ref.shape[0]

    @pl.when(step == 0)
    def _():
        back = back_ref[...].astype(F32)
        tail = jnp.sum(back[:, 16:, :], axis=0)
        small_ref[...] = tail[:, 128:]
        flat = back[:, :16, :].reshape(-1, width).astype(BF16)
        want = jnp.concatenate([want_ref[k : k + 1, :] for k in range(16)], axis=1)
        for at in range(0, nodes, 256):
            grad = mm(hot_rows(want - at, 256), flat).astype(BF16)
            grad_ref[at : at + 256, :] = grad
            degree = jnp.sum(degree_ref[:, at : at + 256], axis=0, keepdims=True)
            column = jnp.transpose(jnp.broadcast_to(jnp.maximum(degree, 1.0), (128, 256)))
            scaled = mm(grad, neigh_ref[...], NT) / jnp.concatenate([column, column], axis=1)
            mean_ref[at : at + 256, :] = scaled.astype(BF16)
        both = jnp.concatenate(
            [mm(feat_ref[...], grad_ref[...], TN), mm(agg_ref[...], grad_ref[...], TN)], axis=0
        )
        both = both.reshape(-1, 8, width)
        tail = jnp.broadcast_to(tail[None, :, :128], (both.shape[0], 8, 128))
        even = jnp.concatenate([both[:, :, :128], tail], axis=2)
        odd = jnp.concatenate([both[:, :, 128:], tail], axis=2)
        joined = jnp.stack([even, odd], axis=1).reshape(-1, 8, width)
        send_ref[:, 8:16, :] = joined.astype(BF16)

    grad = mm(count_ref[...], mean_ref[...])

    @pl.when(step < halo_steps)
    def _():
        peers = rows // 8
        send_ref[pl.ds(step * peers, peers), 0:8, :] = grad.reshape(peers, 8, width).astype(BF16)

    @pl.when(step >= halo_steps)
    def _():
        at = pl.multiple_of((step - halo_steps) * rows, rows)
        direct_ref[...] = mm(grad_ref[pl.ds(at, rows), :], self_ref[...], NT) + grad


def spread(counts, back, want, features, agg, degree, w_self, w_neigh):
    table, nodes = counts.shape
    width = features.shape[1]
    rows = 512
    own = nodes // rows
    return pl.pallas_call(
        spread_body,
        grid=(table // rows,),
        out_shape=(
            shape_of((back.shape[0], 16, width), BF16),
            shape_of((nodes, width), F32),
            shape_of((8, 128), F32),
        ),
        in_specs=[
            pl.BlockSpec((rows, nodes), lambda i: ((i + own) % (table // rows), 0)),
            whole(), whole(), whole(), whole(), whole(), whole(), whole(),
        ],
        out_specs=(
            pl.BlockSpec((back.shape[0], 16, width), lambda i: (0, 0, 0)),
            pl.BlockSpec((rows, width), lambda i: (jnp.maximum(i - 2, 0), 0)),
            pl.BlockSpec((8, 128), lambda i: (0, 0)),
        ),
        scratch_shapes=[pltpu.VMEM((nodes, width), BF16), pltpu.VMEM((nodes, width), BF16)],
        compiler_params=LIMIT,
        cost_estimate=cost(7 * 10**9, 20 * 10**6),
        name="spread",
    )(counts, back, want, features, agg, degree, w_self, w_neigh)


def chunk_body(back_ref, out_ref):
    tail = jnp.sum(back_ref[:, 8:, :].astype(F32), axis=0)[:, :128]
    out_ref[...] = jnp.broadcast_to(tail[None], out_ref.shape).astype(BF16)


def chunk(back):
    return pl.pallas_call(
        chunk_body,
        out_shape=shape_of((back.shape[0], 8, 128), BF16),
        in_specs=[whole()],
        out_specs=whole(),
        compiler_params=LIMIT,
        cost_estimate=cost(10**6, 10**6),
        name="chunk",
    )(back)


def join_lanes(pieces):
    pieces = pieces.reshape(-1, 2, 8, 128)
    return jnp.concatenate([pieces[:, 0], pieces[:, 1]], axis=2).reshape(-1, 256)


def final_body(direct_ref, back_ref, halo_ref, small_ref, out_ref, hidden_ref, bias_ref, wout_ref):
    back = back_ref[...].astype(F32)
    width = back.shape[2]
    flat = back[:, :8, :].reshape(-1, width).astype(BF16)
    halo = jnp.concatenate([halo_ref[k : k + 1, :] for k in range(8)], axis=1)
    for at in range(0, out_ref.shape[0], 256):
        out_ref[at : at + 256, :] = direct_ref[at : at + 256, :] + mm(hot_rows(halo - at, 256), flat)
    hidden_ref[...] = join_lanes(back[:, 8:, 128:])
    bias_ref[...] = small_ref[0:2, :] + small_ref[2:4, :]
    wout_ref[...] = small_ref[4:6, :] + small_ref[6:8, :]


def final(direct, back, halo, small):
    nodes, width = direct.shape
    return pl.pallas_call(
        final_body,
        out_shape=(
            shape_of((nodes, width), F32),
            shape_of((2 * width, width), F32),
            shape_of((2, 128), F32),
            shape_of((2, 128), F32),
        ),
        in_specs=[whole()] * 4,
        out_specs=(whole(),) * 4,
        compiler_params=LIMIT,
        cost_estimate=cost(2 * 10**9, 6 * 10**6),
        name="final",
    )(direct, back, halo, small)


def weights_body(pieces_ref, self_ref, neigh_ref):
    both = join_lanes(pieces_ref[...].astype(F32))
    half = both.shape[0] // 2
    self_ref[...] = both[:half, :]
    neigh_ref[...] = both[half:, :]


def weights(pieces):
    shape = shape_of((256, 256), F32)
    return pl.pallas_call(
        weights_body,
        out_shape=(shape, shape),
        in_specs=[whole()],
        out_specs=(whole(), whole()),
        compiler_params=LIMIT,
        cost_estimate=cost(10**6, 10**6),
        name="weights",
    )(pieces)


def exchange(rows):
    return lax.all_to_all(rows, AXES, split_axis=0, concat_axis=0, tiled=True)


def per_device(
    features, edge_src, edge_dst, edge_count, halo_index, request_rows, pair_ends,
    labels, pair_weight, w_self, w_neigh, w_hidden, b_hidden, w_out,
):
    nodes, width = features.shape
    parts, halo_len = halo_index.shape[1:]
    table = nodes + parts * halo_len
    slots = edge_src.shape[0]
    me = lax.axis_index("dom") * lax.axis_size("grp") + lax.axis_index("grp")

    sent = send_rows((me % 8).reshape(1), halo_index[0].T, request_rows[0].T, features)
    arrived = exchange(sent)

    src_blocks = table // SRC_BLOCK
    buckets = nodes // DST_BLOCK * src_blocks
    bucket = edge_dst // DST_BLOCK * src_blocks + edge_src // SRC_BLOCK
    packed = (bucket << 18) | ((edge_dst % DST_BLOCK) << 10) | (edge_src % SRC_BLOCK)
    live = jnp.arange(slots, dtype=I32) < edge_count[0]
    keys = jnp.where(live, packed, buckets << 18)
    bounds = jnp.arange(buckets + 1, dtype=I32) << 18
    starts = jnp.sum((keys[None, :] < bounds[:, None]).astype(I32), axis=1)
    keys = lax.sort(keys, is_stable=False)
    counts, degree = edge_counts(starts, keys.reshape(slots // 128, 128), nodes, table)

    served, agg, want = embed(counts, arrived, features, degree, w_self, w_neigh)
    got = exchange(served.reshape(parts, -1, width)).reshape(-1, width)
    logits, pair_back = decode(
        got, pair_ends.T, labels.reshape(1, -1), pair_weight.reshape(1, -1),
        w_hidden, b_hidden.reshape(1, -1), w_out.reshape(1, -1), parts,
    )
    back = exchange(pair_back)
    halo_back, direct, small = spread(counts, back, want, features, agg, degree, w_self, w_neigh)
    returned = exchange(halo_back)
    pieces = exchange(chunk(returned))
    grad_features, grad_hidden, grad_bias, grad_out = final(
        direct, returned, halo_index[0].reshape(8, -1), small
    )
    grad_self, grad_neigh = weights(pieces)
    return (
        logits.reshape(-1), grad_features, grad_self, grad_neigh, grad_hidden,
        grad_bias.reshape(-1), grad_out.reshape(-1),
    )


def solution(mesh):
    split, rows, cubes = P(AXES), P(AXES, None), P(AXES, None, None)
    in_specs = (
        rows, split, split, split, cubes, cubes, rows, split, split, P(), P(), P(), P(), P(),
    )
    out_specs = (split, rows, P(), P(), P(), P(), P())
    return jax.shard_map(
        per_device, mesh=mesh, in_specs=in_specs, out_specs=out_specs, check_vma=False
    )
```

```python
import functools

import jax
import jax.numpy as jnp
from jax import lax
from jax.experimental import pallas as pl
from jax.experimental.pallas import tpu as pltpu
from jax.sharding import PartitionSpec as P

BF16, F32, I16, I32 = jnp.bfloat16, jnp.float32, jnp.int16, jnp.int32
NN = (((1,), (0,)), ((), ()))
NT = (((1,), (1,)), ((), ()))
TN = (((0,), (0,)), ((), ()))
AXES = ("dom", "grp")
DST_BLOCK = 256
SRC_BLOCK = 1024
SEND_MIB, EDGES_MIB, EMBED_MIB, DECODE_MIB, SPREAD_MIB = 8, 24, 24, 16, 24
CHUNK_MIB, FINAL_MIB, WEIGHTS_MIB = 8, 16, 8


def limit(mib):
    return pltpu.CompilerParams(vmem_limit_bytes=mib * 1024 * 1024)


def mm(left, right, dims=NN):
    return lax.dot_general(left, right, dims, preferred_element_type=F32)


def spread_hot(diff, step, count, axis):
    one, zero = jnp.ones((), BF16), jnp.zeros((), BF16)
    pieces = [jnp.where(diff == jnp.int16(step * k), one, zero) for k in range(count)]
    return jnp.concatenate(pieces, axis=axis)


def hot_rows(row, height):
    width = row.shape[1]
    wide = jnp.broadcast_to(row, (16, width)) - lax.broadcasted_iota(I32, (16, width), 0)
    return spread_hot(wide.astype(I16), 16, height // 16, 0)


def hot_tile(tile, width):
    diff = tile - lax.broadcasted_iota(I32, tile.shape, 1)
    return spread_hot(diff.astype(I16), 128, width // 128, 1)


def whole(memory_space=pltpu.VMEM):
    return pl.BlockSpec(memory_space=memory_space)


def shape_of(shape, dtype):
    return jax.ShapeDtypeStruct(shape, dtype)


def cost(flops, moved):
    return pl.CostEstimate(flops=flops, bytes_accessed=moved, transcendentals=0)


def send_body(slot_ref, halo_ref, want_ref, feat_ref, out_ref):
    parts = out_ref.shape[0]
    want = jnp.transpose(want_ref[...])
    tiled = jnp.concatenate([want] * 8, axis=1)
    lane = lax.broadcasted_iota(I32, tiled.shape, 1)
    mine = lax.shift_right_logical(lane, 4) == slot_ref[0]
    tiled = jnp.where(mine, tiled, 0)
    index = jnp.concatenate(
        [lax.shift_right_logical(tiled, 7).astype(F32), (tiled & 127).astype(F32)], axis=1
    )
    halo = halo_ref[...]
    for at in range(0, parts, 16):
        tile = jnp.concatenate(
            [jnp.broadcast_to(halo[:, p : p + 1], (8, 128)) for p in range(at, at + 16)], axis=0
        )
        rows = mm(hot_tile(tile, feat_ref.shape[0]), feat_ref[...])
        rows = rows.reshape(16, 8, rows.shape[1])
        notes = jnp.broadcast_to(index[at : at + 16, None, :], rows.shape)
        out_ref[at : at + 16] = jnp.concatenate([rows, notes], axis=1).astype(BF16)


def send_rows(slot, halo, want, features):
    parts = want.shape[1]
    return pl.pallas_call(
        send_body,
        out_shape=shape_of((parts, 16, features.shape[1]), BF16),
        in_specs=[whole(pltpu.SMEM), whole(), whole(), whole()],
        out_specs=whole(),
        compiler_params=limit(SEND_MIB),
        cost_estimate=cost(10**9, 2 * 10**6),
        name="send_rows",
    )(slot, halo, want, features)


def edges_body(src_blocks, starts_ref, keys_ref, count_ref, degree_ref, held_ref, acc_ref, sem):
    top = keys_ref.shape[0] - 1
    buckets = degree_ref.shape[1] // DST_BLOCK * src_blocks
    degree_ref[...] = jnp.zeros_like(degree_ref)
    ones = (lax.broadcasted_iota(I32, (16, 512), 0) == 0).astype(F32).astype(BF16)

    def block_of(bucket):
        tall = pl.multiple_of(lax.rem(bucket, src_blocks) * SRC_BLOCK, SRC_BLOCK)
        return bucket // src_blocks, pl.ds(tall, SRC_BLOCK)

    def flush(bucket):
        outer, tall = block_of(bucket)
        return pltpu.make_async_copy(held_ref.at[outer, tall], count_ref.at[outer, tall], sem)

    def products(bucket, row):
        wanted = jnp.where(bucket < buckets, bucket, -1)
        src, dst = [], []
        for i in range(4):
            keys = keys_ref[pl.ds(jnp.minimum(row + i, top), 1), :]
            live = jnp.logical_and(lax.shift_right_logical(keys, 18) == wanted, row + i <= top)
            dst.append(jnp.where(live, lax.shift_right_logical(keys, 10) & 255, -1))
            src.append(keys & 1023)
        src, dst = jnp.concatenate(src, axis=1), jnp.concatenate(dst, axis=1)
        right = hot_rows(dst, DST_BLOCK)
        both = mm(jnp.concatenate([hot_rows(src, SRC_BLOCK), ones], axis=0), right, NT)
        return both[:SRC_BLOCK], both[SRC_BLOCK : SRC_BLOCK + 8]

    def store(bucket, fresh, parts, degree):
        last = jnp.minimum(bucket, buckets - 1)
        outer, _ = block_of(last)
        wide = pl.ds(pl.multiple_of(outer * DST_BLOCK, DST_BLOCK), DST_BLOCK)
        base = lax.rem(last, src_blocks) * SRC_BLOCK
        for i in range(SRC_BLOCK // 256):
            rows = slice(i * 256, (i + 1) * 256)
            total = parts[rows] + jnp.where(fresh, 0.0, acc_ref[rows, :])
            acc_ref[rows, :] = total
            tall = pl.ds(pl.multiple_of(base + i * 256, 256), 256)
            held_ref[outer, tall, :] = total.astype(BF16)
        degree_ref[:, wide] += degree

    def advance(bucket, row):
        last = starts_ref[jnp.minimum(bucket + 1, buckets)]
        ended = (row + 4) * 128 >= last
        after = jnp.minimum(bucket + ended.astype(I32), buckets)
        return after, jnp.where(ended, lax.shift_right_logical(starts_ref[after], 7), row + 4), ended

    def body(carry):
        bucket, row, fresh = carry
        bucket1, row1, ended = advance(bucket, row)
        bucket2, row2, ended1 = advance(bucket1, row1)
        first = products(bucket, row)
        second = products(bucket1, row1)
        store(bucket, fresh == 1, *first)
        store(bucket1, jnp.logical_and(ended, bucket1 < buckets), *second)

        @pl.when(ended)
        def _():
            flush(bucket).start()

        @pl.when(jnp.logical_and(ended1, bucket1 < buckets))
        def _():
            flush(bucket1).start()

        return bucket2, row2, ended1.astype(I32)

    start = (jnp.int32(0), lax.shift_right_logical(starts_ref[0], 7), jnp.int32(1))
    lax.while_loop(lambda carry: carry[0] < buckets, body, start)
    pltpu.make_async_copy(held_ref, count_ref, sem).wait()


def edge_counts(starts, keys, nodes, table):
    blocks = nodes // DST_BLOCK
    return pl.pallas_call(
        functools.partial(edges_body, table // SRC_BLOCK),
        out_shape=(pltpu.HBM((blocks, table, DST_BLOCK), BF16), shape_of((8, nodes), F32)),
        in_specs=[whole(pltpu.SMEM), whole()],
        out_specs=(whole(pltpu.HBM), whole()),
        scratch_shapes=[
            pltpu.VMEM((blocks, table, DST_BLOCK), BF16),
            pltpu.VMEM((SRC_BLOCK, DST_BLOCK), F32),
            pltpu.SemaphoreType.DMA,
        ],
        compiler_params=limit(EDGES_MIB),
        cost_estimate=cost(14 * 10**9, 13 * 10**6),
        name="edge_counts",
    )(starts, keys)


def embed_body(
    count_ref, arrived_ref, feat_ref, degree_ref, self_ref, neigh_ref,
    served_ref, agg_ref, want_ref, held_ref, table_ref, emb_ref, sems,
):
    blocks = count_ref.shape[0]
    copies = [pltpu.make_async_copy(count_ref.at[i], held_ref.at[i], sems.at[i]) for i in range(blocks)]
    for copy in copies:
        copy.start()
    nodes = feat_ref.shape[0]
    table_ref[:, :nodes] = jnp.transpose(feat_ref[...])
    arrived = arrived_ref[...].astype(F32)
    halo = arrived[:, :8, :].reshape(-1, arrived.shape[2]).astype(BF16)
    table_ref[:, nodes:] = jnp.transpose(halo)
    notes = arrived[:, 8:, :]
    grouped = notes.reshape(notes.shape[0] // 8, 8, 8, notes.shape[2])
    summed = jnp.sum(grouped, axis=1)[:, 0, :]
    want = (summed[:, :128] * 128.0 + summed[:, 128:]).astype(I32)
    want_ref[...] = want
    columns = jnp.transpose(want)
    for at in range(0, nodes, DST_BLOCK):
        span = slice(at, at + DST_BLOCK)
        copies[at // DST_BLOCK].wait()
        sums = mm(table_ref[...], held_ref[at // DST_BLOCK])
        degree = jnp.sum(degree_ref[:, span], axis=0, keepdims=True)
        mean = (sums / jnp.maximum(degree, 1.0)).astype(BF16)
        mean = jnp.transpose(mean)
        agg_ref[span, :] = mean
        both = mm(feat_ref[span, :], self_ref[...]) + mm(mean, neigh_ref[...])
        emb_ref[span, :] = both.astype(BF16)
    for k in range(0, columns.shape[1], 8):
        tiles = [jnp.broadcast_to(columns[:, i : i + 1], (128, 128)) for i in range(k, k + 8)]
        hot = hot_tile(jnp.concatenate(tiles, axis=0), nodes)
        served_ref[k * 128 : (k + 8) * 128, :] = mm(hot, emb_ref[...]).astype(BF16)


def embed(counts, arrived, features, degree, w_self, w_neigh):
    blocks, table, _ = counts.shape
    nodes, width = features.shape
    return pl.pallas_call(
        embed_body,
        out_shape=(
            shape_of((nodes, width), BF16),
            shape_of((nodes, width), BF16),
            shape_of((16, 128), I32),
        ),
        in_specs=[whole(pltpu.HBM)] + [whole()] * 5,
        out_specs=(whole(),) * 3,
        scratch_shapes=[
            pltpu.VMEM(counts.shape, BF16),
            pltpu.VMEM((width, table), BF16),
            pltpu.VMEM((nodes, width), BF16),
            pltpu.SemaphoreType.DMA((blocks,)),
        ],
        compiler_params=limit(EMBED_MIB),
        cost_estimate=cost(6 * 10**9, 16 * 10**6),
        name="embed",
    )(counts, arrived, features, degree, w_self, w_neigh)


def decode_body(
    got_ref, ends_ref, label_ref, weight_ref, hid_ref, bias_ref, wout_ref,
    logit_ref, send_ref, both_ref, delta_ref, grad_ref, hidden_ref,
):
    rows, width = got_ref.shape
    pairs = ends_ref.shape[1]
    block = 256
    wide = 1024
    meta = jnp.concatenate(
        [
            ends_ref[...].astype(F32),
            label_ref[...].astype(F32),
            weight_ref[...],
            jnp.zeros((4, pairs), F32),
        ],
        axis=0,
    )
    cols = jnp.transpose(meta)
    ends = cols.astype(I32)
    for side in range(2):
        for at in range(0, pairs, wide):
            tile = jnp.broadcast_to(ends[at : at + wide, side : side + 1], (wide, 128))
            picked = mm(hot_tile(tile, rows), got_ref[...])
            both_ref[at : at + wide, side * width : (side + 1) * width] = picked.astype(BF16)
    bias_sum = jnp.zeros((8, width), F32)
    wout_sum = jnp.zeros((8, width), F32)
    for at in range(0, pairs, block):
        span = slice(at, at + block)
        pre = mm(both_ref[span, :], hid_ref[...]) + bias_ref[...]
        hidden = jnp.maximum(pre, 0.0)
        logits = jnp.sum(hidden * wout_ref[...], axis=1, keepdims=True)
        logit_ref[:, span] = jnp.transpose(jnp.broadcast_to(logits, (block, 128)))[0:1, :]
        slope = cols[span, 3:4] * (jax.nn.sigmoid(logits) - cols[span, 2:3])
        delta = jnp.where(pre > 0, slope * wout_ref[...], 0.0)
        bias_sum += jnp.sum(delta.reshape(block // 8, 8, width), axis=0)
        wout_sum += jnp.sum((slope * hidden).reshape(block // 8, 8, width), axis=0)
        delta = delta.astype(BF16)
        delta_ref[span, :] = delta
        grad_ref[span, :] = mm(delta, hid_ref[...], NT).astype(BF16)
    for at in range(0, rows, wide):
        grad = mm(hot_rows(ends_ref[0:1, :] - at, wide), grad_ref[:, :width])
        grad += mm(hot_rows(ends_ref[1:2, :] - at, wide), grad_ref[:, width:])
        send_ref[at // 16 : (at + wide) // 16, 0:16, :] = grad.reshape(-1, 16, width).astype(BF16)
    hidden_ref[...] = mm(both_ref[...], delta_ref[...], TN)
    bias = jnp.sum(bias_sum, axis=0, keepdims=True)
    wout = jnp.sum(wout_sum, axis=0, keepdims=True)
    lines = []
    for line in (bias, wout):
        high = line.astype(BF16).astype(F32)
        for half in (high, line - high):
            lines += [half[:, :128], half[:, 128:]]
    tail = jnp.concatenate(lines, axis=0)
    total = hidden_ref[...].reshape(-1, 8, width)
    tail = jnp.broadcast_to(tail[None], (total.shape[0], 8, 128))
    even = jnp.concatenate([total[:, :, :128], tail], axis=2)
    odd = jnp.concatenate([total[:, :, 128:], tail], axis=2)
    joined = jnp.stack([even, odd], axis=1).reshape(-1, 8, width)
    send_ref[:, 16:24, :] = joined.astype(BF16)


def decode(got, ends, labels, weights, w_hidden, bias, w_out, parts):
    rows, width = got.shape
    pairs = ends.shape[1]
    return pl.pallas_call(
        decode_body,
        out_shape=(shape_of((1, pairs), F32), shape_of((parts, 24, width), BF16)),
        in_specs=[whole()] * 7,
        out_specs=(whole(), whole()),
        scratch_shapes=[
            pltpu.VMEM((pairs, 2 * width), BF16),
            pltpu.VMEM((pairs, width), BF16),
            pltpu.VMEM((pairs, 2 * width), BF16),
            pltpu.VMEM((2 * width, width), F32),
        ],
        compiler_params=limit(DECODE_MIB),
        cost_estimate=cost(10 * 10**9, 4 * 10**6),
        name="decode",
    )(got, ends, labels, weights, w_hidden, bias, w_out)


def spread_body(
    count_ref, back_ref, want_ref, feat_ref, agg_ref, degree_ref, self_ref, neigh_ref,
    send_ref, direct_ref, small_ref, held_ref, grad_ref, mean_ref, sems,
):
    nodes, width = feat_ref.shape
    rows = 1024
    copies = []
    for i in range(count_ref.shape[1] // rows):
        part = (slice(None), slice(i * rows, (i + 1) * rows))
        copies.append(pltpu.make_async_copy(count_ref.at[part], held_ref.at[part], sems.at[i]))
        copies[-1].start()
    back = back_ref[...].astype(F32)
    tail = jnp.sum(back[:, 16:, :], axis=0)
    small_ref[...] = tail[:, 128:]
    flat = back[:, :16, :].reshape(-1, width).astype(BF16)
    want = jnp.concatenate([want_ref[k : k + 1, :] for k in range(16)], axis=1)
    for at in range(0, nodes, 1024):
        grad_ref[at : at + 1024, :] = mm(hot_rows(want - at, 1024), flat).astype(BF16)
    for at in range(0, nodes, 256):
        grad = grad_ref[at : at + 256, :]
        degree = jnp.sum(degree_ref[:, at : at + 256], axis=0, keepdims=True)
        column = jnp.transpose(jnp.broadcast_to(jnp.maximum(degree, 1.0), (128, 256)))
        scaled = mm(grad, neigh_ref[...], NT) / jnp.concatenate([column, column], axis=1)
        mean_ref[at : at + 256, :] = scaled.astype(BF16)
    both = jnp.concatenate(
        [mm(feat_ref[...], grad_ref[...], TN), mm(agg_ref[...], grad_ref[...], TN)], axis=0
    )
    both = both.reshape(-1, 8, width)
    tail = jnp.broadcast_to(tail[None, :, :128], (both.shape[0], 8, 128))
    even = jnp.concatenate([both[:, :, :128], tail], axis=2)
    odd = jnp.concatenate([both[:, :, 128:], tail], axis=2)
    joined = jnp.stack([even, odd], axis=1).reshape(-1, 8, width)
    send_ref[:, 8:16, :] = joined.astype(BF16)

    def table_rows(at):
        copies[at // rows].wait()
        blocks = range(0, nodes, DST_BLOCK)
        parts = [mm(held_ref[n // DST_BLOCK, at : at + rows, :], mean_ref[n : n + DST_BLOCK, :]) for n in blocks]
        return sum(parts[1:], parts[0])

    for at in range(0, nodes, rows):
        grad = mm(grad_ref[at : at + rows, :], self_ref[...], NT)
        direct_ref[at : at + rows, :] = grad + table_rows(at)
    for at in range(0, count_ref.shape[1] - nodes, rows):
        peers = rows // 8
        grad = table_rows(nodes + at).reshape(peers, 8, width)
        send_ref[at // 8 : at // 8 + peers, 0:8, :] = grad.astype(BF16)


def spread(counts, back, want, features, agg, degree, w_self, w_neigh):
    nodes, width = features.shape
    return pl.pallas_call(
        spread_body,
        out_shape=(
            shape_of((back.shape[0], 16, width), BF16),
            pltpu.HBM((nodes, width), F32),
            shape_of((8, 128), F32),
        ),
        in_specs=[whole(pltpu.HBM)] + [whole()] * 7,
        out_specs=(whole(),) * 3,
        scratch_shapes=[
            pltpu.VMEM(counts.shape, BF16),
            pltpu.VMEM((nodes, width), BF16),
            pltpu.VMEM((nodes, width), BF16),
            pltpu.SemaphoreType.DMA((counts.shape[1] // 1024,)),
        ],
        compiler_params=limit(SPREAD_MIB),
        cost_estimate=cost(7 * 10**9, 20 * 10**6),
        name="spread",
    )(counts, back, want, features, agg, degree, w_self, w_neigh)


def chunk_body(back_ref, out_ref):
    tail = jnp.sum(back_ref[:, 8:, :].astype(F32), axis=0)[:, :128]
    out_ref[...] = jnp.broadcast_to(tail[None], out_ref.shape).astype(BF16)


def chunk(back):
    return pl.pallas_call(
        chunk_body,
        out_shape=shape_of((back.shape[0], 8, 128), BF16),
        in_specs=[whole()],
        out_specs=whole(),
        compiler_params=limit(CHUNK_MIB),
        cost_estimate=cost(10**6, 10**6),
        name="chunk",
    )(back)


def join_lanes(pieces):
    pieces = pieces.reshape(-1, 2, 8, 128)
    return jnp.concatenate([pieces[:, 0], pieces[:, 1]], axis=2).reshape(-1, 256)


def final_body(
    direct_ref, back_ref, halo_ref, small_ref, out_ref, hidden_ref, bias_ref, wout_ref, held_ref, sems
):
    rows = 512
    copies = []
    for i in range(out_ref.shape[0] // rows):
        part = slice(i * rows, (i + 1) * rows)
        copies.append(pltpu.make_async_copy(direct_ref.at[part], held_ref.at[part], sems.at[i]))
        copies[-1].start()
    back = back_ref[...].astype(F32)
    width = back.shape[2]
    flat = back[:, :8, :].reshape(-1, width).astype(BF16)
    halo = jnp.concatenate([halo_ref[k : k + 1, :] for k in range(8)], axis=1)
    for i, copy in enumerate(copies):
        part = slice(i * rows, (i + 1) * rows)
        extra = mm(hot_rows(halo - i * rows, rows), flat)
        copy.wait()
        out_ref[part, :] = held_ref[part, :] + extra
    hidden_ref[...] = join_lanes(back[:, 8:, 128:])
    bias_ref[...] = small_ref[0:2, :] + small_ref[2:4, :]
    wout_ref[...] = small_ref[4:6, :] + small_ref[6:8, :]


def final(direct, back, halo, small):
    nodes, width = direct.shape
    return pl.pallas_call(
        final_body,
        out_shape=(
            shape_of((nodes, width), F32),
            shape_of((2 * width, width), F32),
            shape_of((2, 128), F32),
            shape_of((2, 128), F32),
        ),
        in_specs=[whole(pltpu.HBM)] + [whole()] * 3,
        out_specs=(whole(),) * 4,
        scratch_shapes=[
            pltpu.VMEM((nodes, width), F32),
            pltpu.SemaphoreType.DMA((nodes // 512,)),
        ],
        compiler_params=limit(FINAL_MIB),
        cost_estimate=cost(2 * 10**9, 6 * 10**6),
        name="final",
    )(direct, back, halo, small)


def weights_body(pieces_ref, self_ref, neigh_ref):
    both = join_lanes(pieces_ref[...].astype(F32))
    half = both.shape[0] // 2
    self_ref[...] = both[:half, :]
    neigh_ref[...] = both[half:, :]


def weights(pieces):
    shape = shape_of((256, 256), F32)
    return pl.pallas_call(
        weights_body,
        out_shape=(shape, shape),
        in_specs=[whole()],
        out_specs=(whole(), whole()),
        compiler_params=limit(WEIGHTS_MIB),
        cost_estimate=cost(10**6, 10**6),
        name="weights",
    )(pieces)


def exchange(rows):
    return lax.all_to_all(rows, AXES, split_axis=0, concat_axis=0, tiled=True)


def per_device(
    features, edge_src, edge_dst, edge_count, halo_index, request_rows, pair_ends,
    labels, pair_weight, w_self, w_neigh, w_hidden, b_hidden, w_out,
):
    nodes, width = features.shape
    parts, halo_len = halo_index.shape[1:]
    table = nodes + parts * halo_len
    slots = edge_src.shape[0]
    me = lax.axis_index("dom") * lax.axis_size("grp") + lax.axis_index("grp")

    sent = send_rows((me % 8).reshape(1), halo_index[0].T, request_rows[0].T, features)
    arrived = exchange(sent)

    src_blocks = table // SRC_BLOCK
    buckets = nodes // DST_BLOCK * src_blocks
    bucket = edge_dst // DST_BLOCK * src_blocks + edge_src // SRC_BLOCK
    packed = (bucket << 18) | ((edge_dst % DST_BLOCK) << 10) | (edge_src % SRC_BLOCK)
    live = jnp.arange(slots, dtype=I32) < edge_count[0]
    keys = jnp.where(live, packed, buckets << 18)
    bounds = jnp.arange(buckets + 1, dtype=I32) << 18
    starts = jnp.sum((keys[None, :] < bounds[:, None]).astype(I32), axis=1)
    keys = lax.sort(keys, is_stable=False)
    counts, degree = edge_counts(starts, keys.reshape(slots // 128, 128), nodes, table)

    counts = pltpu.with_memory_space_constraint(counts, pltpu.HBM)
    served, agg, want = embed(counts, arrived, features, degree, w_self, w_neigh)
    got = exchange(served.reshape(parts, -1, width)).reshape(-1, width)
    logits, pair_back = decode(
        got, pair_ends.T, labels.reshape(1, -1), pair_weight.reshape(1, -1),
        w_hidden, b_hidden.reshape(1, -1), w_out.reshape(1, -1), parts,
    )
    back = exchange(pair_back)
    halo_back, direct, small = spread(counts, back, want, features, agg, degree, w_self, w_neigh)
    direct = pltpu.with_memory_space_constraint(direct, pltpu.HBM)
    returned = exchange(halo_back)
    pieces = exchange(chunk(returned))
    grad_features, grad_hidden, grad_bias, grad_out = final(
        direct, returned, halo_index[0].reshape(8, -1), small
    )
    grad_self, grad_neigh = weights(pieces)
    return (
        logits.reshape(-1), grad_features, grad_self, grad_neigh, grad_hidden,
        grad_bias.reshape(-1), grad_out.reshape(-1),
    )


def solution(mesh):
    split, rows, cubes = P(AXES), P(AXES, None), P(AXES, None, None)
    in_specs = (
        rows, split, split, split, cubes, cubes, rows, split, split, P(), P(), P(), P(), P(),
    )
    out_specs = (split, rows, P(), P(), P(), P(), P())
    return jax.shard_map(
        per_device, mesh=mesh, in_specs=in_specs, out_specs=out_specs, check_vma=False
    )
```

```python
import functools

import jax
import jax.numpy as jnp
from jax import lax
from jax.experimental import pallas as pl
from jax.experimental.pallas import tpu as pltpu
from jax.sharding import PartitionSpec as P

BF16, F32, I16, I32 = jnp.bfloat16, jnp.float32, jnp.int16, jnp.int32
NN = (((1,), (0,)), ((), ()))
NT = (((1,), (1,)), ((), ()))
TN = (((0,), (0,)), ((), ()))
AXES = ("dom", "grp")
DST_BLOCK = 256
SRC_BLOCK = 256
VISITS = 8
UNROLL = 2
SEND_MIB, EDGES_MIB, EMBED_MIB, DECODE_MIB, SPREAD_MIB = 8, 24, 24, 16, 20
CHUNK_MIB, FINAL_MIB, WEIGHTS_MIB = 8, 16, 8


def limit(mib):
    return pltpu.CompilerParams(vmem_limit_bytes=mib * 1024 * 1024)


def mm(left, right, dims=NN):
    return lax.dot_general(left, right, dims, preferred_element_type=F32)


def spread_hot(diff, step, count, axis):
    one, zero = jnp.ones((), BF16), jnp.zeros((), BF16)
    pieces = [jnp.where(diff == jnp.int16(step * k), one, zero) for k in range(count)]
    return jnp.concatenate(pieces, axis=axis)


def hot_rows(row, height):
    width = row.shape[1]
    wide = jnp.broadcast_to(row, (16, width)) - lax.broadcasted_iota(I32, (16, width), 0)
    return spread_hot(wide.astype(I16), 16, height // 16, 0)


def lane_diff(tile):
    return (tile - lax.broadcasted_iota(I32, tile.shape, 1)).astype(I16)


def hot_lanes(diff, width):
    return spread_hot(diff, 128, width // 128, 1)


def hot_tile(tile, width):
    return hot_lanes(lane_diff(tile), width)


def whole(memory_space=pltpu.VMEM):
    return pl.BlockSpec(memory_space=memory_space)


def shape_of(shape, dtype):
    return jax.ShapeDtypeStruct(shape, dtype)


def cost(flops, moved):
    return pl.CostEstimate(flops=flops, bytes_accessed=moved, transcendentals=0)


def send_body(slot_ref, halo_ref, want_ref, feat_ref, out_ref):
    parts = out_ref.shape[0]
    want = jnp.transpose(want_ref[...])
    tiled = jnp.concatenate([want] * 8, axis=1)
    lane = lax.broadcasted_iota(I32, tiled.shape, 1)
    mine = lax.shift_right_logical(lane, 4) == slot_ref[0]
    tiled = jnp.where(mine, tiled, 0)
    index = jnp.concatenate(
        [lax.shift_right_logical(tiled, 7).astype(F32), (tiled & 127).astype(F32)], axis=1
    )
    halo = halo_ref[...]
    tiles = [jnp.broadcast_to(halo[:, p : p + 1], (8, 128)) for p in range(parts)]
    diff = lane_diff(jnp.concatenate(tiles, axis=0))
    rows = mm(hot_lanes(diff, feat_ref.shape[0]), feat_ref[...])
    rows = rows.reshape(parts, 8, rows.shape[1])
    notes = jnp.broadcast_to(index[:, None, :], rows.shape)
    out_ref[...] = jnp.concatenate([rows, notes], axis=1).astype(BF16)


def send_rows(slot, halo, want, features):
    parts = want.shape[1]
    return pl.pallas_call(
        send_body,
        out_shape=shape_of((parts, 16, features.shape[1]), BF16),
        in_specs=[whole(pltpu.SMEM), whole(), whole(), whole()],
        out_specs=whole(),
        compiler_params=limit(SEND_MIB),
        cost_estimate=cost(10**9, 2 * 10**6),
        name="send_rows",
    )(slot, halo, want, features)


def edges_body(src_blocks, starts_ref, keys_ref, count_ref, degree_ref, held_ref, acc_ref, sem):
    top = keys_ref.shape[0] - 1
    buckets = degree_ref.shape[1] // DST_BLOCK * src_blocks
    degree_ref[...] = jnp.zeros_like(degree_ref)
    ones = (lax.broadcasted_iota(I32, (16, 512), 0) == 0).astype(F32).astype(BF16)

    def block_of(bucket):
        tall = pl.multiple_of(lax.rem(bucket, src_blocks) * SRC_BLOCK, SRC_BLOCK)
        return bucket // src_blocks, pl.ds(tall, SRC_BLOCK)

    def flush(bucket):
        outer, tall = block_of(bucket)
        return pltpu.make_async_copy(held_ref.at[outer, tall], count_ref.at[outer, tall], sem)

    def products(bucket, row):
        wanted = jnp.where(bucket < buckets, bucket, -1)
        src, dst = [], []
        for i in range(4):
            keys = keys_ref[pl.ds(jnp.minimum(row + i, top), 1), :]
            live = jnp.logical_and(lax.shift_right_logical(keys, 18) == wanted, row + i <= top)
            dst.append(jnp.where(live, lax.shift_right_logical(keys, 10) & 255, -1))
            src.append(keys & 1023)
        src, dst = jnp.concatenate(src, axis=1), jnp.concatenate(dst, axis=1)
        right = hot_rows(dst, DST_BLOCK)
        both = mm(jnp.concatenate([hot_rows(src, SRC_BLOCK), ones], axis=0), right, NT)
        return both[:SRC_BLOCK], both[SRC_BLOCK : SRC_BLOCK + 8]

    def store(bucket, fresh, parts, degree):
        last = jnp.minimum(bucket, buckets - 1)
        outer, _ = block_of(last)
        wide = pl.ds(pl.multiple_of(outer * DST_BLOCK, DST_BLOCK), DST_BLOCK)
        base = lax.rem(last, src_blocks) * SRC_BLOCK
        for i in range(SRC_BLOCK // 256):
            rows = slice(i * 256, (i + 1) * 256)
            total = parts[rows] + jnp.where(fresh, 0.0, acc_ref[rows, :])
            acc_ref[rows, :] = total
            tall = pl.ds(pl.multiple_of(base + i * 256, 256), 256)
            held_ref[outer, tall, :] = total.astype(BF16)
        degree_ref[:, wide] += degree

    def advance(bucket, row):
        last = starts_ref[jnp.minimum(bucket + 1, buckets)]
        ended = (row + 4) * 128 >= last
        after = jnp.minimum(bucket + ended.astype(I32), buckets)
        return after, jnp.where(ended, lax.shift_right_logical(starts_ref[after], 7), row + 4), ended

    def body(carry):
        bucket, row, fresh = carry
        visits = []
        for _ in range(VISITS):
            after, following, ended = advance(bucket, row)
            visits.append((bucket, row, fresh == 1, ended))
            bucket, row = after, following
            fresh = jnp.logical_and(ended, bucket < buckets).astype(I32)
        made = [products(*visit[:2]) for visit in visits]
        for visit, both in zip(visits, made):
            store(visit[0], visit[2], *both)
        for visit in visits:
            @pl.when(jnp.logical_and(visit[3], visit[0] < buckets))
            def _(visit=visit):
                flush(visit[0]).start()

        return bucket, row, fresh

    start = (jnp.int32(0), lax.shift_right_logical(starts_ref[0], 7), jnp.int32(1))
    lax.while_loop(lambda carry: carry[0] < buckets, body, start)
    pltpu.make_async_copy(held_ref, count_ref, sem).wait()


def edge_counts(starts, keys, nodes, table):
    blocks = nodes // DST_BLOCK
    return pl.pallas_call(
        functools.partial(edges_body, table // SRC_BLOCK),
        out_shape=(pltpu.HBM((blocks, table, DST_BLOCK), BF16), shape_of((8, nodes), F32)),
        in_specs=[whole(pltpu.SMEM), whole()],
        out_specs=(whole(pltpu.HBM), whole()),
        scratch_shapes=[
            pltpu.VMEM((blocks, table, DST_BLOCK), BF16),
            pltpu.VMEM((SRC_BLOCK, DST_BLOCK), F32),
            pltpu.SemaphoreType.DMA,
        ],
        compiler_params=limit(EDGES_MIB),
        cost_estimate=cost(14 * 10**9, 13 * 10**6),
        name="edge_counts",
    )(starts, keys)


def embed_body(
    count_ref, arrived_ref, feat_ref, degree_ref, self_ref, neigh_ref,
    served_ref, agg_ref, want_ref, held_ref, table_ref, emb_ref, sems,
):
    blocks = count_ref.shape[0]
    copies = [pltpu.make_async_copy(count_ref.at[i], held_ref.at[i], sems.at[i]) for i in range(blocks)]
    for copy in copies:
        copy.start()
    nodes = feat_ref.shape[0]
    table_ref[:, :nodes] = jnp.transpose(feat_ref[...])
    arrived = arrived_ref[...].astype(F32)
    halo = arrived[:, :8, :].reshape(-1, arrived.shape[2]).astype(BF16)
    table_ref[:, nodes:] = jnp.transpose(halo)
    notes = arrived[:, 8:, :]
    grouped = notes.reshape(notes.shape[0] // 8, 8, 8, notes.shape[2])
    summed = jnp.sum(grouped, axis=1)[:, 0, :]
    want = (summed[:, :128] * 128.0 + summed[:, 128:]).astype(I32)
    want_ref[...] = want
    columns = jnp.transpose(want)
    def node_block(i, carry):
        span = pl.ds(pl.multiple_of(i * DST_BLOCK, DST_BLOCK), DST_BLOCK)
        pltpu.make_async_copy(count_ref.at[i], held_ref.at[i], sems.at[i]).wait()
        sums = mm(table_ref[...], held_ref[i])
        degree = jnp.sum(degree_ref[:, span], axis=0, keepdims=True)
        mean = (sums / jnp.maximum(degree, 1.0)).astype(BF16)
        mean = jnp.transpose(mean)
        agg_ref[span, :] = mean
        both = mm(feat_ref[span, :], self_ref[...]) + mm(mean, neigh_ref[...])
        emb_ref[span, :] = both.astype(BF16)
        return carry

    lax.fori_loop(0, nodes // DST_BLOCK, node_block, 0)
    for k in range(0, columns.shape[1], 8):
        tiles = [jnp.broadcast_to(columns[:, i : i + 1], (128, 128)) for i in range(k, k + 8)]
        hot = hot_tile(jnp.concatenate(tiles, axis=0), nodes)
        served_ref[k * 128 : (k + 8) * 128, :] = mm(hot, emb_ref[...]).astype(BF16)


def embed(counts, arrived, features, degree, w_self, w_neigh):
    blocks, table, _ = counts.shape
    nodes, width = features.shape
    return pl.pallas_call(
        embed_body,
        out_shape=(
            shape_of((nodes, width), BF16),
            shape_of((nodes, width), BF16),
            shape_of((16, 128), I32),
        ),
        in_specs=[whole(pltpu.HBM)] + [whole()] * 5,
        out_specs=(whole(),) * 3,
        scratch_shapes=[
            pltpu.VMEM(counts.shape, BF16),
            pltpu.VMEM((width, table), BF16),
            pltpu.VMEM((nodes, width), BF16),
            pltpu.SemaphoreType.DMA((blocks,)),
        ],
        compiler_params=limit(EMBED_MIB),
        cost_estimate=cost(6 * 10**9, 16 * 10**6),
        name="embed",
    )(counts, arrived, features, degree, w_self, w_neigh)


def decode_body(
    got_ref, ends_ref, label_ref, weight_ref, hid_ref, bias_ref, wout_ref,
    logit_ref, send_ref, both_ref, delta_ref, grad_ref, hidden_ref,
):
    rows, width = got_ref.shape
    pairs = ends_ref.shape[1]
    block = 256
    wide = 1024
    meta = jnp.concatenate(
        [
            ends_ref[...].astype(F32),
            label_ref[...].astype(F32),
            weight_ref[...],
            jnp.zeros((4, pairs), F32),
        ],
        axis=0,
    )
    cols = jnp.transpose(meta)
    ends = cols.astype(I32)
    for side in range(2):
        for at in range(0, pairs, wide):
            tile = jnp.broadcast_to(ends[at : at + wide, side : side + 1], (wide, 128))
            picked = mm(hot_tile(tile, rows), got_ref[...])
            both_ref[at : at + wide, side * width : (side + 1) * width] = picked.astype(BF16)
    bias_sum = jnp.zeros((8, width), F32)
    wout_sum = jnp.zeros((8, width), F32)
    for at in range(0, pairs, block):
        span = slice(at, at + block)
        pre = mm(both_ref[span, :], hid_ref[...]) + bias_ref[...]
        hidden = jnp.maximum(pre, 0.0)
        logits = jnp.sum(hidden * wout_ref[...], axis=1, keepdims=True)
        logit_ref[:, span] = jnp.transpose(jnp.broadcast_to(logits, (block, 128)))[0:1, :]
        slope = cols[span, 3:4] * (jax.nn.sigmoid(logits) - cols[span, 2:3])
        delta = jnp.where(pre > 0, slope * wout_ref[...], 0.0)
        bias_sum += jnp.sum(delta.reshape(block // 8, 8, width), axis=0)
        wout_sum += jnp.sum((slope * hidden).reshape(block // 8, 8, width), axis=0)
        delta = delta.astype(BF16)
        delta_ref[span, :] = delta
        grad_ref[span, :] = mm(delta, hid_ref[...], NT).astype(BF16)
    for at in range(0, rows, wide):
        grad = mm(hot_rows(ends_ref[0:1, :] - at, wide), grad_ref[:, :width])
        grad += mm(hot_rows(ends_ref[1:2, :] - at, wide), grad_ref[:, width:])
        send_ref[at // 16 : (at + wide) // 16, 0:16, :] = grad.reshape(-1, 16, width).astype(BF16)
    hidden_ref[...] = mm(both_ref[...], delta_ref[...], TN)
    bias = jnp.sum(bias_sum, axis=0, keepdims=True)
    wout = jnp.sum(wout_sum, axis=0, keepdims=True)
    lines = []
    for line in (bias, wout):
        high = line.astype(BF16).astype(F32)
        for half in (high, line - high):
            lines += [half[:, :128], half[:, 128:]]
    tail = jnp.concatenate(lines, axis=0)
    total = hidden_ref[...].reshape(-1, 8, width)
    tail = jnp.broadcast_to(tail[None], (total.shape[0], 8, 128))
    even = jnp.concatenate([total[:, :, :128], tail], axis=2)
    odd = jnp.concatenate([total[:, :, 128:], tail], axis=2)
    joined = jnp.stack([even, odd], axis=1).reshape(-1, 8, width)
    send_ref[:, 16:24, :] = joined.astype(BF16)


def decode(got, ends, labels, weights, w_hidden, bias, w_out, parts):
    rows, width = got.shape
    pairs = ends.shape[1]
    return pl.pallas_call(
        decode_body,
        out_shape=(shape_of((1, pairs), F32), shape_of((parts, 24, width), BF16)),
        in_specs=[whole()] * 7,
        out_specs=(whole(), whole()),
        scratch_shapes=[
            pltpu.VMEM((pairs, 2 * width), BF16),
            pltpu.VMEM((pairs, width), BF16),
            pltpu.VMEM((pairs, 2 * width), BF16),
            pltpu.VMEM((2 * width, width), F32),
        ],
        compiler_params=limit(DECODE_MIB),
        cost_estimate=cost(10 * 10**9, 4 * 10**6),
        name="decode",
    )(got, ends, labels, weights, w_hidden, bias, w_out)


def spread_body(
    count_ref, back_ref, want_ref, feat_ref, agg_ref, degree_ref, self_ref, neigh_ref,
    send_ref, direct_ref, small_ref, grad_ref, mean_ref,
):
    nodes, width = feat_ref.shape
    rows = 1024
    back = back_ref[...].astype(F32)
    tail = jnp.sum(back[:, 16:, :], axis=0)
    small_ref[...] = tail[:, 128:]
    flat = back[:, :16, :].reshape(-1, width).astype(BF16)
    want = jnp.concatenate([want_ref[k : k + 1, :] for k in range(16)], axis=1)

    def gather(i, carry):
        at = i * rows
        span = pl.ds(pl.multiple_of(at, rows), rows)
        grad_ref[span, :] = mm(hot_rows(want - at, rows), flat).astype(BF16)
        return carry

    lax.fori_loop(0, nodes // rows, gather, 0)

    def scale(i, carry):
        span = pl.ds(pl.multiple_of(i * 256, 256), 256)
        degree = jnp.sum(degree_ref[:, span], axis=0, keepdims=True)
        column = jnp.transpose(jnp.broadcast_to(jnp.maximum(degree, 1.0), (128, 256)))
        scaled = mm(grad_ref[span, :], neigh_ref[...], NT) / jnp.concatenate([column, column], axis=1)
        mean_ref[span, :] = scaled.astype(BF16)
        return carry

    lax.fori_loop(0, nodes // 256, scale, 0, unroll=UNROLL)
    both = jnp.concatenate(
        [mm(feat_ref[...], grad_ref[...], TN), mm(agg_ref[...], grad_ref[...], TN)], axis=0
    )
    both = both.reshape(-1, 8, width)
    tail = jnp.broadcast_to(tail[None, :, :128], (both.shape[0], 8, 128))
    even = jnp.concatenate([both[:, :, :128], tail], axis=2)
    odd = jnp.concatenate([both[:, :, 128:], tail], axis=2)
    joined = jnp.stack([even, odd], axis=1).reshape(-1, 8, width)
    send_ref[:, 8:16, :] = joined.astype(BF16)

    def table_rows(at):
        blocks = range(0, nodes, DST_BLOCK)
        span = pl.ds(pl.multiple_of(at, rows), rows)
        parts = [mm(count_ref[n // DST_BLOCK, span, :], mean_ref[n : n + DST_BLOCK, :]) for n in blocks]
        return sum(parts[1:], parts[0])

    def own(i, carry):
        span = pl.ds(pl.multiple_of(i * rows, rows), rows)
        direct_ref[span, :] = mm(grad_ref[span, :], self_ref[...], NT) + table_rows(i * rows)
        return carry

    lax.fori_loop(0, nodes // rows, own, 0)
    for at in range(0, count_ref.shape[1] - nodes, rows):
        peers = rows // 8
        grad = table_rows(nodes + at).reshape(peers, 8, width)
        send_ref[at // 8 : at // 8 + peers, 0:8, :] = grad.astype(BF16)


def spread(counts, back, want, features, agg, degree, w_self, w_neigh):
    nodes, width = features.shape
    return pl.pallas_call(
        spread_body,
        out_shape=(
            shape_of((back.shape[0], 16, width), BF16),
            pltpu.HBM((nodes, width), F32),
            shape_of((8, 128), F32),
        ),
        in_specs=[whole()] * 8,
        out_specs=(whole(),) * 3,
        scratch_shapes=[pltpu.VMEM((nodes, width), BF16), pltpu.VMEM((nodes, width), BF16)],
        compiler_params=limit(SPREAD_MIB),
        cost_estimate=cost(7 * 10**9, 20 * 10**6),
        name="spread",
    )(counts, back, want, features, agg, degree, w_self, w_neigh)


def chunk_body(back_ref, out_ref):
    tail = jnp.sum(back_ref[:, 8:, :].astype(F32), axis=0)[:, :128]
    out_ref[...] = jnp.broadcast_to(tail[None], out_ref.shape).astype(BF16)


def chunk(back):
    return pl.pallas_call(
        chunk_body,
        out_shape=shape_of((back.shape[0], 8, 128), BF16),
        in_specs=[whole()],
        out_specs=whole(),
        compiler_params=limit(CHUNK_MIB),
        cost_estimate=cost(10**6, 10**6),
        name="chunk",
    )(back)


def join_lanes(pieces):
    pieces = pieces.reshape(-1, 2, 8, 128)
    return jnp.concatenate([pieces[:, 0], pieces[:, 1]], axis=2).reshape(-1, 256)


def final_body(
    direct_ref, back_ref, halo_ref, small_ref, out_ref, hidden_ref, bias_ref, wout_ref, held_ref, sems
):
    rows = 512
    copies = []
    for i in range(out_ref.shape[0] // rows):
        part = slice(i * rows, (i + 1) * rows)
        copies.append(pltpu.make_async_copy(direct_ref.at[part], held_ref.at[part], sems.at[i]))
        copies[-1].start()
    back = back_ref[...].astype(F32)
    width = back.shape[2]
    flat = back[:, :8, :].reshape(-1, width).astype(BF16)
    halo = jnp.concatenate([halo_ref[k : k + 1, :] for k in range(8)], axis=1)

    def add(i, carry):
        part = pl.ds(pl.multiple_of(i * rows, rows), rows)
        extra = mm(hot_rows(halo - i * rows, rows), flat)
        pltpu.make_async_copy(direct_ref.at[part], held_ref.at[part], sems.at[i]).wait()
        out_ref[part, :] = held_ref[part, :] + extra
        return carry

    lax.fori_loop(0, len(copies), add, 0)
    hidden_ref[...] = join_lanes(back[:, 8:, 128:])
    bias_ref[...] = small_ref[0:2, :] + small_ref[2:4, :]
    wout_ref[...] = small_ref[4:6, :] + small_ref[6:8, :]


def final(direct, back, halo, small):
    nodes, width = direct.shape
    return pl.pallas_call(
        final_body,
        out_shape=(
            shape_of((nodes, width), F32),
            shape_of((2 * width, width), F32),
            shape_of((2, 128), F32),
            shape_of((2, 128), F32),
        ),
        in_specs=[whole(pltpu.HBM)] + [whole()] * 3,
        out_specs=(whole(),) * 4,
        scratch_shapes=[
            pltpu.VMEM((nodes, width), F32),
            pltpu.SemaphoreType.DMA((nodes // 512,)),
        ],
        compiler_params=limit(FINAL_MIB),
        cost_estimate=cost(2 * 10**9, 6 * 10**6),
        name="final",
    )(direct, back, halo, small)


def weights_body(pieces_ref, self_ref, neigh_ref):
    both = join_lanes(pieces_ref[...].astype(F32))
    half = both.shape[0] // 2
    self_ref[...] = both[:half, :]
    neigh_ref[...] = both[half:, :]


def weights(pieces):
    shape = shape_of((256, 256), F32)
    return pl.pallas_call(
        weights_body,
        out_shape=(shape, shape),
        in_specs=[whole()],
        out_specs=(whole(), whole()),
        compiler_params=limit(WEIGHTS_MIB),
        cost_estimate=cost(10**6, 10**6),
        name="weights",
    )(pieces)


def exchange(rows):
    return lax.all_to_all(rows, AXES, split_axis=0, concat_axis=0, tiled=True)


def per_device(
    features, edge_src, edge_dst, edge_count, halo_index, request_rows, pair_ends,
    labels, pair_weight, w_self, w_neigh, w_hidden, b_hidden, w_out,
):
    nodes, width = features.shape
    parts, halo_len = halo_index.shape[1:]
    table = nodes + parts * halo_len
    slots = edge_src.shape[0]
    me = lax.axis_index("dom") * lax.axis_size("grp") + lax.axis_index("grp")

    sent = send_rows((me % 8).reshape(1), halo_index[0].T, request_rows[0].T, features)
    arrived = exchange(sent)

    src_blocks = table // SRC_BLOCK
    buckets = nodes // DST_BLOCK * src_blocks
    bucket = edge_dst // DST_BLOCK * src_blocks + edge_src // SRC_BLOCK
    packed = (bucket << 18) | ((edge_dst % DST_BLOCK) << 10) | (edge_src % SRC_BLOCK)
    live = jnp.arange(slots, dtype=I32) < edge_count[0]
    keys = jnp.where(live, packed, buckets << 18)
    bounds = jnp.arange(buckets + 1, dtype=I32) << 18
    starts = jnp.sum((keys[None, :] < bounds[:, None]).astype(I32), axis=1)
    keys = lax.sort(keys, is_stable=False)
    counts, degree = edge_counts(starts, keys.reshape(slots // 128, 128), nodes, table)

    fixed = pltpu.with_memory_space_constraint(counts, pltpu.HBM)
    served, agg, want = embed(fixed, arrived, features, degree, w_self, w_neigh)
    got = exchange(served.reshape(parts, -1, width)).reshape(-1, width)
    logits, pair_back = decode(
        got, pair_ends.T, labels.reshape(1, -1), pair_weight.reshape(1, -1),
        w_hidden, b_hidden.reshape(1, -1), w_out.reshape(1, -1), parts,
    )
    back = exchange(pair_back)
    halo_back, direct, small = spread(counts, back, want, features, agg, degree, w_self, w_neigh)
    direct = pltpu.with_memory_space_constraint(direct, pltpu.HBM)
    returned = exchange(halo_back)
    pieces = exchange(chunk(returned))
    grad_features, grad_hidden, grad_bias, grad_out = final(
        direct, returned, halo_index[0].reshape(8, -1), small
    )
    grad_self, grad_neigh = weights(pieces)
    return (
        logits.reshape(-1), grad_features, grad_self, grad_neigh, grad_hidden,
        grad_bias.reshape(-1), grad_out.reshape(-1),
    )


def solution(mesh):
    split, rows, cubes = P(AXES), P(AXES, None), P(AXES, None, None)
    in_specs = (
        rows, split, split, split, cubes, cubes, rows, split, split, P(), P(), P(), P(), P(),
    )
    out_specs = (split, rows, P(), P(), P(), P(), P())
    return jax.shard_map(
        per_device, mesh=mesh, in_specs=in_specs, out_specs=out_specs, check_vma=False
    )
```

```python
import functools

import jax
import jax.numpy as jnp
from jax import lax
from jax.experimental import pallas as pl
from jax.experimental.pallas import tpu as pltpu
from jax.sharding import PartitionSpec as P

BF16, F32, I16, I32 = jnp.bfloat16, jnp.float32, jnp.int16, jnp.int32
NN = (((1,), (0,)), ((), ()))
NT = (((1,), (1,)), ((), ()))
TN = (((0,), (0,)), ((), ()))
AXES = ("dom", "grp")
DST_BLOCK = 256
SRC_BLOCK = 256
VISITS = 8
UNROLL = 2
SEND_MIB, EDGES_MIB, EMBED_MIB, DECODE_MIB, SPREAD_MIB = 8, 24, 24, 16, 16
DIRECT_MIB = 16
CHUNK_MIB, FINAL_MIB, WEIGHTS_MIB = 8, 16, 8


def limit(mib):
    return pltpu.CompilerParams(vmem_limit_bytes=mib * 1024 * 1024)


def mm(left, right, dims=NN):
    return lax.dot_general(left, right, dims, preferred_element_type=F32)


def spread_hot(diff, step, count, axis):
    one, zero = jnp.ones((), BF16), jnp.zeros((), BF16)
    pieces = [jnp.where(diff == jnp.int16(step * k), one, zero) for k in range(count)]
    return jnp.concatenate(pieces, axis=axis)


def hot_rows(row, height):
    width = row.shape[1]
    wide = jnp.broadcast_to(row, (16, width)) - lax.broadcasted_iota(I32, (16, width), 0)
    return spread_hot(wide.astype(I16), 16, height // 16, 0)


def lane_diff(tile):
    return (tile - lax.broadcasted_iota(I32, tile.shape, 1)).astype(I16)


def hot_lanes(diff, width):
    return spread_hot(diff, 128, width // 128, 1)


def hot_tile(tile, width):
    return hot_lanes(lane_diff(tile), width)


def whole(memory_space=pltpu.VMEM):
    return pl.BlockSpec(memory_space=memory_space)


def shape_of(shape, dtype):
    return jax.ShapeDtypeStruct(shape, dtype)


def cost(flops, moved):
    return pl.CostEstimate(flops=flops, bytes_accessed=moved, transcendentals=0)


def send_body(slot_ref, halo_hbm, want_hbm, feat_hbm, out_ref, halo_ref, want_ref, feat_ref, sems):
    pairs = ((halo_hbm, halo_ref), (want_hbm, want_ref), (feat_hbm, feat_ref))
    copies = [pltpu.make_async_copy(*pair, sems.at[i]) for i, pair in enumerate(pairs)]
    for copy in copies:
        copy.start()
    copies[0].wait()
    copies[1].wait()
    parts = out_ref.shape[0]
    want = jnp.transpose(want_ref[...])
    tiled = jnp.concatenate([want] * 8, axis=1)
    lane = lax.broadcasted_iota(I32, tiled.shape, 1)
    mine = lax.shift_right_logical(lane, 4) == slot_ref[0]
    tiled = jnp.where(mine, tiled, 0)
    index = jnp.concatenate(
        [lax.shift_right_logical(tiled, 7).astype(F32), (tiled & 127).astype(F32)], axis=1
    )
    halo = halo_ref[...]
    tiles = [jnp.broadcast_to(halo[:, p : p + 1], (8, 128)) for p in range(parts)]
    diff = lane_diff(jnp.concatenate(tiles, axis=0))
    copies[2].wait()
    rows = mm(hot_lanes(diff, feat_ref.shape[0]), feat_ref[...])
    rows = rows.reshape(parts, 8, rows.shape[1])
    notes = jnp.broadcast_to(index[:, None, :], rows.shape)
    out_ref[...] = jnp.concatenate([rows, notes], axis=1).astype(BF16)


def send_rows(slot, halo, want, features):
    parts = want.shape[1]
    return pl.pallas_call(
        send_body,
        out_shape=shape_of((parts, 16, features.shape[1]), BF16),
        in_specs=[whole(pltpu.SMEM)] + [whole(pltpu.HBM)] * 3,
        out_specs=whole(),
        scratch_shapes=[
            pltpu.VMEM(halo.shape, I32),
            pltpu.VMEM(want.shape, I32),
            pltpu.VMEM(features.shape, BF16),
            pltpu.SemaphoreType.DMA((3,)),
        ],
        compiler_params=limit(SEND_MIB),
        cost_estimate=cost(10**9, 2 * 10**6),
        name="send_rows",
    )(slot, halo, want, features)


def edges_body(src_blocks, starts_ref, keys_ref, count_ref, degree_ref, held_ref, acc_ref, sem):
    top = keys_ref.shape[0] - 1
    buckets = degree_ref.shape[1] // DST_BLOCK * src_blocks
    degree_ref[...] = jnp.zeros_like(degree_ref)
    ones = (lax.broadcasted_iota(I32, (16, 512), 0) == 0).astype(F32).astype(BF16)

    def block_of(bucket):
        tall = pl.multiple_of(lax.rem(bucket, src_blocks) * SRC_BLOCK, SRC_BLOCK)
        return bucket // src_blocks, pl.ds(tall, SRC_BLOCK)

    def flush(bucket):
        outer, tall = block_of(bucket)
        return pltpu.make_async_copy(held_ref.at[outer, tall], count_ref.at[outer, tall], sem)

    def products(bucket, row):
        wanted = jnp.where(bucket < buckets, bucket, -1)
        src, dst = [], []
        for i in range(4):
            keys = keys_ref[pl.ds(jnp.minimum(row + i, top), 1), :]
            live = jnp.logical_and(lax.shift_right_logical(keys, 18) == wanted, row + i <= top)
            dst.append(jnp.where(live, lax.shift_right_logical(keys, 10) & 255, -1))
            src.append(keys & 1023)
        src, dst = jnp.concatenate(src, axis=1), jnp.concatenate(dst, axis=1)
        right = hot_rows(dst, DST_BLOCK)
        both = mm(jnp.concatenate([hot_rows(src, SRC_BLOCK), ones], axis=0), right, NT)
        return both[:SRC_BLOCK], both[SRC_BLOCK : SRC_BLOCK + 8]

    def store(bucket, fresh, parts, degree):
        last = jnp.minimum(bucket, buckets - 1)
        outer, _ = block_of(last)
        wide = pl.ds(pl.multiple_of(outer * DST_BLOCK, DST_BLOCK), DST_BLOCK)
        base = lax.rem(last, src_blocks) * SRC_BLOCK
        for i in range(SRC_BLOCK // 256):
            rows = slice(i * 256, (i + 1) * 256)
            total = parts[rows] + jnp.where(fresh, 0.0, acc_ref[rows, :])
            acc_ref[rows, :] = total
            tall = pl.ds(pl.multiple_of(base + i * 256, 256), 256)
            held_ref[outer, tall, :] = total.astype(BF16)
        degree_ref[:, wide] += degree

    def advance(bucket, row):
        last = starts_ref[jnp.minimum(bucket + 1, buckets)]
        ended = (row + 4) * 128 >= last
        after = jnp.minimum(bucket + ended.astype(I32), buckets)
        return after, jnp.where(ended, lax.shift_right_logical(starts_ref[after], 7), row + 4), ended

    def body(carry):
        bucket, row, fresh = carry
        visits = []
        for _ in range(VISITS):
            after, following, ended = advance(bucket, row)
            visits.append((bucket, row, fresh == 1, ended))
            bucket, row = after, following
            fresh = jnp.logical_and(ended, bucket < buckets).astype(I32)
        made = [products(*visit[:2]) for visit in visits]
        for visit, both in zip(visits, made):
            store(visit[0], visit[2], *both)
        for visit in visits:
            @pl.when(jnp.logical_and(visit[3], visit[0] < buckets))
            def _(visit=visit):
                flush(visit[0]).start()

        return bucket, row, fresh

    start = (jnp.int32(0), lax.shift_right_logical(starts_ref[0], 7), jnp.int32(1))
    lax.while_loop(lambda carry: carry[0] < buckets, body, start)
    pltpu.make_async_copy(held_ref, count_ref, sem).wait()


def edge_counts(starts, keys, nodes, table):
    blocks = nodes // DST_BLOCK
    return pl.pallas_call(
        functools.partial(edges_body, table // SRC_BLOCK),
        out_shape=(pltpu.HBM((blocks, table, DST_BLOCK), BF16), shape_of((8, nodes), F32)),
        in_specs=[whole(pltpu.SMEM), whole()],
        out_specs=(whole(pltpu.HBM), whole()),
        scratch_shapes=[
            pltpu.VMEM((blocks, table, DST_BLOCK), BF16),
            pltpu.VMEM((SRC_BLOCK, DST_BLOCK), F32),
            pltpu.SemaphoreType.DMA,
        ],
        compiler_params=limit(EDGES_MIB),
        cost_estimate=cost(14 * 10**9, 13 * 10**6),
        name="edge_counts",
    )(starts, keys)


def embed_body(
    count_ref, arrived_ref, feat_ref, degree_ref, self_ref, neigh_ref,
    served_ref, agg_ref, want_ref, held_ref, table_ref, mean_ref, emb_ref, sems,
):
    blocks = count_ref.shape[0]
    copies = [pltpu.make_async_copy(count_ref.at[i], held_ref.at[i], sems.at[i]) for i in range(blocks)]
    for copy in copies:
        copy.start()
    nodes = feat_ref.shape[0]
    table_ref[:, :nodes] = jnp.transpose(feat_ref[...])
    arrived = arrived_ref[...].astype(F32)
    halo = arrived[:, :8, :].reshape(-1, arrived.shape[2]).astype(BF16)
    table_ref[:, nodes:] = jnp.transpose(halo)
    notes = arrived[:, 8:, :]
    grouped = notes.reshape(notes.shape[0] // 8, 8, 8, notes.shape[2])
    summed = jnp.sum(grouped, axis=1)[:, 0, :]
    want = (summed[:, :128] * 128.0 + summed[:, 128:]).astype(I32)
    want_ref[...] = want
    columns = jnp.transpose(want)
    def node_block(i, carry):
        span = pl.ds(pl.multiple_of(i * DST_BLOCK, DST_BLOCK), DST_BLOCK)
        pltpu.make_async_copy(count_ref.at[i], held_ref.at[i], sems.at[i]).wait()
        sums = mm(table_ref[...], held_ref[i])
        degree = jnp.sum(degree_ref[:, span], axis=0, keepdims=True)
        mean_ref[:, span] = (sums / jnp.maximum(degree, 1.0)).astype(BF16)
        return carry

    lax.fori_loop(0, nodes // DST_BLOCK, node_block, 0)
    agg_ref[...] = jnp.transpose(mean_ref[...])
    for at in range(0, nodes, 1024):
        span = slice(at, at + 1024)
        both = mm(feat_ref[span, :], self_ref[...]) + mm(agg_ref[span, :], neigh_ref[...])
        emb_ref[span, :] = both.astype(BF16)
    for k in range(0, columns.shape[1], 8):
        tiles = [jnp.broadcast_to(columns[:, i : i + 1], (128, 128)) for i in range(k, k + 8)]
        hot = hot_tile(jnp.concatenate(tiles, axis=0), nodes)
        served_ref[k * 128 : (k + 8) * 128, :] = mm(hot, emb_ref[...]).astype(BF16)


def embed(counts, arrived, features, degree, w_self, w_neigh):
    blocks, table, _ = counts.shape
    nodes, width = features.shape
    return pl.pallas_call(
        embed_body,
        out_shape=(
            shape_of((nodes, width), BF16),
            shape_of((nodes, width), BF16),
            shape_of((16, 128), I32),
        ),
        in_specs=[whole(pltpu.HBM)] + [whole()] * 5,
        out_specs=(whole(),) * 3,
        scratch_shapes=[
            pltpu.VMEM(counts.shape, BF16),
            pltpu.VMEM((width, table), BF16),
            pltpu.VMEM((width, nodes), BF16),
            pltpu.VMEM((nodes, width), BF16),
            pltpu.SemaphoreType.DMA((blocks,)),
        ],
        compiler_params=limit(EMBED_MIB),
        cost_estimate=cost(6 * 10**9, 16 * 10**6),
        name="embed",
    )(counts, arrived, features, degree, w_self, w_neigh)


def decode_body(
    got_ref, ends_ref, label_ref, weight_ref, hid_ref, bias_ref, wout_ref,
    logit_ref, send_ref, both_ref, delta_ref, grad_ref, hidden_ref,
):
    rows, width = got_ref.shape
    pairs = ends_ref.shape[1]
    block = 256
    wide = 1024
    meta = jnp.concatenate(
        [
            ends_ref[...].astype(F32),
            label_ref[...].astype(F32),
            weight_ref[...],
            jnp.zeros((4, pairs), F32),
        ],
        axis=0,
    )
    cols = jnp.transpose(meta)
    ends = cols.astype(I32)
    for side in range(2):
        for at in range(0, pairs, wide):
            tile = jnp.broadcast_to(ends[at : at + wide, side : side + 1], (wide, 128))
            picked = mm(hot_tile(tile, rows), got_ref[...])
            both_ref[at : at + wide, side * width : (side + 1) * width] = picked.astype(BF16)
    bias_sum = jnp.zeros((8, width), F32)
    wout_sum = jnp.zeros((8, width), F32)
    for at in range(0, pairs, block):
        span = slice(at, at + block)
        pre = mm(both_ref[span, :], hid_ref[...]) + bias_ref[...]
        hidden = jnp.maximum(pre, 0.0)
        logits = jnp.sum(hidden * wout_ref[...], axis=1, keepdims=True)
        logit_ref[:, span] = jnp.transpose(jnp.broadcast_to(logits, (block, 128)))[0:1, :]
        slope = cols[span, 3:4] * (jax.nn.sigmoid(logits) - cols[span, 2:3])
        delta = jnp.where(pre > 0, slope * wout_ref[...], 0.0)
        bias_sum += jnp.sum(delta.reshape(block // 8, 8, width), axis=0)
        wout_sum += jnp.sum((slope * hidden).reshape(block // 8, 8, width), axis=0)
        delta = delta.astype(BF16)
        delta_ref[span, :] = delta
        grad_ref[span, :] = mm(delta, hid_ref[...], NT).astype(BF16)
    for at in range(0, rows, wide):
        grad = mm(hot_rows(ends_ref[0:1, :] - at, wide), grad_ref[:, :width])
        grad += mm(hot_rows(ends_ref[1:2, :] - at, wide), grad_ref[:, width:])
        send_ref[at // 16 : (at + wide) // 16, 0:16, :] = grad.reshape(-1, 16, width).astype(BF16)
    hidden_ref[...] = mm(both_ref[...], delta_ref[...], TN)
    bias = jnp.sum(bias_sum, axis=0, keepdims=True)
    wout = jnp.sum(wout_sum, axis=0, keepdims=True)
    lines = []
    for line in (bias, wout):
        high = line.astype(BF16).astype(F32)
        for half in (high, line - high):
            lines += [half[:, :128], half[:, 128:]]
    tail = jnp.concatenate(lines, axis=0)
    total = hidden_ref[...].reshape(-1, 8, width)
    tail = jnp.broadcast_to(tail[None], (total.shape[0], 8, 128))
    even = jnp.concatenate([total[:, :, :128], tail], axis=2)
    odd = jnp.concatenate([total[:, :, 128:], tail], axis=2)
    joined = jnp.stack([even, odd], axis=1).reshape(-1, 8, width)
    send_ref[:, 16:24, :] = joined.astype(BF16)


def decode(got, ends, labels, weights, w_hidden, bias, w_out, parts):
    rows, width = got.shape
    pairs = ends.shape[1]
    return pl.pallas_call(
        decode_body,
        out_shape=(shape_of((1, pairs), F32), shape_of((parts, 24, width), BF16)),
        in_specs=[whole()] * 7,
        out_specs=(whole(), whole()),
        scratch_shapes=[
            pltpu.VMEM((pairs, 2 * width), BF16),
            pltpu.VMEM((pairs, width), BF16),
            pltpu.VMEM((pairs, 2 * width), BF16),
            pltpu.VMEM((2 * width, width), F32),
        ],
        compiler_params=limit(DECODE_MIB),
        cost_estimate=cost(10 * 10**9, 4 * 10**6),
        name="decode",
    )(got, ends, labels, weights, w_hidden, bias, w_out)


def spread_body(
    count_ref, back_ref, want_ref, feat_ref, agg_ref, degree_ref, neigh_ref,
    send_hbm, small_ref, grad_hbm, mean_hbm, send_ref, grad_ref, mean_ref, held_ref, sem, out_sems,
):
    nodes, width = feat_ref.shape
    rows = 1024
    copy = pltpu.make_async_copy(count_ref.at[:, nodes : nodes + held_ref.shape[1]], held_ref, sem)
    copy.start()
    back = back_ref[...].astype(F32)
    tail = jnp.sum(back[:, 16:, :], axis=0)
    small_ref[...] = tail[:, 128:]
    flat = back[:, :16, :].reshape(-1, width).astype(BF16)
    want = jnp.concatenate([want_ref[k : k + 1, :] for k in range(16)], axis=1)

    def gather(i, carry):
        at = i * rows
        span = pl.ds(pl.multiple_of(at, rows), rows)
        grad_ref[span, :] = mm(hot_rows(want - at, rows), flat).astype(BF16)
        return carry

    lax.fori_loop(0, nodes // rows, gather, 0)

    def scale(i, carry):
        span = pl.ds(pl.multiple_of(i * 256, 256), 256)
        degree = jnp.sum(degree_ref[:, span], axis=0, keepdims=True)
        column = jnp.transpose(jnp.broadcast_to(jnp.maximum(degree, 1.0), (128, 256)))
        scaled = mm(grad_ref[span, :], neigh_ref[...], NT) / jnp.concatenate([column, column], axis=1)
        mean_ref[span, :] = scaled.astype(BF16)
        return carry

    lax.fori_loop(0, nodes // 256, scale, 0, unroll=2)
    halves = [(slice(None), slice(0, 8)), (slice(None), slice(8, 16))]
    pairs = [(send_ref.at[half], send_hbm.at[half]) for half in halves]
    pairs += [(grad_ref, grad_hbm), (mean_ref, mean_hbm)]
    leaving = [pltpu.make_async_copy(*pair, out_sems.at[i]) for i, pair in enumerate(pairs)]
    leaving[2].start()
    leaving[3].start()
    both = jnp.concatenate(
        [mm(feat_ref[...], grad_ref[...], TN), mm(agg_ref[...], grad_ref[...], TN)], axis=0
    )
    both = both.reshape(-1, 8, width)
    tail = jnp.broadcast_to(tail[None, :, :128], (both.shape[0], 8, 128))
    even = jnp.concatenate([both[:, :, :128], tail], axis=2)
    odd = jnp.concatenate([both[:, :, 128:], tail], axis=2)
    joined = jnp.stack([even, odd], axis=1).reshape(-1, 8, width)
    send_ref[:, 8:16, :] = joined.astype(BF16)
    leaving[1].start()
    copy.wait()
    blocks = range(0, nodes, DST_BLOCK)
    parts = [mm(held_ref[n // DST_BLOCK], mean_ref[n : n + DST_BLOCK, :]) for n in blocks]
    grad = sum(parts[1:], parts[0]).reshape(-1, 8, width)
    send_ref[:, 0:8, :] = grad.astype(BF16)
    leaving[0].start()
    for copy in leaving:
        copy.wait()


def spread(counts, back, want, features, agg, degree, w_neigh):
    blocks, table, _ = counts.shape
    nodes, width = features.shape
    return pl.pallas_call(
        spread_body,
        out_shape=(
            pltpu.HBM((back.shape[0], 16, width), BF16),
            shape_of((8, 128), F32),
            pltpu.HBM((nodes, width), BF16),
            pltpu.HBM((nodes, width), BF16),
        ),
        in_specs=[whole(pltpu.HBM)] + [whole()] * 6,
        out_specs=(whole(pltpu.HBM), whole(), whole(pltpu.HBM), whole(pltpu.HBM)),
        scratch_shapes=[
            pltpu.VMEM((back.shape[0], 16, width), BF16),
            pltpu.VMEM((nodes, width), BF16),
            pltpu.VMEM((nodes, width), BF16),
            pltpu.VMEM((blocks, table - nodes, DST_BLOCK), BF16),
            pltpu.SemaphoreType.DMA,
            pltpu.SemaphoreType.DMA((4,)),
        ],
        compiler_params=limit(SPREAD_MIB),
        cost_estimate=cost(5 * 10**9, 10 * 10**6),
        name="spread",
    )(counts, back, want, features, agg, degree, w_neigh)


def direct_body(count_ref, grad_ref, mean_ref, self_ref, out_ref, held_ref, sems):
    nodes = out_ref.shape[0]
    rows = 512

    def fetch(i):
        span = pl.ds(pl.multiple_of(i * rows, rows), rows)
        return pltpu.make_async_copy(count_ref.at[:, span], held_ref.at[:, span], sems.at[i])

    for i in range(nodes // rows):
        fetch(i).start()

    def own(i, carry):
        span = pl.ds(pl.multiple_of(i * rows, rows), rows)
        blocks = range(0, nodes, DST_BLOCK)
        total = mm(grad_ref[span, :], self_ref[...], NT)
        fetch(i).wait()
        parts = [mm(held_ref[n // DST_BLOCK, span, :], mean_ref[n : n + DST_BLOCK, :]) for n in blocks]
        out_ref[span, :] = sum(parts[1:], parts[0]) + total
        return carry

    lax.fori_loop(0, nodes // rows, own, 0)


def direct_rows(counts, grad, mean, w_self):
    nodes, width = grad.shape
    return pl.pallas_call(
        direct_body,
        out_shape=pltpu.HBM((nodes, width), F32),
        in_specs=[whole(pltpu.HBM)] + [whole()] * 3,
        out_specs=whole(),
        scratch_shapes=[
            pltpu.VMEM((counts.shape[0], nodes, DST_BLOCK), BF16),
            pltpu.SemaphoreType.DMA((nodes // 512,)),
        ],
        compiler_params=limit(DIRECT_MIB),
        cost_estimate=cost(3 * 10**9, 12 * 10**6),
        name="direct_rows",
    )(counts, grad, mean, w_self)


def chunk_body(back_ref, direct_ref, out_ref):
    del direct_ref
    tail = jnp.sum(back_ref[:, 8:, :].astype(F32), axis=0)[:, :128]
    out_ref[...] = jnp.broadcast_to(tail[None], out_ref.shape).astype(BF16)


def chunk(back, direct):
    return pl.pallas_call(
        chunk_body,
        out_shape=shape_of((back.shape[0], 8, 128), BF16),
        in_specs=[whole(), whole(pltpu.HBM)],
        out_specs=whole(),
        compiler_params=limit(CHUNK_MIB),
        cost_estimate=cost(10**6, 10**6),
        name="chunk",
    )(back, direct)


def join_lanes(pieces):
    pieces = pieces.reshape(-1, 2, 8, 128)
    return jnp.concatenate([pieces[:, 0], pieces[:, 1]], axis=2).reshape(-1, 256)


def final_body(
    direct_ref, back_ref, halo_ref, small_ref, out_ref, hidden_ref, bias_ref, wout_ref, held_ref, sems
):
    rows = 512
    copies = []
    for i in range(out_ref.shape[0] // rows):
        part = slice(i * rows, (i + 1) * rows)
        copies.append(pltpu.make_async_copy(direct_ref.at[part], held_ref.at[part], sems.at[i]))
        copies[-1].start()
    back = back_ref[...].astype(F32)
    width = back.shape[2]
    flat = back[:, :8, :].reshape(-1, width).astype(BF16)
    halo = jnp.concatenate([halo_ref[k : k + 1, :] for k in range(8)], axis=1)

    def add(i, carry):
        part = pl.ds(pl.multiple_of(i * rows, rows), rows)
        extra = mm(hot_rows(halo - i * rows, rows), flat)
        pltpu.make_async_copy(direct_ref.at[part], held_ref.at[part], sems.at[i]).wait()
        out_ref[part, :] = held_ref[part, :] + extra
        return carry

    lax.fori_loop(0, len(copies), add, 0)
    hidden_ref[...] = join_lanes(back[:, 8:, 128:])
    bias_ref[...] = small_ref[0:2, :] + small_ref[2:4, :]
    wout_ref[...] = small_ref[4:6, :] + small_ref[6:8, :]


def final(direct, back, halo, small):
    nodes, width = direct.shape
    return pl.pallas_call(
        final_body,
        out_shape=(
            shape_of((nodes, width), F32),
            shape_of((2 * width, width), F32),
            shape_of((2, 128), F32),
            shape_of((2, 128), F32),
        ),
        in_specs=[whole(pltpu.HBM)] + [whole()] * 3,
        out_specs=(whole(),) * 4,
        scratch_shapes=[
            pltpu.VMEM((nodes, width), F32),
            pltpu.SemaphoreType.DMA((nodes // 512,)),
        ],
        compiler_params=limit(FINAL_MIB),
        cost_estimate=cost(2 * 10**9, 6 * 10**6),
        name="final",
    )(direct, back, halo, small)


def weights_body(pieces_ref, self_ref, neigh_ref):
    both = join_lanes(pieces_ref[...].astype(F32))
    half = both.shape[0] // 2
    self_ref[...] = both[:half, :]
    neigh_ref[...] = both[half:, :]


def weights(pieces):
    shape = shape_of((256, 256), F32)
    return pl.pallas_call(
        weights_body,
        out_shape=(shape, shape),
        in_specs=[whole()],
        out_specs=(whole(), whole()),
        compiler_params=limit(WEIGHTS_MIB),
        cost_estimate=cost(10**6, 10**6),
        name="weights",
    )(pieces)


def exchange(rows):
    return lax.all_to_all(rows, AXES, split_axis=0, concat_axis=0, tiled=True)


def per_device(
    features, edge_src, edge_dst, edge_count, halo_index, request_rows, pair_ends,
    labels, pair_weight, w_self, w_neigh, w_hidden, b_hidden, w_out,
):
    nodes, width = features.shape
    parts, halo_len = halo_index.shape[1:]
    table = nodes + parts * halo_len
    slots = edge_src.shape[0]
    me = lax.axis_index("dom") * lax.axis_size("grp") + lax.axis_index("grp")

    held = [pltpu.with_memory_space_constraint(x, pltpu.HBM) for x in (halo_index[0].T, request_rows[0].T, features)]
    sent = send_rows((me % 8).reshape(1), *held)
    arrived = exchange(sent)

    src_blocks = table // SRC_BLOCK
    buckets = nodes // DST_BLOCK * src_blocks
    bucket = edge_dst // DST_BLOCK * src_blocks + edge_src // SRC_BLOCK
    packed = (bucket << 18) | ((edge_dst % DST_BLOCK) << 10) | (edge_src % SRC_BLOCK)
    live = jnp.arange(slots, dtype=I32) < edge_count[0]
    keys = jnp.where(live, packed, buckets << 18)
    bounds = jnp.arange(buckets + 1, dtype=I32) << 18
    starts = jnp.sum((keys[None, :] < bounds[:, None]).astype(I32), axis=1)
    keys = lax.sort(keys, is_stable=False)
    counts, degree = edge_counts(starts, keys.reshape(slots // 128, 128), nodes, table)

    fixed = pltpu.with_memory_space_constraint(counts, pltpu.HBM)
    served, agg, want = embed(fixed, arrived, features, degree, w_self, w_neigh)
    got = exchange(served.reshape(parts, -1, width)).reshape(-1, width)
    logits, pair_back = decode(
        got, pair_ends.T, labels.reshape(1, -1), pair_weight.reshape(1, -1),
        w_hidden, b_hidden.reshape(1, -1), w_out.reshape(1, -1), parts,
    )
    back = exchange(pair_back)
    halo_back, small, grad, mean = spread(fixed, back, want, features, agg, degree, w_neigh)
    returned = exchange(halo_back)
    direct = direct_rows(fixed, grad, mean, w_self)
    direct = pltpu.with_memory_space_constraint(direct, pltpu.HBM)
    pieces = exchange(chunk(returned, direct))
    grad_features, grad_hidden, grad_bias, grad_out = final(
        direct, returned, halo_index[0].reshape(8, -1), small
    )
    grad_self, grad_neigh = weights(pieces)
    return (
        logits.reshape(-1), grad_features, grad_self, grad_neigh, grad_hidden,
        grad_bias.reshape(-1), grad_out.reshape(-1),
    )


def solution(mesh):
    split, rows, cubes = P(AXES), P(AXES, None), P(AXES, None, None)
    in_specs = (
        rows, split, split, split, cubes, cubes, rows, split, split, P(), P(), P(), P(), P(),
    )
    out_specs = (split, rows, P(), P(), P(), P(), P())
    return jax.shard_map(
        per_device, mesh=mesh, in_specs=in_specs, out_specs=out_specs, check_vma=False
    )
```

```python
import functools

import jax
import jax.numpy as jnp
from jax import lax
from jax.experimental import pallas as pl
from jax.experimental.pallas import tpu as pltpu
from jax.sharding import PartitionSpec as P

BF16, F32, I16, I32 = jnp.bfloat16, jnp.float32, jnp.int16, jnp.int32
NN = (((1,), (0,)), ((), ()))
NT = (((1,), (1,)), ((), ()))
TN = (((0,), (0,)), ((), ()))
AXES = ("dom", "grp")
DST_BLOCK = 256
SRC_BLOCK = 256
VISITS = 8
UNROLL = 2
SEND_MIB, EDGES_MIB, EMBED_MIB, DECODE_MIB, SPREAD_MIB = 8, 24, 24, 16, 16
DIRECT_MIB = 16
CHUNK_MIB, FINAL_MIB, WEIGHTS_MIB = 8, 16, 8


def limit(mib):
    return pltpu.CompilerParams(vmem_limit_bytes=mib * 1024 * 1024)


def mm(left, right, dims=NN):
    return lax.dot_general(left, right, dims, preferred_element_type=F32)


def spread_hot(diff, step, count, axis):
    one, zero = jnp.ones((), BF16), jnp.zeros((), BF16)
    pieces = [jnp.where(diff == jnp.int16(step * k), one, zero) for k in range(count)]
    return jnp.concatenate(pieces, axis=axis)


def hot_rows(row, height):
    width = row.shape[1]
    wide = jnp.broadcast_to(row, (16, width)) - lax.broadcasted_iota(I32, (16, width), 0)
    return spread_hot(wide.astype(I16), 16, height // 16, 0)


def lane_diff(tile):
    return (tile - lax.broadcasted_iota(I32, tile.shape, 1)).astype(I16)


def hot_lanes(diff, width):
    return spread_hot(diff, 128, width // 128, 1)


def hot_tile(tile, width):
    return hot_lanes(lane_diff(tile), width)


def whole(memory_space=pltpu.VMEM):
    return pl.BlockSpec(memory_space=memory_space)


def shape_of(shape, dtype):
    return jax.ShapeDtypeStruct(shape, dtype)


def cost(flops, moved):
    return pl.CostEstimate(flops=flops, bytes_accessed=moved, transcendentals=0)


def send_body(slot_ref, halo_hbm, want_hbm, feat_hbm, out_ref, halo_ref, want_ref, feat_ref, sems):
    pairs = ((halo_hbm, halo_ref), (want_hbm, want_ref), (feat_hbm, feat_ref))
    copies = [pltpu.make_async_copy(*pair, sems.at[i]) for i, pair in enumerate(pairs)]
    for copy in copies:
        copy.start()
    copies[0].wait()
    copies[1].wait()
    parts = out_ref.shape[0]
    want = jnp.transpose(want_ref[...])
    tiled = jnp.concatenate([want] * 8, axis=1)
    lane = lax.broadcasted_iota(I32, tiled.shape, 1)
    mine = lax.shift_right_logical(lane, 4) == slot_ref[0]
    tiled = jnp.where(mine, tiled, 0)
    high, low = lax.shift_right_logical(tiled, 7).astype(F32), (tiled & 127).astype(F32)
    halo = halo_ref[...]
    tiles = [jnp.broadcast_to(halo[:, p : p + 1], (8, 128)) for p in range(parts)]
    diff = lane_diff(jnp.concatenate(tiles, axis=0))
    copies[2].wait()
    rows = mm(hot_lanes(diff, feat_ref.shape[0]), feat_ref[...])
    rows = rows.reshape(parts, 8, rows.shape[1])
    upper = lax.broadcasted_iota(I32, (parts, 8, 128), 1) < 4
    notes = jnp.where(upper, high[:, None, :], low[:, None, :])
    out_ref[...] = jnp.concatenate([rows[:, :, :128], rows[:, :, 128:], notes], axis=1).astype(BF16)


def send_rows(slot, halo, want, features):
    parts = want.shape[1]
    return pl.pallas_call(
        send_body,
        out_shape=shape_of((parts, 24, 128), BF16),
        in_specs=[whole(pltpu.SMEM)] + [whole(pltpu.HBM)] * 3,
        out_specs=whole(),
        scratch_shapes=[
            pltpu.VMEM(halo.shape, I32),
            pltpu.VMEM(want.shape, I32),
            pltpu.VMEM(features.shape, BF16),
            pltpu.SemaphoreType.DMA((3,)),
        ],
        compiler_params=limit(SEND_MIB),
        cost_estimate=cost(10**9, 2 * 10**6),
        name="send_rows",
    )(slot, halo, want, features)


def sort_body(src_blocks, blocks, live_ref, src_ref, dst_ref, out_ref):
    shape = (8, 128)
    count = src_ref.shape[0] // 8
    dead = blocks << 18
    sub = lax.broadcasted_iota(I32, shape, 0)
    lane = lax.broadcasted_iota(I32, shape, 1)
    shift = SRC_BLOCK.bit_length() - 1
    keys = []
    for v in range(count):
        src, dst = src_ref[8 * v : 8 * v + 8, :], dst_ref[8 * v : 8 * v + 8, :]
        block = lax.shift_right_logical(dst, 8) * src_blocks + lax.shift_right_logical(src, shift)
        packed = (block << 18) | ((dst & 255) << 10) | (src & (SRC_BLOCK - 1))
        keys.append(jnp.where(1024 * v + 128 * sub + lane < live_ref[0], packed, dead))
    bits = [None] * 4
    bits += [-(lax.shift_right_logical(sub, b) & 1) for b in range(3)]
    bits += [-(lax.shift_right_logical(lane, b) & 1) for b in range(7)]
    total = len(bits)

    def flips(k):
        if k == 0 or k == total:
            return [0] * count
        if k < 4:
            return [-((v >> k) & 1) for v in range(count)]
        return [bits[k]] * count

    for k in range(1, total + 1):
        for v, (old, new) in enumerate(zip(flips(k - 1), flips(k))):
            for flip in (old, new):
                if not isinstance(flip, int):
                    keys[v] = keys[v] ^ flip
                elif flip:
                    keys[v] = ~keys[v]
        for j in reversed(range(k)):
            if j < 4:
                for v in range(count):
                    if not (v >> j) & 1:
                        a, b = keys[v], keys[v | 1 << j]
                        keys[v], keys[v | 1 << j] = jnp.minimum(a, b), jnp.maximum(a, b)
                continue
            axis, step, size = (0, 1 << (j - 4), 8) if j < 7 else (1, 1 << (j - 7), 128)
            low = bits[j] == 0
            for v in range(count):
                key = keys[v]
                after = pltpu.roll(key, size - step, axis)
                before = after if 2 * step == size else pltpu.roll(key, step, axis)
                keys[v] = jnp.where(low, jnp.minimum(key, after), jnp.maximum(key, before))
    out_ref[...] = jnp.transpose(jnp.concatenate(keys, axis=0))


def sort_edges(live, src, dst, src_blocks, blocks):
    return pl.pallas_call(
        functools.partial(sort_body, src_blocks, blocks),
        out_shape=shape_of(src.shape, I32),
        in_specs=[whole(pltpu.SMEM), whole(), whole()],
        out_specs=whole(),
        compiler_params=limit(8),
        cost_estimate=cost(10**9, 2 * 10**5),
        name="sort_edges",
    )(live, src, dst)


def edges_body(src_blocks, starts_ref, keys_ref, count_ref, degree_ref, held_ref, acc_ref, sem):
    top = keys_ref.shape[0] - 1
    buckets = degree_ref.shape[1] // DST_BLOCK * src_blocks
    degree_ref[...] = jnp.zeros_like(degree_ref)
    ones = (lax.broadcasted_iota(I32, (16, 512), 0) == 0).astype(F32).astype(BF16)

    def block_of(bucket):
        tall = pl.multiple_of(lax.rem(bucket, src_blocks) * SRC_BLOCK, SRC_BLOCK)
        return bucket // src_blocks, pl.ds(tall, SRC_BLOCK)

    def flush(bucket):
        outer, tall = block_of(bucket)
        return pltpu.make_async_copy(held_ref.at[outer, tall], count_ref.at[outer, tall], sem)

    def products(bucket, row):
        wanted = jnp.where(bucket < buckets, bucket, -1)
        src, dst = [], []
        for i in range(4):
            keys = keys_ref[pl.ds(jnp.minimum(row + i, top), 1), :]
            live = jnp.logical_and(lax.shift_right_logical(keys, 18) == wanted, row + i <= top)
            dst.append(jnp.where(live, lax.shift_right_logical(keys, 10) & 255, -1))
            src.append(keys & 1023)
        src, dst = jnp.concatenate(src, axis=1), jnp.concatenate(dst, axis=1)
        right = hot_rows(dst, DST_BLOCK)
        both = mm(jnp.concatenate([hot_rows(src, SRC_BLOCK), ones], axis=0), right, NT)
        return both[:SRC_BLOCK], both[SRC_BLOCK : SRC_BLOCK + 8]

    def store(bucket, fresh, parts, degree):
        last = jnp.minimum(bucket, buckets - 1)
        outer, _ = block_of(last)
        wide = pl.ds(pl.multiple_of(outer * DST_BLOCK, DST_BLOCK), DST_BLOCK)
        base = lax.rem(last, src_blocks) * SRC_BLOCK
        for i in range(SRC_BLOCK // 256):
            rows = slice(i * 256, (i + 1) * 256)
            total = parts[rows] + jnp.where(fresh, 0.0, acc_ref[rows, :])
            acc_ref[rows, :] = total
            tall = pl.ds(pl.multiple_of(base + i * 256, 256), 256)
            held_ref[outer, tall, :] = total.astype(BF16)
        degree_ref[:, wide] += degree

    def advance(bucket, row):
        last = starts_ref[jnp.minimum(bucket + 1, buckets)]
        ended = (row + 4) * 128 >= last
        after = jnp.minimum(bucket + ended.astype(I32), buckets)
        return after, jnp.where(ended, lax.shift_right_logical(starts_ref[after], 7), row + 4), ended

    def body(carry):
        bucket, row, fresh = carry
        visits = []
        for _ in range(VISITS):
            after, following, ended = advance(bucket, row)
            visits.append((bucket, row, fresh == 1, ended))
            bucket, row = after, following
            fresh = jnp.logical_and(ended, bucket < buckets).astype(I32)
        made = [products(*visit[:2]) for visit in visits]
        for visit, both in zip(visits, made):
            store(visit[0], visit[2], *both)
        for visit in visits:
            @pl.when(jnp.logical_and(visit[3], visit[0] < buckets))
            def _(visit=visit):
                flush(visit[0]).start()

        return bucket, row, fresh

    start = (jnp.int32(0), lax.shift_right_logical(starts_ref[0], 7), jnp.int32(1))
    lax.while_loop(lambda carry: carry[0] < buckets, body, start)
    pltpu.make_async_copy(held_ref, count_ref, sem).wait()


def edge_counts(starts, keys, nodes, table):
    blocks = nodes // DST_BLOCK
    return pl.pallas_call(
        functools.partial(edges_body, table // SRC_BLOCK),
        out_shape=(pltpu.HBM((blocks, table, DST_BLOCK), BF16), shape_of((8, nodes), F32)),
        in_specs=[whole(pltpu.SMEM), whole()],
        out_specs=(whole(pltpu.HBM), whole()),
        scratch_shapes=[
            pltpu.VMEM((blocks, table, DST_BLOCK), BF16),
            pltpu.VMEM((SRC_BLOCK, DST_BLOCK), F32),
            pltpu.SemaphoreType.DMA,
        ],
        compiler_params=limit(EDGES_MIB),
        cost_estimate=cost(14 * 10**9, 13 * 10**6),
        name="edge_counts",
    )(starts, keys)


def embed_body(
    count_ref, arrived_ref, feat_ref, degree_ref, self_ref, neigh_ref,
    served_ref, agg_ref, want_ref, held_ref, table_ref, mean_ref, emb_ref, sems,
):
    blocks = count_ref.shape[0]
    copies = [pltpu.make_async_copy(count_ref.at[i], held_ref.at[i], sems.at[i]) for i in range(blocks)]
    for copy in copies:
        copy.start()
    nodes = feat_ref.shape[0]
    table_ref[:, :nodes] = jnp.transpose(feat_ref[...])
    arrived = arrived_ref[...].astype(F32)
    for half in range(2):
        halo = arrived[:, 8 * half : 8 * half + 8, :].reshape(-1, 128).astype(BF16)
        table_ref[128 * half : 128 * half + 128, nodes:] = jnp.transpose(halo)
    notes = arrived[:, 16:, :]
    grouped = notes.reshape(notes.shape[0] // 8, 8, 8, notes.shape[2])
    summed = jnp.sum(grouped, axis=1)
    want = (summed[:, 0, :] * 128.0 + summed[:, 4, :]).astype(I32)
    want_ref[...] = want
    columns = jnp.transpose(want)
    def node_block(i, carry):
        span = pl.ds(pl.multiple_of(i * DST_BLOCK, DST_BLOCK), DST_BLOCK)
        pltpu.make_async_copy(count_ref.at[i], held_ref.at[i], sems.at[i]).wait()
        sums = mm(table_ref[...], held_ref[i])
        degree = jnp.sum(degree_ref[:, span], axis=0, keepdims=True)
        mean_ref[:, span] = (sums / jnp.maximum(degree, 1.0)).astype(BF16)
        return carry

    lax.fori_loop(0, nodes // DST_BLOCK, node_block, 0)
    agg_ref[...] = jnp.transpose(mean_ref[...])
    for at in range(0, nodes, 1024):
        span = slice(at, at + 1024)
        both = mm(feat_ref[span, :], self_ref[...]) + mm(agg_ref[span, :], neigh_ref[...])
        emb_ref[span, :] = both.astype(BF16)
    for k in range(0, columns.shape[1], 8):
        tiles = [jnp.broadcast_to(columns[:, i : i + 1], (128, 128)) for i in range(k, k + 8)]
        hot = hot_tile(jnp.concatenate(tiles, axis=0), nodes)
        served_ref[k * 128 : (k + 8) * 128, :] = mm(hot, emb_ref[...]).astype(BF16)


def embed(counts, arrived, features, degree, w_self, w_neigh):
    blocks, table, _ = counts.shape
    nodes, width = features.shape
    return pl.pallas_call(
        embed_body,
        out_shape=(
            shape_of((nodes, width), BF16),
            shape_of((nodes, width), BF16),
            shape_of((16, 128), I32),
        ),
        in_specs=[whole(pltpu.HBM)] + [whole()] * 5,
        out_specs=(whole(),) * 3,
        scratch_shapes=[
            pltpu.VMEM(counts.shape, BF16),
            pltpu.VMEM((width, table), BF16),
            pltpu.VMEM((width, nodes), BF16),
            pltpu.VMEM((nodes, width), BF16),
            pltpu.SemaphoreType.DMA((blocks,)),
        ],
        compiler_params=limit(EMBED_MIB),
        cost_estimate=cost(6 * 10**9, 16 * 10**6),
        name="embed",
    )(counts, arrived, features, degree, w_self, w_neigh)


def decode_body(
    got_ref, ends_ref, label_ref, weight_ref, hid_ref, bias_ref, wout_ref,
    logit_ref, send_ref, both_ref, delta_ref, grad_ref, hidden_ref,
):
    rows, width = got_ref.shape
    pairs = ends_ref.shape[1]
    block = 512
    wide = 1024
    meta = jnp.concatenate(
        [
            ends_ref[...].astype(F32),
            label_ref[...].astype(F32),
            weight_ref[...],
            jnp.zeros((4, pairs), F32),
        ],
        axis=0,
    )
    cols = jnp.transpose(meta)
    ends = cols.astype(I32)
    for side in range(2):
        for at in range(0, pairs, wide):
            tile = jnp.broadcast_to(ends[at : at + wide, side : side + 1], (wide, 128))
            picked = mm(hot_tile(tile, rows), got_ref[...])
            both_ref[at : at + wide, side * width : (side + 1) * width] = picked.astype(BF16)
    bias_sum = jnp.zeros((8, width), F32)
    wout_sum = jnp.zeros((8, width), F32)
    for at in range(0, pairs, block):
        span = slice(at, at + block)
        pre = mm(both_ref[span, :], hid_ref[...]) + bias_ref[...]
        hidden = jnp.maximum(pre, 0.0)
        logits = jnp.sum(hidden * wout_ref[...], axis=1, keepdims=True)
        logit_ref[:, span] = jnp.transpose(jnp.broadcast_to(logits, (block, 128)))[0:1, :]
        slope = cols[span, 3:4] * (jax.nn.sigmoid(logits) - cols[span, 2:3])
        delta = jnp.where(pre > 0, slope * wout_ref[...], 0.0)
        bias_sum += jnp.sum(delta.reshape(block // 8, 8, width), axis=0)
        wout_sum += jnp.sum((slope * hidden).reshape(block // 8, 8, width), axis=0)
        delta = delta.astype(BF16)
        delta_ref[span, :] = delta
        grad_ref[span, :] = mm(delta, hid_ref[...], NT).astype(BF16)
    for at in range(0, rows, wide):
        grad = mm(hot_rows(ends_ref[0:1, :] - at, wide), grad_ref[:, :width])
        grad += mm(hot_rows(ends_ref[1:2, :] - at, wide), grad_ref[:, width:])
        send_ref[at // 16 : (at + wide) // 16, 0:16, :] = grad.reshape(-1, 16, width).astype(BF16)
    hidden_ref[...] = mm(both_ref[...], delta_ref[...], TN)
    bias = jnp.sum(bias_sum, axis=0, keepdims=True)
    wout = jnp.sum(wout_sum, axis=0, keepdims=True)
    lines = []
    for line in (bias, wout):
        high = line.astype(BF16).astype(F32)
        for half in (high, line - high):
            lines += [half[:, :128], half[:, 128:]]
    tail = jnp.concatenate(lines, axis=0)
    total = hidden_ref[...].reshape(-1, 8, width)
    tail = jnp.broadcast_to(tail[None], (total.shape[0], 8, 128))
    even = jnp.concatenate([total[:, :, :128], tail], axis=2)
    odd = jnp.concatenate([total[:, :, 128:], tail], axis=2)
    joined = jnp.stack([even, odd], axis=1).reshape(-1, 8, width)
    send_ref[:, 16:24, :] = joined.astype(BF16)


def decode(got, ends, labels, weights, w_hidden, bias, w_out, parts):
    rows, width = got.shape
    pairs = ends.shape[1]
    return pl.pallas_call(
        decode_body,
        out_shape=(shape_of((1, pairs), F32), shape_of((parts, 24, width), BF16)),
        in_specs=[whole()] * 7,
        out_specs=(whole(), whole()),
        scratch_shapes=[
            pltpu.VMEM((pairs, 2 * width), BF16),
            pltpu.VMEM((pairs, width), BF16),
            pltpu.VMEM((pairs, 2 * width), BF16),
            pltpu.VMEM((2 * width, width), F32),
        ],
        compiler_params=limit(DECODE_MIB),
        cost_estimate=cost(10 * 10**9, 4 * 10**6),
        name="decode",
    )(got, ends, labels, weights, w_hidden, bias, w_out)


def spread_body(
    count_ref, back_ref, want_ref, feat_ref, agg_ref, degree_ref, neigh_ref,
    send_hbm, small_ref, grad_hbm, mean_hbm, send_ref, grad_ref, mean_ref, held_ref, sem, out_sems,
):
    nodes, width = feat_ref.shape
    rows = 1024
    copy = pltpu.make_async_copy(count_ref.at[:, nodes : nodes + held_ref.shape[1]], held_ref, sem)
    copy.start()
    back = back_ref[...].astype(F32)
    tail = jnp.sum(back[:, 16:, :], axis=0)
    small_ref[...] = tail[:, 128:]
    flat = back[:, :16, :].reshape(-1, width).astype(BF16)
    want = jnp.concatenate([want_ref[k : k + 1, :] for k in range(16)], axis=1)

    def gather(i, carry):
        at = i * rows
        span = pl.ds(pl.multiple_of(at, rows), rows)
        grad_ref[span, :] = mm(hot_rows(want - at, rows), flat).astype(BF16)
        return carry

    lax.fori_loop(0, nodes // rows, gather, 0)

    def scale(i, carry):
        span = pl.ds(pl.multiple_of(i * 256, 256), 256)
        degree = jnp.sum(degree_ref[:, span], axis=0, keepdims=True)
        column = jnp.transpose(jnp.broadcast_to(jnp.maximum(degree, 1.0), (128, 256)))
        scaled = mm(grad_ref[span, :], neigh_ref[...], NT) / jnp.concatenate([column, column], axis=1)
        mean_ref[span, :] = scaled.astype(BF16)
        return carry

    lax.fori_loop(0, nodes // 256, scale, 0, unroll=2)
    halves = [(slice(None), slice(0, 8)), (slice(None), slice(8, 16))]
    pairs = [(send_ref.at[half], send_hbm.at[half]) for half in halves]
    pairs += [(grad_ref, grad_hbm), (mean_ref, mean_hbm)]
    leaving = [pltpu.make_async_copy(*pair, out_sems.at[i]) for i, pair in enumerate(pairs)]
    leaving[2].start()
    leaving[3].start()
    both = jnp.concatenate(
        [mm(feat_ref[...], grad_ref[...], TN), mm(agg_ref[...], grad_ref[...], TN)], axis=0
    )
    both = both.reshape(-1, 8, width)
    tail = jnp.broadcast_to(tail[None, :, :128], (both.shape[0], 8, 128))
    even = jnp.concatenate([both[:, :, :128], tail], axis=2)
    odd = jnp.concatenate([both[:, :, 128:], tail], axis=2)
    joined = jnp.stack([even, odd], axis=1).reshape(-1, 8, width)
    send_ref[:, 8:16, :] = joined.astype(BF16)
    leaving[1].start()
    copy.wait()
    blocks = range(0, nodes, DST_BLOCK)
    parts = [mm(held_ref[n // DST_BLOCK], mean_ref[n : n + DST_BLOCK, :]) for n in blocks]
    grad = sum(parts[1:], parts[0]).reshape(-1, 8, width)
    send_ref[:, 0:8, :] = grad.astype(BF16)
    leaving[0].start()
    for copy in leaving:
        copy.wait()


def spread(counts, back, want, features, agg, degree, w_neigh):
    blocks, table, _ = counts.shape
    nodes, width = features.shape
    return pl.pallas_call(
        spread_body,
        out_shape=(
            pltpu.HBM((back.shape[0], 16, width), BF16),
            shape_of((8, 128), F32),
            pltpu.HBM((nodes, width), BF16),
            pltpu.HBM((nodes, width), BF16),
        ),
        in_specs=[whole(pltpu.HBM)] + [whole()] * 6,
        out_specs=(whole(pltpu.HBM), whole(), whole(pltpu.HBM), whole(pltpu.HBM)),
        scratch_shapes=[
            pltpu.VMEM((back.shape[0], 16, width), BF16),
            pltpu.VMEM((nodes, width), BF16),
            pltpu.VMEM((nodes, width), BF16),
            pltpu.VMEM((blocks, table - nodes, DST_BLOCK), BF16),
            pltpu.SemaphoreType.DMA,
            pltpu.SemaphoreType.DMA((4,)),
        ],
        compiler_params=limit(SPREAD_MIB),
        cost_estimate=cost(5 * 10**9, 10 * 10**6),
        name="spread",
    )(counts, back, want, features, agg, degree, w_neigh)


def direct_body(count_ref, grad_ref, mean_ref, self_ref, out_ref, held_ref, sems):
    nodes = out_ref.shape[0]
    rows = 512

    def fetch(i):
        span = pl.ds(pl.multiple_of(i * rows, rows), rows)
        return pltpu.make_async_copy(count_ref.at[:, span], held_ref.at[:, span], sems.at[i])

    for i in range(nodes // rows):
        fetch(i).start()

    def own(i, carry):
        span = pl.ds(pl.multiple_of(i * rows, rows), rows)
        blocks = range(0, nodes, DST_BLOCK)
        total = mm(grad_ref[span, :], self_ref[...], NT)
        fetch(i).wait()
        parts = [mm(held_ref[n // DST_BLOCK, span, :], mean_ref[n : n + DST_BLOCK, :]) for n in blocks]
        out_ref[span, :] = sum(parts[1:], parts[0]) + total
        return carry

    lax.fori_loop(0, nodes // rows, own, 0)


def direct_rows(counts, grad, mean, w_self):
    nodes, width = grad.shape
    return pl.pallas_call(
        direct_body,
        out_shape=pltpu.HBM((nodes, width), F32),
        in_specs=[whole(pltpu.HBM)] + [whole()] * 3,
        out_specs=whole(),
        scratch_shapes=[
            pltpu.VMEM((counts.shape[0], nodes, DST_BLOCK), BF16),
            pltpu.SemaphoreType.DMA((nodes // 512,)),
        ],
        compiler_params=limit(DIRECT_MIB),
        cost_estimate=cost(3 * 10**9, 12 * 10**6),
        name="direct_rows",
    )(counts, grad, mean, w_self)


def chunk_body(back_ref, direct_ref, out_ref):
    del direct_ref
    tail = jnp.sum(back_ref[:, 8:, :].astype(F32), axis=0)[:, :128]
    out_ref[...] = jnp.broadcast_to(tail[None], out_ref.shape).astype(BF16)


def chunk(back, direct):
    return pl.pallas_call(
        chunk_body,
        out_shape=shape_of((back.shape[0], 8, 128), BF16),
        in_specs=[whole(), whole(pltpu.HBM)],
        out_specs=whole(),
        compiler_params=limit(CHUNK_MIB),
        cost_estimate=cost(10**6, 10**6),
        name="chunk",
    )(back, direct)


def join_lanes(pieces):
    pieces = pieces.reshape(-1, 2, 8, 128)
    return jnp.concatenate([pieces[:, 0], pieces[:, 1]], axis=2).reshape(-1, 256)


def final_body(
    direct_ref, back_ref, halo_ref, small_ref, out_ref, hidden_ref, bias_ref, wout_ref, held_ref, sems
):
    rows = 512
    copies = []
    for i in range(out_ref.shape[0] // rows):
        part = slice(i * rows, (i + 1) * rows)
        copies.append(pltpu.make_async_copy(direct_ref.at[part], held_ref.at[part], sems.at[i]))
        copies[-1].start()
    back = back_ref[...].astype(F32)
    width = back.shape[2]
    flat = back[:, :8, :].reshape(-1, width).astype(BF16)
    halo = jnp.concatenate([halo_ref[k : k + 1, :] for k in range(8)], axis=1)

    def add(i, carry):
        part = pl.ds(pl.multiple_of(i * rows, rows), rows)
        extra = mm(hot_rows(halo - i * rows, rows), flat)
        pltpu.make_async_copy(direct_ref.at[part], held_ref.at[part], sems.at[i]).wait()
        out_ref[part, :] = held_ref[part, :] + extra
        return carry

    lax.fori_loop(0, len(copies), add, 0)
    hidden_ref[...] = join_lanes(back[:, 8:, 128:])
    bias_ref[...] = small_ref[0:2, :] + small_ref[2:4, :]
    wout_ref[...] = small_ref[4:6, :] + small_ref[6:8, :]


def final(direct, back, halo, small):
    nodes, width = direct.shape
    return pl.pallas_call(
        final_body,
        out_shape=(
            shape_of((nodes, width), F32),
            shape_of((2 * width, width), F32),
            shape_of((2, 128), F32),
            shape_of((2, 128), F32),
        ),
        in_specs=[whole(pltpu.HBM)] + [whole()] * 3,
        out_specs=(whole(),) * 4,
        scratch_shapes=[
            pltpu.VMEM((nodes, width), F32),
            pltpu.SemaphoreType.DMA((nodes // 512,)),
        ],
        compiler_params=limit(FINAL_MIB),
        cost_estimate=cost(2 * 10**9, 6 * 10**6),
        name="final",
    )(direct, back, halo, small)


def weights_body(pieces_ref, self_ref, neigh_ref):
    both = join_lanes(pieces_ref[...].astype(F32))
    half = both.shape[0] // 2
    self_ref[...] = both[:half, :]
    neigh_ref[...] = both[half:, :]


def weights(pieces):
    shape = shape_of((256, 256), F32)
    return pl.pallas_call(
        weights_body,
        out_shape=(shape, shape),
        in_specs=[whole()],
        out_specs=(whole(), whole()),
        compiler_params=limit(WEIGHTS_MIB),
        cost_estimate=cost(10**6, 10**6),
        name="weights",
    )(pieces)


def exchange(rows):
    return lax.all_to_all(rows, AXES, split_axis=0, concat_axis=0, tiled=True)


def per_device(
    features, edge_src, edge_dst, edge_count, halo_index, request_rows, pair_ends,
    labels, pair_weight, w_self, w_neigh, w_hidden, b_hidden, w_out,
):
    nodes, width = features.shape
    parts, halo_len = halo_index.shape[1:]
    table = nodes + parts * halo_len
    slots = edge_src.shape[0]
    me = lax.axis_index("dom") * lax.axis_size("grp") + lax.axis_index("grp")

    held = [pltpu.with_memory_space_constraint(x, pltpu.HBM) for x in (halo_index[0].T, request_rows[0].T, features)]
    sent = send_rows((me % 8).reshape(1), *held)
    arrived = exchange(sent)

    src_blocks = table // SRC_BLOCK
    buckets = nodes // DST_BLOCK * src_blocks
    square = (slots // 128, 128)
    keys = sort_edges(edge_count, edge_src.reshape(square), edge_dst.reshape(square), src_blocks, buckets)
    bounds = jnp.arange(buckets + 1, dtype=I32) << 18
    starts = jnp.sum((keys.reshape(1, -1) < bounds[:, None]).astype(I32), axis=1)
    counts, degree = edge_counts(starts, keys, nodes, table)

    fixed = pltpu.with_memory_space_constraint(counts, pltpu.HBM)
    served, agg, want = embed(fixed, arrived, features, degree, w_self, w_neigh)
    got = exchange(served.reshape(parts, -1, width)).reshape(-1, width)
    logits, pair_back = decode(
        got, pair_ends.T, labels.reshape(1, -1), pair_weight.reshape(1, -1),
        w_hidden, b_hidden.reshape(1, -1), w_out.reshape(1, -1), parts,
    )
    back = exchange(pair_back)
    halo_back, small, grad, mean = spread(fixed, back, want, features, agg, degree, w_neigh)
    returned = exchange(halo_back)
    direct = direct_rows(fixed, grad, mean, w_self)
    direct = pltpu.with_memory_space_constraint(direct, pltpu.HBM)
    pieces = exchange(chunk(returned, direct))
    grad_features, grad_hidden, grad_bias, grad_out = final(
        direct, returned, halo_index[0].reshape(8, -1), small
    )
    grad_self, grad_neigh = weights(pieces)
    return (
        logits.reshape(-1), grad_features, grad_self, grad_neigh, grad_hidden,
        grad_bias.reshape(-1), grad_out.reshape(-1),
    )


def solution(mesh):
    split, rows, cubes = P(AXES), P(AXES, None), P(AXES, None, None)
    in_specs = (
        rows, split, split, split, cubes, cubes, rows, split, split, P(), P(), P(), P(), P(),
    )
    out_specs = (split, rows, P(), P(), P(), P(), P())
    return jax.shard_map(
        per_device, mesh=mesh, in_specs=in_specs, out_specs=out_specs, check_vma=False
    )
```

```python
import functools

import jax
import jax.numpy as jnp
from jax import lax
from jax.experimental import pallas as pl
from jax.experimental.pallas import tpu as pltpu
from jax.sharding import PartitionSpec as P

BF16, F32, I16, I32 = jnp.bfloat16, jnp.float32, jnp.int16, jnp.int32
NN = (((1,), (0,)), ((), ()))
NT = (((1,), (1,)), ((), ()))
TN = (((0,), (0,)), ((), ()))
AXES = ("dom", "grp")
DST_BLOCK = 256
SRC_BLOCK = 256
VISITS = 8
KEY_ROWS = 2
UNROLL = 2
SEND_MIB, EDGES_MIB, EMBED_MIB, DECODE_MIB, SPREAD_MIB = 8, 24, 24, 16, 16
DIRECT_MIB = 16
CHUNK_MIB, FINAL_MIB, WEIGHTS_MIB = 8, 16, 8


def limit(mib):
    return pltpu.CompilerParams(vmem_limit_bytes=mib * 1024 * 1024)


def mm(left, right, dims=NN):
    return lax.dot_general(left, right, dims, preferred_element_type=F32)


def spread_hot(diff, step, count, axis):
    one, zero = jnp.ones((), BF16), jnp.zeros((), BF16)
    pieces = [jnp.where(diff == jnp.int16(step * k), one, zero) for k in range(count)]
    return jnp.concatenate(pieces, axis=axis)


def hot_rows(row, height):
    width = row.shape[1]
    wide = jnp.broadcast_to(row, (16, width)) - lax.broadcasted_iota(I32, (16, width), 0)
    return spread_hot(wide.astype(I16), 16, height // 16, 0)


def lane_diff(tile):
    return (tile - lax.broadcasted_iota(I32, tile.shape, 1)).astype(I16)


def hot_lanes(diff, width):
    return spread_hot(diff, 128, width // 128, 1)


def hot_tile(tile, width):
    return hot_lanes(lane_diff(tile), width)


def whole(memory_space=pltpu.VMEM):
    return pl.BlockSpec(memory_space=memory_space)


def shape_of(shape, dtype):
    return jax.ShapeDtypeStruct(shape, dtype)


def cost(flops, moved):
    return pl.CostEstimate(flops=flops, bytes_accessed=moved, transcendentals=0)


def send_body(slot_ref, halo_hbm, want_hbm, feat_hbm, out_ref, halo_ref, want_ref, feat_ref, sems):
    pairs = ((halo_hbm, halo_ref), (want_hbm, want_ref), (feat_hbm, feat_ref))
    copies = [pltpu.make_async_copy(*pair, sems.at[i]) for i, pair in enumerate(pairs)]
    for copy in copies:
        copy.start()
    copies[0].wait()
    copies[1].wait()
    parts = out_ref.shape[0]
    want = jnp.transpose(want_ref[...])
    tiled = jnp.concatenate([want] * 8, axis=1)
    lane = lax.broadcasted_iota(I32, tiled.shape, 1)
    mine = lax.shift_right_logical(lane, 4) == slot_ref[0]
    tiled = jnp.where(mine, tiled, 0)
    high, low = lax.shift_right_logical(tiled, 7).astype(F32), (tiled & 127).astype(F32)
    halo = halo_ref[...]
    tiles = [jnp.broadcast_to(halo[:, p : p + 1], (8, 128)) for p in range(parts)]
    diff = lane_diff(jnp.concatenate(tiles, axis=0))
    copies[2].wait()
    rows = mm(hot_lanes(diff, feat_ref.shape[0]), feat_ref[...])
    rows = rows.reshape(parts, 8, rows.shape[1])
    upper = lax.broadcasted_iota(I32, (parts, 8, 128), 1) < 4
    notes = jnp.where(upper, high[:, None, :], low[:, None, :])
    out_ref[...] = jnp.concatenate([rows[:, :, :128], rows[:, :, 128:], notes], axis=1).astype(BF16)


def send_rows(slot, halo, want, features):
    parts = want.shape[1]
    return pl.pallas_call(
        send_body,
        out_shape=shape_of((parts, 24, 128), BF16),
        in_specs=[whole(pltpu.SMEM)] + [whole(pltpu.HBM)] * 3,
        out_specs=whole(),
        scratch_shapes=[
            pltpu.VMEM(halo.shape, I32),
            pltpu.VMEM(want.shape, I32),
            pltpu.VMEM(features.shape, BF16),
            pltpu.SemaphoreType.DMA((3,)),
        ],
        compiler_params=limit(SEND_MIB),
        cost_estimate=cost(10**9, 2 * 10**6),
        name="send_rows",
    )(slot, halo, want, features)


def sort_body(src_blocks, blocks, live_ref, src_ref, dst_ref, out_ref):
    shape = (8, 128)
    count = src_ref.shape[0] // 8
    dead = blocks << 18
    sub = lax.broadcasted_iota(I32, shape, 0)
    lane = lax.broadcasted_iota(I32, shape, 1)
    shift = SRC_BLOCK.bit_length() - 1
    keys = []
    for v in range(count):
        src, dst = src_ref[8 * v : 8 * v + 8, :], dst_ref[8 * v : 8 * v + 8, :]
        block = lax.shift_right_logical(dst, 8) * src_blocks + lax.shift_right_logical(src, shift)
        packed = (block << 18) | ((dst & 255) << 10) | (src & (SRC_BLOCK - 1))
        keys.append(jnp.where(1024 * v + 128 * sub + lane < live_ref[0], packed, dead))
    bits = [None] * 4
    bits += [-(lax.shift_right_logical(sub, b) & 1) for b in range(3)]
    bits += [-(lax.shift_right_logical(lane, b) & 1) for b in range(7)]
    total = len(bits)

    def flips(k):
        if k == 0 or k == total:
            return [0] * count
        if k < 4:
            return [-((v >> k) & 1) for v in range(count)]
        return [bits[k]] * count

    for k in range(1, total + 1):
        for v, (old, new) in enumerate(zip(flips(k - 1), flips(k))):
            for flip in (old, new):
                if not isinstance(flip, int):
                    keys[v] = keys[v] ^ flip
                elif flip:
                    keys[v] = ~keys[v]
        for j in reversed(range(k)):
            if j < 4:
                for v in range(count):
                    if not (v >> j) & 1:
                        a, b = keys[v], keys[v | 1 << j]
                        keys[v], keys[v | 1 << j] = jnp.minimum(a, b), jnp.maximum(a, b)
                continue
            axis, step, size = (0, 1 << (j - 4), 8) if j < 7 else (1, 1 << (j - 7), 128)
            low = bits[j] == 0
            for v in range(count):
                key = keys[v]
                after = pltpu.roll(key, size - step, axis)
                before = after if 2 * step == size else pltpu.roll(key, step, axis)
                keys[v] = jnp.where(low, jnp.minimum(key, after), jnp.maximum(key, before))
    out_ref[...] = jnp.transpose(jnp.concatenate(keys, axis=0))


def sort_edges(live, src, dst, src_blocks, blocks):
    return pl.pallas_call(
        functools.partial(sort_body, src_blocks, blocks),
        out_shape=shape_of(src.shape, I32),
        in_specs=[whole(pltpu.SMEM), whole(), whole()],
        out_specs=whole(),
        compiler_params=limit(8),
        cost_estimate=cost(10**9, 2 * 10**5),
        name="sort_edges",
    )(live, src, dst)


def edges_body(src_blocks, starts_ref, keys_ref, count_ref, degree_ref, held_ref, acc_ref, sem):
    top = keys_ref.shape[0] - 1
    buckets = degree_ref.shape[1] // DST_BLOCK * src_blocks
    degree_ref[...] = jnp.zeros_like(degree_ref)
    ones = (lax.broadcasted_iota(I32, (16, 128 * KEY_ROWS), 0) == 0).astype(F32).astype(BF16)

    def block_of(bucket):
        tall = pl.multiple_of(lax.rem(bucket, src_blocks) * SRC_BLOCK, SRC_BLOCK)
        return bucket // src_blocks, pl.ds(tall, SRC_BLOCK)

    def flush(bucket):
        outer, tall = block_of(bucket)
        return pltpu.make_async_copy(held_ref.at[outer, tall], count_ref.at[outer, tall], sem)

    def products(bucket, row):
        wanted = jnp.where(bucket < buckets, bucket, -1)
        src, dst = [], []
        for i in range(KEY_ROWS):
            keys = keys_ref[pl.ds(jnp.minimum(row + i, top), 1), :]
            live = jnp.logical_and(lax.shift_right_logical(keys, 18) == wanted, row + i <= top)
            dst.append(jnp.where(live, lax.shift_right_logical(keys, 10) & 255, -1))
            src.append(keys & 1023)
        src, dst = jnp.concatenate(src, axis=1), jnp.concatenate(dst, axis=1)
        right = hot_rows(dst, DST_BLOCK)
        both = mm(jnp.concatenate([hot_rows(src, SRC_BLOCK), ones], axis=0), right, NT)
        return both[:SRC_BLOCK], both[SRC_BLOCK : SRC_BLOCK + 8]

    def store(bucket, fresh, parts, degree):
        last = jnp.minimum(bucket, buckets - 1)
        outer, _ = block_of(last)
        wide = pl.ds(pl.multiple_of(outer * DST_BLOCK, DST_BLOCK), DST_BLOCK)
        base = lax.rem(last, src_blocks) * SRC_BLOCK
        for i in range(SRC_BLOCK // 256):
            rows = slice(i * 256, (i + 1) * 256)
            total = parts[rows] + jnp.where(fresh, 0.0, acc_ref[rows, :])
            acc_ref[rows, :] = total
            tall = pl.ds(pl.multiple_of(base + i * 256, 256), 256)
            held_ref[outer, tall, :] = total.astype(BF16)
        degree_ref[:, wide] += degree

    def advance(bucket, row):
        last = starts_ref[jnp.minimum(bucket + 1, buckets)]
        ended = (row + KEY_ROWS) * 128 >= last
        after = jnp.minimum(bucket + ended.astype(I32), buckets)
        return after, jnp.where(ended, lax.shift_right_logical(starts_ref[after], 7), row + KEY_ROWS), ended

    def body(carry):
        bucket, row, fresh = carry
        visits = []
        for _ in range(VISITS):
            after, following, ended = advance(bucket, row)
            visits.append((bucket, row, fresh == 1, ended))
            bucket, row = after, following
            fresh = jnp.logical_and(ended, bucket < buckets).astype(I32)
        made = [products(*visit[:2]) for visit in visits]
        for visit, both in zip(visits, made):
            store(visit[0], visit[2], *both)
        for visit in visits:
            @pl.when(jnp.logical_and(visit[3], visit[0] < buckets))
            def _(visit=visit):
                flush(visit[0]).start()

        return bucket, row, fresh

    start = (jnp.int32(0), lax.shift_right_logical(starts_ref[0], 7), jnp.int32(1))
    lax.while_loop(lambda carry: carry[0] < buckets, body, start)
    pltpu.make_async_copy(held_ref, count_ref, sem).wait()


def edge_counts(starts, keys, nodes, table):
    blocks = nodes // DST_BLOCK
    return pl.pallas_call(
        functools.partial(edges_body, table // SRC_BLOCK),
        out_shape=(pltpu.HBM((blocks, table, DST_BLOCK), BF16), shape_of((8, nodes), F32)),
        in_specs=[whole(pltpu.SMEM), whole()],
        out_specs=(whole(pltpu.HBM), whole()),
        scratch_shapes=[
            pltpu.VMEM((blocks, table, DST_BLOCK), BF16),
            pltpu.VMEM((SRC_BLOCK, DST_BLOCK), F32),
            pltpu.SemaphoreType.DMA,
        ],
        compiler_params=limit(EDGES_MIB),
        cost_estimate=cost(14 * 10**9, 13 * 10**6),
        name="edge_counts",
    )(starts, keys)


def embed_body(
    count_ref, arrived_ref, feat_ref, degree_ref, self_ref, neigh_ref,
    served_ref, agg_ref, want_ref, held_ref, table_ref, mean_ref, emb_ref, sems,
):
    blocks = count_ref.shape[0]
    copies = [pltpu.make_async_copy(count_ref.at[i], held_ref.at[i], sems.at[i]) for i in range(blocks)]
    for copy in copies:
        copy.start()
    nodes = feat_ref.shape[0]
    table_ref[:, :nodes] = jnp.transpose(feat_ref[...])
    arrived = arrived_ref[...].astype(F32)
    for half in range(2):
        halo = arrived[:, 8 * half : 8 * half + 8, :].reshape(-1, 128).astype(BF16)
        table_ref[128 * half : 128 * half + 128, nodes:] = jnp.transpose(halo)
    notes = arrived[:, 16:, :]
    grouped = notes.reshape(notes.shape[0] // 8, 8, 8, notes.shape[2])
    summed = jnp.sum(grouped, axis=1)
    want = (summed[:, 0, :] * 128.0 + summed[:, 4, :]).astype(I32)
    want_ref[...] = want
    columns = jnp.transpose(want)
    def node_block(i, carry):
        span = pl.ds(pl.multiple_of(i * DST_BLOCK, DST_BLOCK), DST_BLOCK)
        pltpu.make_async_copy(count_ref.at[i], held_ref.at[i], sems.at[i]).wait()
        sums = mm(table_ref[...], held_ref[i])
        degree = jnp.sum(degree_ref[:, span], axis=0, keepdims=True)
        mean_ref[:, span] = (sums / jnp.maximum(degree, 1.0)).astype(BF16)
        return carry

    lax.fori_loop(0, nodes // DST_BLOCK, node_block, 0)
    agg_ref[...] = jnp.transpose(mean_ref[...])
    for at in range(0, nodes, 1024):
        span = slice(at, at + 1024)
        both = mm(feat_ref[span, :], self_ref[...]) + mm(agg_ref[span, :], neigh_ref[...])
        emb_ref[span, :] = both.astype(BF16)
    for k in range(0, columns.shape[1], 8):
        tiles = [jnp.broadcast_to(columns[:, i : i + 1], (128, 128)) for i in range(k, k + 8)]
        hot = hot_tile(jnp.concatenate(tiles, axis=0), nodes)
        served_ref[k * 128 : (k + 8) * 128, :] = mm(hot, emb_ref[...]).astype(BF16)


def embed(counts, arrived, features, degree, w_self, w_neigh):
    blocks, table, _ = counts.shape
    nodes, width = features.shape
    return pl.pallas_call(
        embed_body,
        out_shape=(
            shape_of((nodes, width), BF16),
            shape_of((nodes, width), BF16),
            shape_of((16, 128), I32),
        ),
        in_specs=[whole(pltpu.HBM)] + [whole()] * 5,
        out_specs=(whole(),) * 3,
        scratch_shapes=[
            pltpu.VMEM(counts.shape, BF16),
            pltpu.VMEM((width, table), BF16),
            pltpu.VMEM((width, nodes), BF16),
            pltpu.VMEM((nodes, width), BF16),
            pltpu.SemaphoreType.DMA((blocks,)),
        ],
        compiler_params=limit(EMBED_MIB),
        cost_estimate=cost(6 * 10**9, 16 * 10**6),
        name="embed",
    )(counts, arrived, features, degree, w_self, w_neigh)


def decode_body(
    got_ref, ends_ref, label_ref, weight_ref, hid_ref, bias_ref, wout_ref,
    logit_ref, send_ref, both_ref, delta_ref, grad_ref, hidden_ref,
):
    rows, width = got_ref.shape
    pairs = ends_ref.shape[1]
    block = 512
    wide = 1024
    meta = jnp.concatenate(
        [
            ends_ref[...].astype(F32),
            label_ref[...].astype(F32),
            weight_ref[...],
            jnp.zeros((4, pairs), F32),
        ],
        axis=0,
    )
    cols = jnp.transpose(meta)
    ends = cols.astype(I32)
    for side in range(2):
        for at in range(0, pairs, wide):
            tile = jnp.broadcast_to(ends[at : at + wide, side : side + 1], (wide, 128))
            picked = mm(hot_tile(tile, rows), got_ref[...])
            both_ref[at : at + wide, side * width : (side + 1) * width] = picked.astype(BF16)
    bias_sum = jnp.zeros((8, width), F32)
    wout_sum = jnp.zeros((8, width), F32)
    for at in range(0, pairs, block):
        span = slice(at, at + block)
        pre = mm(both_ref[span, :], hid_ref[...]) + bias_ref[...]
        hidden = jnp.maximum(pre, 0.0)
        logits = jnp.sum(hidden * wout_ref[...], axis=1, keepdims=True)
        logit_ref[:, span] = jnp.transpose(jnp.broadcast_to(logits, (block, 128)))[0:1, :]
        slope = cols[span, 3:4] * (jax.nn.sigmoid(logits) - cols[span, 2:3])
        delta = jnp.where(pre > 0, slope * wout_ref[...], 0.0)
        bias_sum += jnp.sum(delta.reshape(block // 8, 8, width), axis=0)
        wout_sum += jnp.sum((slope * hidden).reshape(block // 8, 8, width), axis=0)
        delta = delta.astype(BF16)
        delta_ref[span, :] = delta
        grad_ref[span, :] = mm(delta, hid_ref[...], NT).astype(BF16)
    for at in range(0, rows, wide):
        grad = mm(hot_rows(ends_ref[0:1, :] - at, wide), grad_ref[:, :width])
        grad += mm(hot_rows(ends_ref[1:2, :] - at, wide), grad_ref[:, width:])
        send_ref[at // 16 : (at + wide) // 16, 0:16, :] = grad.reshape(-1, 16, width).astype(BF16)
    hidden_ref[...] = mm(both_ref[...], delta_ref[...], TN)
    bias = jnp.sum(bias_sum, axis=0, keepdims=True)
    wout = jnp.sum(wout_sum, axis=0, keepdims=True)
    lines = []
    for line in (bias, wout):
        high = line.astype(BF16).astype(F32)
        for half in (high, line - high):
            lines += [half[:, :128], half[:, 128:]]
    tail = jnp.concatenate(lines, axis=0)
    total = hidden_ref[...].reshape(-1, 8, width)
    tail = jnp.broadcast_to(tail[None], (total.shape[0], 8, 128))
    even = jnp.concatenate([total[:, :, :128], tail], axis=2)
    odd = jnp.concatenate([total[:, :, 128:], tail], axis=2)
    joined = jnp.stack([even, odd], axis=1).reshape(-1, 8, width)
    send_ref[:, 16:24, :] = joined.astype(BF16)


def decode(got, ends, labels, weights, w_hidden, bias, w_out, parts):
    rows, width = got.shape
    pairs = ends.shape[1]
    return pl.pallas_call(
        decode_body,
        out_shape=(shape_of((1, pairs), F32), shape_of((parts, 24, width), BF16)),
        in_specs=[whole()] * 7,
        out_specs=(whole(), whole()),
        scratch_shapes=[
            pltpu.VMEM((pairs, 2 * width), BF16),
            pltpu.VMEM((pairs, width), BF16),
            pltpu.VMEM((pairs, 2 * width), BF16),
            pltpu.VMEM((2 * width, width), F32),
        ],
        compiler_params=limit(DECODE_MIB),
        cost_estimate=cost(10 * 10**9, 4 * 10**6),
        name="decode",
    )(got, ends, labels, weights, w_hidden, bias, w_out)


def spread_body(
    count_ref, back_ref, want_ref, feat_ref, agg_ref, degree_ref, neigh_ref,
    send_hbm, small_ref, grad_hbm, mean_hbm, send_ref, grad_ref, mean_ref, held_ref, sem, out_sems,
):
    nodes, width = feat_ref.shape
    rows = 1024
    copy = pltpu.make_async_copy(count_ref.at[:, nodes : nodes + held_ref.shape[1]], held_ref, sem)
    copy.start()
    back = back_ref[...].astype(F32)
    tail = jnp.sum(back[:, 16:, :], axis=0)
    small_ref[...] = tail[:, 128:]
    flat = back[:, :16, :].reshape(-1, width).astype(BF16)
    want = jnp.concatenate([want_ref[k : k + 1, :] for k in range(16)], axis=1)

    def gather(i, carry):
        at = i * rows
        span = pl.ds(pl.multiple_of(at, rows), rows)
        grad_ref[span, :] = mm(hot_rows(want - at, rows), flat).astype(BF16)
        return carry

    lax.fori_loop(0, nodes // rows, gather, 0)

    def scale(i, carry):
        span = pl.ds(pl.multiple_of(i * 256, 256), 256)
        degree = jnp.sum(degree_ref[:, span], axis=0, keepdims=True)
        column = jnp.transpose(jnp.broadcast_to(jnp.maximum(degree, 1.0), (128, 256)))
        scaled = mm(grad_ref[span, :], neigh_ref[...], NT) / jnp.concatenate([column, column], axis=1)
        mean_ref[span, :] = scaled.astype(BF16)
        return carry

    lax.fori_loop(0, nodes // 256, scale, 0, unroll=2)
    halves = [(slice(None), slice(0, 8)), (slice(None), slice(8, 16))]
    pairs = [(send_ref.at[half], send_hbm.at[half]) for half in halves]
    pairs += [(grad_ref, grad_hbm), (mean_ref, mean_hbm)]
    leaving = [pltpu.make_async_copy(*pair, out_sems.at[i]) for i, pair in enumerate(pairs)]
    leaving[2].start()
    leaving[3].start()
    both = jnp.concatenate(
        [mm(feat_ref[...], grad_ref[...], TN), mm(agg_ref[...], grad_ref[...], TN)], axis=0
    )
    both = both.reshape(-1, 8, width)
    tail = jnp.broadcast_to(tail[None, :, :128], (both.shape[0], 8, 128))
    even = jnp.concatenate([both[:, :, :128], tail], axis=2)
    odd = jnp.concatenate([both[:, :, 128:], tail], axis=2)
    joined = jnp.stack([even, odd], axis=1).reshape(-1, 8, width)
    send_ref[:, 8:16, :] = joined.astype(BF16)
    leaving[1].start()
    copy.wait()
    blocks = range(0, nodes, DST_BLOCK)
    parts = [mm(held_ref[n // DST_BLOCK], mean_ref[n : n + DST_BLOCK, :]) for n in blocks]
    grad = sum(parts[1:], parts[0]).reshape(-1, 8, width)
    send_ref[:, 0:8, :] = grad.astype(BF16)
    leaving[0].start()
    for copy in leaving:
        copy.wait()


def spread(counts, back, want, features, agg, degree, w_neigh):
    blocks, table, _ = counts.shape
    nodes, width = features.shape
    return pl.pallas_call(
        spread_body,
        out_shape=(
            pltpu.HBM((back.shape[0], 16, width), BF16),
            shape_of((8, 128), F32),
            pltpu.HBM((nodes, width), BF16),
            pltpu.HBM((nodes, width), BF16),
        ),
        in_specs=[whole(pltpu.HBM)] + [whole()] * 6,
        out_specs=(whole(pltpu.HBM), whole(), whole(pltpu.HBM), whole(pltpu.HBM)),
        scratch_shapes=[
            pltpu.VMEM((back.shape[0], 16, width), BF16),
            pltpu.VMEM((nodes, width), BF16),
            pltpu.VMEM((nodes, width), BF16),
            pltpu.VMEM((blocks, table - nodes, DST_BLOCK), BF16),
            pltpu.SemaphoreType.DMA,
            pltpu.SemaphoreType.DMA((4,)),
        ],
        compiler_params=limit(SPREAD_MIB),
        cost_estimate=cost(5 * 10**9, 10 * 10**6),
        name="spread",
    )(counts, back, want, features, agg, degree, w_neigh)


def direct_body(count_ref, grad_ref, mean_ref, self_ref, out_ref, held_ref, sems):
    nodes = out_ref.shape[0]
    rows = 512

    def fetch(i):
        span = pl.ds(pl.multiple_of(i * rows, rows), rows)
        return pltpu.make_async_copy(count_ref.at[:, span], held_ref.at[:, span], sems.at[i])

    for i in range(nodes // rows):
        fetch(i).start()

    def own(i, carry):
        span = pl.ds(pl.multiple_of(i * rows, rows), rows)
        blocks = range(0, nodes, DST_BLOCK)
        total = mm(grad_ref[span, :], self_ref[...], NT)
        fetch(i).wait()
        parts = [mm(held_ref[n // DST_BLOCK, span, :], mean_ref[n : n + DST_BLOCK, :]) for n in blocks]
        out_ref[span, :] = sum(parts[1:], parts[0]) + total
        return carry

    lax.fori_loop(0, nodes // rows, own, 0)


def direct_rows(counts, grad, mean, w_self):
    nodes, width = grad.shape
    return pl.pallas_call(
        direct_body,
        out_shape=pltpu.HBM((nodes, width), F32),
        in_specs=[whole(pltpu.HBM)] + [whole()] * 3,
        out_specs=whole(),
        scratch_shapes=[
            pltpu.VMEM((counts.shape[0], nodes, DST_BLOCK), BF16),
            pltpu.SemaphoreType.DMA((nodes // 512,)),
        ],
        compiler_params=limit(DIRECT_MIB),
        cost_estimate=cost(3 * 10**9, 12 * 10**6),
        name="direct_rows",
    )(counts, grad, mean, w_self)


def chunk_body(back_ref, direct_ref, out_ref):
    del direct_ref
    tail = jnp.sum(back_ref[:, 8:, :].astype(F32), axis=0)[:, :128]
    out_ref[...] = jnp.broadcast_to(tail[None], out_ref.shape).astype(BF16)


def chunk(back, direct):
    return pl.pallas_call(
        chunk_body,
        out_shape=shape_of((back.shape[0], 8, 128), BF16),
        in_specs=[whole(), whole(pltpu.HBM)],
        out_specs=whole(),
        compiler_params=limit(CHUNK_MIB),
        cost_estimate=cost(10**6, 10**6),
        name="chunk",
    )(back, direct)


def join_lanes(pieces):
    pieces = pieces.reshape(-1, 2, 8, 128)
    return jnp.concatenate([pieces[:, 0], pieces[:, 1]], axis=2).reshape(-1, 256)


def final_body(
    direct_ref, back_ref, halo_ref, small_ref, out_ref, hidden_ref, bias_ref, wout_ref, held_ref, sems
):
    rows = 512
    copies = []
    for i in range(out_ref.shape[0] // rows):
        part = slice(i * rows, (i + 1) * rows)
        copies.append(pltpu.make_async_copy(direct_ref.at[part], held_ref.at[part], sems.at[i]))
        copies[-1].start()
    back = back_ref[...].astype(F32)
    width = back.shape[2]
    flat = back[:, :8, :].reshape(-1, width).astype(BF16)
    halo = jnp.concatenate([halo_ref[k : k + 1, :] for k in range(8)], axis=1)

    def add(i, carry):
        part = pl.ds(pl.multiple_of(i * rows, rows), rows)
        extra = mm(hot_rows(halo - i * rows, rows), flat)
        pltpu.make_async_copy(direct_ref.at[part], held_ref.at[part], sems.at[i]).wait()
        out_ref[part, :] = held_ref[part, :] + extra
        return carry

    lax.fori_loop(0, len(copies), add, 0)
    hidden_ref[...] = join_lanes(back[:, 8:, 128:])
    bias_ref[...] = small_ref[0:2, :] + small_ref[2:4, :]
    wout_ref[...] = small_ref[4:6, :] + small_ref[6:8, :]


def final(direct, back, halo, small):
    nodes, width = direct.shape
    return pl.pallas_call(
        final_body,
        out_shape=(
            shape_of((nodes, width), F32),
            shape_of((2 * width, width), F32),
            shape_of((2, 128), F32),
            shape_of((2, 128), F32),
        ),
        in_specs=[whole(pltpu.HBM)] + [whole()] * 3,
        out_specs=(whole(),) * 4,
        scratch_shapes=[
            pltpu.VMEM((nodes, width), F32),
            pltpu.SemaphoreType.DMA((nodes // 512,)),
        ],
        compiler_params=limit(FINAL_MIB),
        cost_estimate=cost(2 * 10**9, 6 * 10**6),
        name="final",
    )(direct, back, halo, small)


def weights_body(pieces_ref, self_ref, neigh_ref):
    both = join_lanes(pieces_ref[...].astype(F32))
    half = both.shape[0] // 2
    self_ref[...] = both[:half, :]
    neigh_ref[...] = both[half:, :]


def weights(pieces):
    shape = shape_of((256, 256), F32)
    return pl.pallas_call(
        weights_body,
        out_shape=(shape, shape),
        in_specs=[whole()],
        out_specs=(whole(), whole()),
        compiler_params=limit(WEIGHTS_MIB),
        cost_estimate=cost(10**6, 10**6),
        name="weights",
    )(pieces)


def exchange(rows):
    return lax.all_to_all(rows, AXES, split_axis=0, concat_axis=0, tiled=True)


def per_device(
    features, edge_src, edge_dst, edge_count, halo_index, request_rows, pair_ends,
    labels, pair_weight, w_self, w_neigh, w_hidden, b_hidden, w_out,
):
    nodes, width = features.shape
    parts, halo_len = halo_index.shape[1:]
    table = nodes + parts * halo_len
    slots = edge_src.shape[0]
    me = lax.axis_index("dom") * lax.axis_size("grp") + lax.axis_index("grp")

    held = [pltpu.with_memory_space_constraint(x, pltpu.HBM) for x in (halo_index[0].T, request_rows[0].T, features)]
    sent = send_rows((me % 8).reshape(1), *held)
    arrived = exchange(sent)

    src_blocks = table // SRC_BLOCK
    buckets = nodes // DST_BLOCK * src_blocks
    square = (slots // 128, 128)
    keys = sort_edges(edge_count, edge_src.reshape(square), edge_dst.reshape(square), src_blocks, buckets)
    bounds = jnp.arange(buckets + 1, dtype=I32) << 18
    starts = jnp.sum((keys.reshape(1, -1) < bounds[:, None]).astype(I32), axis=1)
    counts, degree = edge_counts(starts, keys, nodes, table)

    fixed = pltpu.with_memory_space_constraint(counts, pltpu.HBM)
    served, agg, want = embed(fixed, arrived, features, degree, w_self, w_neigh)
    got = exchange(served.reshape(parts, -1, width)).reshape(-1, width)
    logits, pair_back = decode(
        got, pair_ends.T, labels.reshape(1, -1), pair_weight.reshape(1, -1),
        w_hidden, b_hidden.reshape(1, -1), w_out.reshape(1, -1), parts,
    )
    back = exchange(pair_back)
    halo_back, small, grad, mean = spread(fixed, back, want, features, agg, degree, w_neigh)
    returned = exchange(halo_back)
    direct = direct_rows(fixed, grad, mean, w_self)
    direct = pltpu.with_memory_space_constraint(direct, pltpu.HBM)
    pieces = exchange(chunk(returned, direct))
    grad_features, grad_hidden, grad_bias, grad_out = final(
        direct, returned, halo_index[0].reshape(8, -1), small
    )
    grad_self, grad_neigh = weights(pieces)
    return (
        logits.reshape(-1), grad_features, grad_self, grad_neigh, grad_hidden,
        grad_bias.reshape(-1), grad_out.reshape(-1),
    )


def solution(mesh):
    split, rows, cubes = P(AXES), P(AXES, None), P(AXES, None, None)
    in_specs = (
        rows, split, split, split, cubes, cubes, rows, split, split, P(), P(), P(), P(), P(),
    )
    out_specs = (split, rows, P(), P(), P(), P(), P())
    return jax.shard_map(
        per_device, mesh=mesh, in_specs=in_specs, out_specs=out_specs, check_vma=False
    )
```

```python
import functools

import jax
import jax.numpy as jnp
from jax import lax
from jax.experimental import pallas as pl
from jax.experimental.pallas import tpu as pltpu
from jax.sharding import PartitionSpec as P

BF16, F32, I16, I32 = jnp.bfloat16, jnp.float32, jnp.int16, jnp.int32
NN = (((1,), (0,)), ((), ()))
NT = (((1,), (1,)), ((), ()))
TN = (((0,), (0,)), ((), ()))
AXES = ("dom", "grp")
DST_BLOCK = 256
SRC_BLOCK = 256
VISITS = 8
KEY_ROWS = 2
UNROLL = 2
SEND_MIB, EDGES_MIB, EMBED_MIB, DECODE_MIB, SPREAD_MIB = 8, 24, 24, 16, 16
DIRECT_MIB = 16
CHUNK_MIB, FINAL_MIB, WEIGHTS_MIB = 8, 16, 8


def limit(mib):
    return pltpu.CompilerParams(vmem_limit_bytes=mib * 1024 * 1024)


def mm(left, right, dims=NN):
    return lax.dot_general(left, right, dims, preferred_element_type=F32)


def spread_hot(diff, step, count, axis):
    one, zero = jnp.ones((), BF16), jnp.zeros((), BF16)
    pieces = [jnp.where(diff == jnp.int16(step * k), one, zero) for k in range(count)]
    return jnp.concatenate(pieces, axis=axis)


def hot_rows(row, height):
    width = row.shape[1]
    wide = jnp.broadcast_to(row, (16, width)) - lax.broadcasted_iota(I32, (16, width), 0)
    return spread_hot(wide.astype(I16), 16, height // 16, 0)


def lane_diff(tile):
    return (tile - lax.broadcasted_iota(I32, tile.shape, 1)).astype(I16)


def hot_lanes(diff, width):
    return spread_hot(diff, 128, width // 128, 1)


def hot_tile(tile, width):
    return hot_lanes(lane_diff(tile), width)


def whole(memory_space=pltpu.VMEM):
    return pl.BlockSpec(memory_space=memory_space)


def shape_of(shape, dtype):
    return jax.ShapeDtypeStruct(shape, dtype)


def cost(flops, moved):
    return pl.CostEstimate(flops=flops, bytes_accessed=moved, transcendentals=0)


def send_body(slot_ref, halo_hbm, want_hbm, feat_hbm, out_ref, halo_ref, want_ref, feat_ref, sems):
    pairs = ((halo_hbm, halo_ref), (want_hbm, want_ref), (feat_hbm, feat_ref))
    copies = [pltpu.make_async_copy(*pair, sems.at[i]) for i, pair in enumerate(pairs)]
    for copy in copies:
        copy.start()
    copies[0].wait()
    copies[1].wait()
    parts = out_ref.shape[0]
    want = jnp.transpose(want_ref[...])
    tiled = jnp.concatenate([want] * 8, axis=1)
    lane = lax.broadcasted_iota(I32, tiled.shape, 1)
    mine = lax.shift_right_logical(lane, 4) == slot_ref[0]
    tiled = jnp.where(mine, tiled, 0)
    high, low = lax.shift_right_logical(tiled, 7).astype(F32), (tiled & 127).astype(F32)
    halo = halo_ref[...]
    tiles = [jnp.broadcast_to(halo[:, p : p + 1], (8, 128)) for p in range(parts)]
    diff = lane_diff(jnp.concatenate(tiles, axis=0))
    copies[2].wait()
    rows = mm(hot_lanes(diff, feat_ref.shape[0]), feat_ref[...])
    rows = rows.reshape(parts, 8, rows.shape[1])
    upper = lax.broadcasted_iota(I32, (parts, 8, 128), 1) < 4
    notes = jnp.where(upper, high[:, None, :], low[:, None, :])
    out_ref[...] = jnp.concatenate([rows[:, :, :128], rows[:, :, 128:], notes], axis=1).astype(BF16)


def send_rows(slot, halo, want, features):
    parts = want.shape[1]
    return pl.pallas_call(
        send_body,
        out_shape=shape_of((parts, 24, 128), BF16),
        in_specs=[whole(pltpu.SMEM)] + [whole(pltpu.HBM)] * 3,
        out_specs=whole(),
        scratch_shapes=[
            pltpu.VMEM(halo.shape, I32),
            pltpu.VMEM(want.shape, I32),
            pltpu.VMEM(features.shape, BF16),
            pltpu.SemaphoreType.DMA((3,)),
        ],
        compiler_params=limit(SEND_MIB),
        cost_estimate=cost(10**9, 2 * 10**6),
        name="send_rows",
    )(slot, halo, want, features)


def sort_body(src_blocks, blocks, live_ref, src_ref, dst_ref, out_ref):
    shape = (8, 128)
    count = src_ref.shape[0] // 8
    dead = blocks << 18
    sub = lax.broadcasted_iota(I32, shape, 0)
    lane = lax.broadcasted_iota(I32, shape, 1)
    shift = SRC_BLOCK.bit_length() - 1
    keys = []
    for v in range(count):
        src, dst = src_ref[8 * v : 8 * v + 8, :], dst_ref[8 * v : 8 * v + 8, :]
        block = lax.shift_right_logical(dst, 8) * src_blocks + lax.shift_right_logical(src, shift)
        packed = (block << 18) | ((dst & 255) << 10) | (src & (SRC_BLOCK - 1))
        keys.append(jnp.where(1024 * v + 128 * sub + lane < live_ref[0], packed, dead))
    bits = [None] * 4
    bits += [-(lax.shift_right_logical(sub, b) & 1) for b in range(3)]
    bits += [-(lax.shift_right_logical(lane, b) & 1) for b in range(7)]
    total = len(bits)

    def flips(k):
        if k == 0 or k == total:
            return [0] * count
        if k < 4:
            return [-((v >> k) & 1) for v in range(count)]
        return [bits[k]] * count

    for k in range(1, total + 1):
        for v, (old, new) in enumerate(zip(flips(k - 1), flips(k))):
            for flip in (old, new):
                if not isinstance(flip, int):
                    keys[v] = keys[v] ^ flip
                elif flip:
                    keys[v] = ~keys[v]
        for j in reversed(range(k)):
            if j < 4:
                for v in range(count):
                    if not (v >> j) & 1:
                        a, b = keys[v], keys[v | 1 << j]
                        keys[v], keys[v | 1 << j] = jnp.minimum(a, b), jnp.maximum(a, b)
                continue
            axis, step, size = (0, 1 << (j - 4), 8) if j < 7 else (1, 1 << (j - 7), 128)
            low = bits[j] == 0
            for v in range(count):
                key = keys[v]
                after = pltpu.roll(key, size - step, axis)
                before = after if 2 * step == size else pltpu.roll(key, step, axis)
                keys[v] = jnp.where(low, jnp.minimum(key, after), jnp.maximum(key, before))
    out_ref[...] = jnp.transpose(jnp.concatenate(keys, axis=0))


def sort_edges(live, src, dst, src_blocks, blocks):
    return pl.pallas_call(
        functools.partial(sort_body, src_blocks, blocks),
        out_shape=shape_of(src.shape, I32),
        in_specs=[whole(pltpu.SMEM), whole(), whole()],
        out_specs=whole(),
        compiler_params=limit(8),
        cost_estimate=cost(10**9, 2 * 10**5),
        name="sort_edges",
    )(live, src, dst)


def edges_body(src_blocks, starts_ref, keys_ref, count_ref, degree_ref, held_ref, acc_ref, sem):
    top = keys_ref.shape[0] - 1
    buckets = degree_ref.shape[1] // DST_BLOCK * src_blocks
    degree_ref[...] = jnp.zeros_like(degree_ref)
    ones = (lax.broadcasted_iota(I32, (16, 128 * KEY_ROWS), 0) == 0).astype(F32).astype(BF16)

    def block_of(bucket):
        tall = pl.multiple_of(lax.rem(bucket, src_blocks) * SRC_BLOCK, SRC_BLOCK)
        return bucket // src_blocks, pl.ds(tall, SRC_BLOCK)

    def flush(bucket):
        outer, tall = block_of(bucket)
        return pltpu.make_async_copy(held_ref.at[outer, tall], count_ref.at[outer, tall], sem)

    def products(bucket, row):
        wanted = jnp.where(bucket < buckets, bucket, -1)
        src, dst = [], []
        for i in range(KEY_ROWS):
            keys = keys_ref[pl.ds(jnp.minimum(row + i, top), 1), :]
            live = jnp.logical_and(lax.shift_right_logical(keys, 18) == wanted, row + i <= top)
            dst.append(jnp.where(live, lax.shift_right_logical(keys, 10) & 255, -1))
            src.append(keys & 1023)
        src, dst = jnp.concatenate(src, axis=1), jnp.concatenate(dst, axis=1)
        right = hot_rows(dst, DST_BLOCK)
        both = mm(jnp.concatenate([hot_rows(src, SRC_BLOCK), ones], axis=0), right, NT)
        return both[:SRC_BLOCK], both[SRC_BLOCK : SRC_BLOCK + 8]

    def store(bucket, fresh, parts, degree):
        last = jnp.minimum(bucket, buckets - 1)
        outer, _ = block_of(last)
        wide = pl.ds(pl.multiple_of(outer * DST_BLOCK, DST_BLOCK), DST_BLOCK)
        base = lax.rem(last, src_blocks) * SRC_BLOCK
        for i in range(SRC_BLOCK // 256):
            rows = slice(i * 256, (i + 1) * 256)
            total = parts[rows] + jnp.where(fresh, 0.0, acc_ref[rows, :])
            acc_ref[rows, :] = total
            tall = pl.ds(pl.multiple_of(base + i * 256, 256), 256)
            held_ref[outer, tall, :] = total.astype(BF16)
        degree_ref[:, wide] += degree

    def advance(bucket, row):
        last = starts_ref[jnp.minimum(bucket + 1, buckets)]
        ended = (row + KEY_ROWS) * 128 >= last
        after = jnp.minimum(bucket + ended.astype(I32), buckets)
        return after, jnp.where(ended, lax.shift_right_logical(starts_ref[after], 7), row + KEY_ROWS), ended

    def body(carry):
        bucket, row, fresh = carry
        visits = []
        for _ in range(VISITS):
            after, following, ended = advance(bucket, row)
            visits.append((bucket, row, fresh == 1, ended))
            bucket, row = after, following
            fresh = jnp.logical_and(ended, bucket < buckets).astype(I32)
        made = [products(*visit[:2]) for visit in visits]
        for visit, both in zip(visits, made):
            store(visit[0], visit[2], *both)
        for visit in visits:
            @pl.when(jnp.logical_and(visit[3], visit[0] < buckets))
            def _(visit=visit):
                flush(visit[0]).start()

        return bucket, row, fresh

    start = (jnp.int32(0), lax.shift_right_logical(starts_ref[0], 7), jnp.int32(1))
    lax.while_loop(lambda carry: carry[0] < buckets, body, start)
    pltpu.make_async_copy(held_ref, count_ref, sem).wait()


def edge_counts(starts, keys, nodes, table):
    blocks = nodes // DST_BLOCK
    return pl.pallas_call(
        functools.partial(edges_body, table // SRC_BLOCK),
        out_shape=(pltpu.HBM((blocks, table, DST_BLOCK), BF16), shape_of((8, nodes), F32)),
        in_specs=[whole(pltpu.SMEM), whole()],
        out_specs=(whole(pltpu.HBM), whole()),
        scratch_shapes=[
            pltpu.VMEM((blocks, table, DST_BLOCK), BF16),
            pltpu.VMEM((SRC_BLOCK, DST_BLOCK), F32),
            pltpu.SemaphoreType.DMA,
        ],
        compiler_params=limit(EDGES_MIB),
        cost_estimate=cost(14 * 10**9, 13 * 10**6),
        name="edge_counts",
    )(starts, keys)


def embed_body(
    count_ref, arrived_ref, feat_ref, degree_ref, self_ref, neigh_ref,
    served_ref, agg_ref, want_ref, held_ref, table_ref, mean_ref, emb_ref, sems,
):
    blocks = count_ref.shape[0]
    copies = [pltpu.make_async_copy(count_ref.at[i], held_ref.at[i], sems.at[i]) for i in range(blocks)]
    for copy in copies:
        copy.start()
    nodes = feat_ref.shape[0]
    table_ref[:, :nodes] = jnp.transpose(feat_ref[...])
    arrived = arrived_ref[...].astype(F32)
    for half in range(2):
        halo = arrived[:, 8 * half : 8 * half + 8, :].reshape(-1, 128).astype(BF16)
        table_ref[128 * half : 128 * half + 128, nodes:] = jnp.transpose(halo)
    notes = arrived[:, 16:, :]
    grouped = notes.reshape(notes.shape[0] // 8, 8, 8, notes.shape[2])
    summed = jnp.sum(grouped, axis=1)
    want = (summed[:, 0, :] * 128.0 + summed[:, 4, :]).astype(I32)
    want_ref[...] = want
    columns = jnp.transpose(want)
    def node_block(i, carry):
        span = pl.ds(pl.multiple_of(i * DST_BLOCK, DST_BLOCK), DST_BLOCK)
        pltpu.make_async_copy(count_ref.at[i], held_ref.at[i], sems.at[i]).wait()
        sums = mm(table_ref[...], held_ref[i])
        degree = jnp.sum(degree_ref[:, span], axis=0, keepdims=True)
        mean_ref[:, span] = (sums / jnp.maximum(degree, 1.0)).astype(BF16)
        return carry

    lax.fori_loop(0, nodes // DST_BLOCK, node_block, 0)
    agg_ref[...] = jnp.transpose(mean_ref[...])
    for at in range(0, nodes, 1024):
        span = slice(at, at + 1024)
        both = mm(feat_ref[span, :], self_ref[...]) + mm(agg_ref[span, :], neigh_ref[...])
        emb_ref[span, :] = both.astype(BF16)
    for k in range(0, columns.shape[1], 8):
        tiles = [jnp.broadcast_to(columns[:, i : i + 1], (128, 128)) for i in range(k, k + 8)]
        hot = hot_tile(jnp.concatenate(tiles, axis=0), nodes)
        served_ref[k * 128 : (k + 8) * 128, :] = mm(hot, emb_ref[...]).astype(BF16)


def embed(counts, arrived, features, degree, w_self, w_neigh):
    blocks, table, _ = counts.shape
    nodes, width = features.shape
    return pl.pallas_call(
        embed_body,
        out_shape=(
            shape_of((nodes, width), BF16),
            shape_of((nodes, width), BF16),
            shape_of((16, 128), I32),
        ),
        in_specs=[whole(pltpu.HBM)] + [whole()] * 5,
        out_specs=(whole(),) * 3,
        scratch_shapes=[
            pltpu.VMEM(counts.shape, BF16),
            pltpu.VMEM((width, table), BF16),
            pltpu.VMEM((width, nodes), BF16),
            pltpu.VMEM((nodes, width), BF16),
            pltpu.SemaphoreType.DMA((blocks,)),
        ],
        compiler_params=limit(EMBED_MIB),
        cost_estimate=cost(6 * 10**9, 16 * 10**6),
        name="embed",
    )(counts, arrived, features, degree, w_self, w_neigh)


def decode_body(
    got_ref, ends_ref, label_ref, weight_ref, hid_ref, bias_ref, wout_ref,
    logit_ref, send_ref, both_ref, delta_ref, grad_ref, hidden_ref,
):
    rows, width = got_ref.shape
    pairs = ends_ref.shape[1]
    block = 512
    wide = 1024
    meta = jnp.concatenate(
        [
            ends_ref[...].astype(F32),
            label_ref[...].astype(F32),
            weight_ref[...],
            jnp.zeros((4, pairs), F32),
        ],
        axis=0,
    )
    cols = jnp.transpose(meta)
    ends = cols.astype(I32)
    for side in range(2):
        for at in range(0, pairs, wide):
            tile = jnp.broadcast_to(ends[at : at + wide, side : side + 1], (wide, 128))
            picked = mm(hot_tile(tile, rows), got_ref[...])
            both_ref[at : at + wide, side * width : (side + 1) * width] = picked.astype(BF16)
    bias_sum = jnp.zeros((8, width), F32)
    wout_sum = jnp.zeros((8, width), F32)
    for at in range(0, pairs, block):
        span = slice(at, at + block)
        pre = mm(both_ref[span, :], hid_ref[...]) + bias_ref[...]
        hidden = jnp.maximum(pre, 0.0)
        logits = jnp.sum(hidden * wout_ref[...], axis=1, keepdims=True)
        logit_ref[:, span] = jnp.transpose(jnp.broadcast_to(logits, (block, 128)))[0:1, :]
        slope = cols[span, 3:4] * (jax.nn.sigmoid(logits) - cols[span, 2:3])
        delta = jnp.where(pre > 0, slope * wout_ref[...], 0.0)
        bias_sum += jnp.sum(delta.reshape(block // 8, 8, width), axis=0)
        wout_sum += jnp.sum((slope * hidden).reshape(block // 8, 8, width), axis=0)
        delta = delta.astype(BF16)
        delta_ref[span, :] = delta
        grad_ref[span, :] = mm(delta, hid_ref[...], NT).astype(BF16)
    for at in range(0, rows, wide):
        grad = mm(hot_rows(ends_ref[0:1, :] - at, wide), grad_ref[:, :width])
        grad += mm(hot_rows(ends_ref[1:2, :] - at, wide), grad_ref[:, width:])
        send_ref[at // 16 : (at + wide) // 16, 0:16, :] = grad.reshape(-1, 16, width).astype(BF16)
    hidden_ref[...] = mm(both_ref[...], delta_ref[...], TN)
    bias = jnp.sum(bias_sum, axis=0, keepdims=True)
    wout = jnp.sum(wout_sum, axis=0, keepdims=True)
    lines = []
    for line in (bias, wout):
        high = line.astype(BF16).astype(F32)
        for half in (high, line - high):
            lines += [half[:, :128], half[:, 128:]]
    tail = jnp.concatenate(lines, axis=0)
    total = hidden_ref[...].reshape(-1, 8, width)
    tail = jnp.broadcast_to(tail[None], (total.shape[0], 8, 128))
    even = jnp.concatenate([total[:, :, :128], tail], axis=2)
    odd = jnp.concatenate([total[:, :, 128:], tail], axis=2)
    joined = jnp.stack([even, odd], axis=1).reshape(-1, 8, width)
    send_ref[:, 16:24, :] = joined.astype(BF16)


def decode(got, ends, labels, weights, w_hidden, bias, w_out, parts):
    rows, width = got.shape
    pairs = ends.shape[1]
    return pl.pallas_call(
        decode_body,
        out_shape=(shape_of((1, pairs), F32), shape_of((parts, 24, width), BF16)),
        in_specs=[whole()] * 7,
        out_specs=(whole(), whole()),
        scratch_shapes=[
            pltpu.VMEM((pairs, 2 * width), BF16),
            pltpu.VMEM((pairs, width), BF16),
            pltpu.VMEM((pairs, 2 * width), BF16),
            pltpu.VMEM((2 * width, width), F32),
        ],
        compiler_params=limit(DECODE_MIB),
        cost_estimate=cost(10 * 10**9, 4 * 10**6),
        name="decode",
    )(got, ends, labels, weights, w_hidden, bias, w_out)


def spread_body(
    count_ref, back_ref, want_ref, feat_ref, agg_ref, degree_ref, neigh_ref,
    send_hbm, small_ref, grad_hbm, mean_hbm, send_ref, grad_ref, mean_ref, held_ref, sem, out_sems,
):
    nodes, width = feat_ref.shape
    rows = 1024
    copy = pltpu.make_async_copy(count_ref.at[:, nodes : nodes + held_ref.shape[1]], held_ref, sem)
    copy.start()
    back = back_ref[...].astype(F32)
    tail = jnp.sum(back[:, 16:, :], axis=0)
    small_ref[...] = tail[:, 128:]
    flat = back[:, :16, :].reshape(-1, width).astype(BF16)
    want = jnp.concatenate([want_ref[k : k + 1, :] for k in range(16)], axis=1)

    def gather(i, carry):
        at = i * rows
        span = pl.ds(pl.multiple_of(at, rows), rows)
        grad_ref[span, :] = mm(hot_rows(want - at, rows), flat).astype(BF16)
        return carry

    lax.fori_loop(0, nodes // rows, gather, 0)

    def scale(i, carry):
        span = pl.ds(pl.multiple_of(i * 256, 256), 256)
        degree = jnp.sum(degree_ref[:, span], axis=0, keepdims=True)
        column = jnp.transpose(jnp.broadcast_to(jnp.maximum(degree, 1.0), (128, 256)))
        scaled = mm(grad_ref[span, :], neigh_ref[...], NT) / jnp.concatenate([column, column], axis=1)
        mean_ref[span, :] = scaled.astype(BF16)
        return carry

    lax.fori_loop(0, nodes // 256, scale, 0, unroll=8)
    halves = [(slice(None), slice(0, 8)), (slice(None), slice(8, 16))]
    pairs = [(send_ref.at[half], send_hbm.at[half]) for half in halves]
    pairs += [(grad_ref, grad_hbm), (mean_ref, mean_hbm)]
    leaving = [pltpu.make_async_copy(*pair, out_sems.at[i]) for i, pair in enumerate(pairs)]
    leaving[2].start()
    leaving[3].start()
    both = jnp.concatenate(
        [mm(feat_ref[...], grad_ref[...], TN), mm(agg_ref[...], grad_ref[...], TN)], axis=0
    )
    both = both.reshape(-1, 8, width)
    tail = jnp.broadcast_to(tail[None, :, :128], (both.shape[0], 8, 128))
    even = jnp.concatenate([both[:, :, :128], tail], axis=2)
    odd = jnp.concatenate([both[:, :, 128:], tail], axis=2)
    joined = jnp.stack([even, odd], axis=1).reshape(-1, 8, width)
    send_ref[:, 8:16, :] = joined.astype(BF16)
    leaving[1].start()
    copy.wait()
    blocks = range(0, nodes, DST_BLOCK)
    parts = [mm(held_ref[n // DST_BLOCK], mean_ref[n : n + DST_BLOCK, :]) for n in blocks]
    grad = sum(parts[1:], parts[0]).reshape(-1, 8, width)
    send_ref[:, 0:8, :] = grad.astype(BF16)
    leaving[0].start()
    for copy in leaving:
        copy.wait()


def spread(counts, back, want, features, agg, degree, w_neigh):
    blocks, table, _ = counts.shape
    nodes, width = features.shape
    return pl.pallas_call(
        spread_body,
        out_shape=(
            pltpu.HBM((back.shape[0], 16, width), BF16),
            shape_of((8, 128), F32),
            pltpu.HBM((nodes, width), BF16),
            pltpu.HBM((nodes, width), BF16),
        ),
        in_specs=[whole(pltpu.HBM)] + [whole()] * 6,
        out_specs=(whole(pltpu.HBM), whole(), whole(pltpu.HBM), whole(pltpu.HBM)),
        scratch_shapes=[
            pltpu.VMEM((back.shape[0], 16, width), BF16),
            pltpu.VMEM((nodes, width), BF16),
            pltpu.VMEM((nodes, width), BF16),
            pltpu.VMEM((blocks, table - nodes, DST_BLOCK), BF16),
            pltpu.SemaphoreType.DMA,
            pltpu.SemaphoreType.DMA((4,)),
        ],
        compiler_params=limit(SPREAD_MIB),
        cost_estimate=cost(5 * 10**9, 10 * 10**6),
        name="spread",
    )(counts, back, want, features, agg, degree, w_neigh)


def direct_body(count_ref, grad_ref, mean_ref, self_ref, out_ref, held_ref, sems):
    nodes = out_ref.shape[0]
    rows = 512

    def fetch(i):
        span = pl.ds(pl.multiple_of(i * rows, rows), rows)
        return pltpu.make_async_copy(count_ref.at[:, span], held_ref.at[:, span], sems.at[i])

    for i in range(nodes // rows):
        fetch(i).start()

    def own(i, carry):
        span = pl.ds(pl.multiple_of(i * rows, rows), rows)
        blocks = range(0, nodes, DST_BLOCK)
        total = mm(grad_ref[span, :], self_ref[...], NT)
        fetch(i).wait()
        parts = [mm(held_ref[n // DST_BLOCK, span, :], mean_ref[n : n + DST_BLOCK, :]) for n in blocks]
        out_ref[span, :] = sum(parts[1:], parts[0]) + total
        return carry

    lax.fori_loop(0, nodes // rows, own, 0)


def direct_rows(counts, grad, mean, w_self):
    nodes, width = grad.shape
    return pl.pallas_call(
        direct_body,
        out_shape=pltpu.HBM((nodes, width), F32),
        in_specs=[whole(pltpu.HBM)] + [whole()] * 3,
        out_specs=whole(),
        scratch_shapes=[
            pltpu.VMEM((counts.shape[0], nodes, DST_BLOCK), BF16),
            pltpu.SemaphoreType.DMA((nodes // 512,)),
        ],
        compiler_params=limit(DIRECT_MIB),
        cost_estimate=cost(3 * 10**9, 12 * 10**6),
        name="direct_rows",
    )(counts, grad, mean, w_self)


def chunk_body(back_ref, direct_ref, out_ref):
    del direct_ref
    tail = jnp.sum(back_ref[:, 8:, :128].astype(F32), axis=0)
    out_ref[...] = jnp.broadcast_to(tail[None], out_ref.shape).astype(BF16)


def chunk(back, direct):
    return pl.pallas_call(
        chunk_body,
        out_shape=shape_of((back.shape[0], 8, 128), BF16),
        in_specs=[whole(), whole(pltpu.HBM)],
        out_specs=whole(),
        compiler_params=limit(CHUNK_MIB),
        cost_estimate=cost(10**6, 10**6),
        name="chunk",
    )(back, direct)


def join_lanes(pieces):
    pieces = pieces.reshape(-1, 2, 8, 128)
    return jnp.concatenate([pieces[:, 0], pieces[:, 1]], axis=2).reshape(-1, 256)


def final_body(
    direct_ref, back_ref, halo_ref, small_ref, out_ref, hidden_ref, bias_ref, wout_ref, held_ref, sems
):
    rows = 512
    copies = []
    for i in range(out_ref.shape[0] // rows):
        part = slice(i * rows, (i + 1) * rows)
        copies.append(pltpu.make_async_copy(direct_ref.at[part], held_ref.at[part], sems.at[i]))
        copies[-1].start()
    back = back_ref[...].astype(F32)
    width = back.shape[2]
    flat = back[:, :8, :].reshape(-1, width).astype(BF16)
    halo = jnp.concatenate([halo_ref[k : k + 1, :] for k in range(8)], axis=1)

    def add(i, carry):
        part = pl.ds(pl.multiple_of(i * rows, rows), rows)
        extra = mm(hot_rows(halo - i * rows, rows), flat)
        pltpu.make_async_copy(direct_ref.at[part], held_ref.at[part], sems.at[i]).wait()
        out_ref[part, :] = held_ref[part, :] + extra
        return carry

    lax.fori_loop(0, len(copies), add, 0)
    hidden_ref[...] = join_lanes(back[:, 8:, 128:])
    bias_ref[...] = small_ref[0:2, :] + small_ref[2:4, :]
    wout_ref[...] = small_ref[4:6, :] + small_ref[6:8, :]


def final(direct, back, halo, small):
    nodes, width = direct.shape
    return pl.pallas_call(
        final_body,
        out_shape=(
            shape_of((nodes, width), F32),
            shape_of((2 * width, width), F32),
            shape_of((2, 128), F32),
            shape_of((2, 128), F32),
        ),
        in_specs=[whole(pltpu.HBM)] + [whole()] * 3,
        out_specs=(whole(),) * 4,
        scratch_shapes=[
            pltpu.VMEM((nodes, width), F32),
            pltpu.SemaphoreType.DMA((nodes // 512,)),
        ],
        compiler_params=limit(FINAL_MIB),
        cost_estimate=cost(2 * 10**9, 6 * 10**6),
        name="final",
    )(direct, back, halo, small)


def weights_body(pieces_ref, self_ref, neigh_ref):
    both = join_lanes(pieces_ref[...].astype(F32))
    half = both.shape[0] // 2
    self_ref[...] = both[:half, :]
    neigh_ref[...] = both[half:, :]


def weights(pieces):
    shape = shape_of((256, 256), F32)
    return pl.pallas_call(
        weights_body,
        out_shape=(shape, shape),
        in_specs=[whole()],
        out_specs=(whole(), whole()),
        compiler_params=limit(WEIGHTS_MIB),
        cost_estimate=cost(10**6, 10**6),
        name="weights",
    )(pieces)


def exchange(rows):
    return lax.all_to_all(rows, AXES, split_axis=0, concat_axis=0, tiled=True)


def per_device(
    features, edge_src, edge_dst, edge_count, halo_index, request_rows, pair_ends,
    labels, pair_weight, w_self, w_neigh, w_hidden, b_hidden, w_out,
):
    nodes, width = features.shape
    parts, halo_len = halo_index.shape[1:]
    table = nodes + parts * halo_len
    slots = edge_src.shape[0]
    me = lax.axis_index("dom") * lax.axis_size("grp") + lax.axis_index("grp")

    held = [pltpu.with_memory_space_constraint(x, pltpu.HBM) for x in (halo_index[0].T, request_rows[0].T, features)]
    sent = send_rows((me % 8).reshape(1), *held)
    arrived = exchange(sent)

    src_blocks = table // SRC_BLOCK
    buckets = nodes // DST_BLOCK * src_blocks
    square = (slots // 128, 128)
    keys = sort_edges(edge_count, edge_src.reshape(square), edge_dst.reshape(square), src_blocks, buckets)
    bounds = jnp.arange(buckets + 1, dtype=I32) << 18
    starts = jnp.sum((keys.reshape(1, -1) < bounds[:, None]).astype(I32), axis=1)
    counts, degree = edge_counts(starts, keys, nodes, table)

    fixed = pltpu.with_memory_space_constraint(counts, pltpu.HBM)
    served, agg, want = embed(fixed, arrived, features, degree, w_self, w_neigh)
    got = exchange(served.reshape(parts, -1, width)).reshape(-1, width)
    logits, pair_back = decode(
        got, pair_ends.T, labels.reshape(1, -1), pair_weight.reshape(1, -1),
        w_hidden, b_hidden.reshape(1, -1), w_out.reshape(1, -1), parts,
    )
    back = exchange(pair_back)
    halo_back, small, grad, mean = spread(fixed, back, want, features, agg, degree, w_neigh)
    returned = exchange(halo_back)
    direct = direct_rows(fixed, grad, mean, w_self)
    direct = pltpu.with_memory_space_constraint(direct, pltpu.HBM)
    pieces = exchange(chunk(returned, direct))
    grad_features, grad_hidden, grad_bias, grad_out = final(
        direct, returned, halo_index[0].reshape(8, -1), small
    )
    grad_self, grad_neigh = weights(pieces)
    return (
        logits.reshape(-1), grad_features, grad_self, grad_neigh, grad_hidden,
        grad_bias.reshape(-1), grad_out.reshape(-1),
    )


def solution(mesh):
    split, rows, cubes = P(AXES), P(AXES, None), P(AXES, None, None)
    in_specs = (
        rows, split, split, split, cubes, cubes, rows, split, split, P(), P(), P(), P(), P(),
    )
    out_specs = (split, rows, P(), P(), P(), P(), P())
    return jax.shard_map(
        per_device, mesh=mesh, in_specs=in_specs, out_specs=out_specs, check_vma=False
    )
```
